128 devices in a mesh: blk: 64 (over x, y, z_lo, core), grp: 2 (over z_hi).
Axes of the slice: x: 4, y: 4, z: 4 (z_hi: 2, z_lo: 2; z = z_hi * 2 + z_lo), core: 2. Of those that a mesh axis runs over, the one named last changes fastest.
Arguments:
- sky_maps: float32 [4, 512, 4096], P(None, ('blk', 'grp')), may hold values from -6 to 6
- legendre: bfloat16 [512, 512, 2048], P(('blk', 'grp')), may hold values from -0.25 to 0.25
- owner_table: int32 [512], replicated, may hold values from 0 to 511, each once
Outputs:
- harmonics: float32 [512, 4, 2, 2048], P(('blk', 'grp'))
- spectra: float32 [10, 2048], P(None, ('blk', 'grp'))
The draws below stay inside these ranges and needn't reach their ends.
Inputs may be any that keep to these rules, and one draw needn't show every extreme that they name: `owner_table`: a permutation of the orders 0 to 511.
All inputs are finite; a program needn't handle non-finite values.
Results may differ from the reference program's by a relative error of at most 0.0034.
Values may be sent and summed in bfloat16 or wider, within the bound.
A program may use at most 128 MiB of HBM per device.

```python
import math
import jax
import jax.numpy as jnp
import numpy as np
from jax import lax

MAPS = 4
M = 512
L = 2048
NPHI = 4096
CYCLES = 512


def levels(own_key, shape, shards, smallest, top_value):
    def one(dim, blocks):
        heights = jax.random.uniform(jax.random.fold_in(jax.random.fold_in(own_key, 6), dim), (blocks,), jnp.float32, smallest / len(shards), top_value / len(shards))
        return jnp.repeat(jnp.exp(heights), shape[dim] // blocks).reshape((-1,) + (1,) * (len(shape) - dim - 1))

    loudness = one(*shards[0])
    for cut in shards[1:]:
        loudness = loudness * one(*cut)
    return loudness


def scatter_about(own_key, dims, scale, limit, pieces=(), kind=jnp.bfloat16):
    array = scale * jax.random.normal(own_key, dims, jnp.float32)
    if pieces:
        array = array * levels(own_key, dims, pieces, -0.22, 0.18)
    return jnp.clip(array, -limit, limit).astype(kind)


def setup_inputs(seed: int = 0) -> dict:
    seeds = jax.random.split(jax.random.key(seed), 4)
    sky_maps = scatter_about(seeds[0], (MAPS, CYCLES, NPHI), 1.0, 6.0, ((1, 128),), jnp.float32)
    legendre = scatter_about(seeds[1], (CYCLES, M, L), CYCLES ** -0.5, 0.25, ((0, 128),))
    owner_table = jax.random.permutation(seeds[2], M).astype(jnp.int32)
    return dict(sky_maps=sky_maps, legendre=legendre, owner_table=owner_table)


def reference(sky_maps, legendre, owner_table):
    coeffs = jnp.fft.rfft(sky_maps, axis=-1)[..., :M] / math.sqrt(NPHI)
    fourier = jnp.stack([jnp.real(coeffs), jnp.imag(coeffs)], axis=2)
    fourier = jnp.transpose(fourier, (1, 0, 2, 3)).reshape(CYCLES, 2 * MAPS, M).astype(jnp.bfloat16)
    ell_index = jnp.arange(L, dtype=jnp.int32)

    def per_block(orders):
        table = jnp.take(legendre, orders, axis=1).astype(jnp.float32)
        values = jnp.take(fourier, orders, axis=2).astype(jnp.float32)
        block = jnp.einsum('rcm,rml->mcl', values, table)
        keep = ell_index[None, None, :] >= orders[:, None, None]
        return jnp.where(keep, block, jnp.zeros_like(block))
    harmonics = lax.map(per_block, owner_table.reshape(M // 64, 64)).reshape(M, MAPS, 2, L)
    weight = jnp.where(owner_table == 0, jnp.float32(1.0), jnp.float32(2.0)).astype(jnp.float32)
    cross = jnp.einsum('m,miql,mjql->ijl', weight, harmonics, harmonics)
    first, second = np.triu_indices(MAPS)
    spectra = cross[first, second] / (2 * ell_index + 1).astype(jnp.float32)
    return (harmonics, spectra)
```

```python
import functools
import math

import jax
import jax.numpy as jnp
import numpy as np
from jax import lax
from jax.experimental import pallas as pl
from jax.experimental.pallas import tpu as pltpu
from jax.sharding import PartitionSpec as P

AXES = ("blk", "grp")
MESH = pl.DeviceIdType.MESH
MIB = 1024 * 1024
F32, BF16, I32 = jnp.float32, jnp.bfloat16, jnp.int32

LANES = 256
HALVES = 2
BLOCKS = 16
STEPS = 4
ORDERS = (
    (0, 4, 3, 2, 1, 5), (1, 4, 5, 0, 2, 3), (2, 3, 4, 1, 0, 5), (3, 1, 2, 5, 4, 0),
    (4, 1, 0, 3, 2, 5), (5, 4, 3, 2, 0, 1), (0, 5, 2, 3, 1, 4), (1, 3, 4, 5, 0, 2),
    (2, 0, 4, 5, 3, 1), (3, 5, 1, 0, 4, 2), (4, 2, 1, 5, 0, 3), (5, 2, 0, 3, 4, 1),
    (0, 5, 1, 3, 2, 4), (1, 0, 5, 4, 2, 3), (2, 4, 0, 1, 3, 5), (3, 5, 2, 4, 0, 1),
)


def split_bf16(values):
    high = values.astype(BF16)
    low = (values - high.astype(F32)).astype(BF16)
    return high, low


def dot3(left, right_high, right_low):
    high, low = split_bf16(left)
    dot = functools.partial(jnp.dot, preferred_element_type=F32)
    return dot(high, right_high) + (dot(high, right_low) + dot(low, right_high))


def fourier_tables(pixels, order_count, width):
    coarse = pixels // width
    k1, m1 = np.meshgrid(np.arange(coarse), np.arange(coarse), indexing="ij")
    angle = 2.0 * math.pi * ((k1 * m1) % coarse) / coarse
    first = np.concatenate([np.cos(angle.T), -np.sin(angle.T)], axis=0)
    k2 = np.arange(width)[:, None]
    m = np.arange(order_count)[None, :]
    angle = 2.0 * math.pi * ((k2 * m) % pixels) / pixels
    cosine, sine = np.cos(angle) / math.sqrt(pixels), np.sin(angle) / math.sqrt(pixels)
    second = np.block([[cosine, -sine], [sine, cosine]]).astype(np.float32)
    high = second.astype(BF16)
    low = (second - high.astype(np.float32)).astype(BF16)
    return first.astype(np.float32), high, low


def position():
    blk, grp = lax.axis_index("blk"), lax.axis_index("grp")
    x, y = blk // 16, (blk // 4) % 4
    z = grp * 2 + (blk // 2) % 2
    return x, y, z, blk % 2


def device_at(x, y, z, core):
    return ((x * 4 + y) * 2 + z % 2) * 2 + core, z // 2


def moved(chip, gen):
    axis, kind = gen % 3, gen // 3
    out = []
    for i, c in enumerate(chip):
        other = jnp.where(kind == 0, c + 1 - 2 * (c % 2), 3 - c)
        out.append(jnp.where(axis == i, other, c))
    return tuple(out)


def look_up(values, index):
    total = jnp.int32(0)
    for i, value in enumerate(values):
        if value:
            total = total + jnp.where(index == i, jnp.int32(value), jnp.int32(0))
    return total


def row_slots():
    out = np.zeros((4, BLOCKS, 256), np.int32)
    for b, order in enumerate(ORDERS):
        for row in range(256):
            part, rel, j = row // 128, (row % 128) // 2, row % 2
            flips = [0, 0, 0]
            for k, gen in enumerate(order):
                if (rel >> (5 - k)) & 1:
                    flips[gen % 3] ^= 1 if gen // 3 == 0 else 3
            out[0, b, row] = flips[0] * 16 + flips[1] * 4 + flips[2]
            out[1, b, row] = part
            out[2, b, row] = (b % HALVES) * 2 + j
    return out[:3]


def spectral_values(rows, coarse, x_ref, first, high, low, order_count):
    columns = 2 * order_count
    m1 = lax.broadcasted_iota(I32, (1, coarse, columns), 1)
    col = lax.broadcasted_iota(I32, (1, coarse, columns), 2)
    keep = (col % coarse) == m1
    stages = []
    for b in range(rows):
        stage = jnp.dot(
            first,
            x_ref[b * coarse : (b + 1) * coarse, :],
            precision=lax.Precision.HIGHEST,
            preferred_element_type=F32,
        )
        stages.append(jnp.concatenate([stage[:coarse], stage[coarse:]], axis=1))
    full = dot3(jnp.concatenate(stages, axis=0), high, low)
    full = full.reshape(rows, coarse, columns)
    return jnp.sum(jnp.where(keep, full, 0.0), axis=1).astype(BF16)


def main_body(
    maps,
    cycles,
    orders,
    legendre_ref,
    sky_ref,
    first_ref,
    high_ref,
    low_ref,
    table_ref,
    owned_ref,
    harm_ref,
    spectra_ref,
    leg,
    sky,
    first_buf,
    high_buf,
    low_buf,
    hot,
    own,
    out_core,
    got,
    four,
    four_got,
    coefs,
    s1,
    r1,
    s2,
    r2,
    s3,
    r3,
    s4,
    r4,
    s5,
    r5,
    acc,
    power,
    power_got,
    column,
    column_got,
    leg_sem,
    in_sem,
    core_send,
    core_recv,
    four_sem,
    step_send,
    step_recv,
    last_send,
    last_recv,
    power_sem,
    column_sem,
):
    x, y, z, core = position()
    chip = (x, y, z)
    place = x * 4 + y
    member = ((z % 2) * 2 + core) * 2 + z // 2
    members = 8
    columns = power.shape[0]
    channels = 2 * maps
    tiles = legendre_ref.shape[2] // LANES

    def leg_copy(t):
        return pltpu.make_async_copy(
            legendre_ref.at[:, :, pl.ds(pl.multiple_of(t * LANES, LANES), LANES)], leg.at[t], leg_sem.at[t]
        )

    leg_copy(0).start()
    loads = [
        pltpu.make_async_copy(src, dst, in_sem.at[i])
        for i, (src, dst) in enumerate(
            [(sky_ref, sky), (first_ref, first_buf), (high_ref, high_buf), (low_ref, low_buf)]
        )
    ]
    for load in loads:
        load.start()
    for t in range(1, tiles):
        leg_copy(t).start()

    barrier = pltpu.get_barrier_semaphore()
    partner = device_at(x, y, z, 1 - core)
    near = [partner] + [device_at(*moved(chip, jnp.int32(g)), core) for g in range(6)]
    for device in near:
        pl.semaphore_signal(barrier, inc=1, device_id=device, device_id_type=MESH)

    def remote(src, dst, send, recv, device):
        return pltpu.make_async_remote_copy(
            src_ref=src, dst_ref=dst, send_sem=send, recv_sem=recv, device_id=device, device_id_type=MESH
        )

    def core_copy(b):
        return remote(out_core.at[b], got.at[b], core_send, core_recv.at[b], partner)

    def permute(b):
        t = b // HALVES
        lane = lax.broadcasted_iota(I32, (256, BLOCKS), 1)
        column = jnp.sum(jnp.where(lane == b, table_ref[...], 0), axis=1, keepdims=True)
        one_hot = jnp.where(column == lax.broadcasted_iota(I32, (256, orders), 1), 1.0, 0.0).astype(BF16)
        hot[b] = one_hot[:128]
        for r in range(cycles):
            picked = jnp.dot(one_hot, leg[t, r], preferred_element_type=F32).astype(BF16)
            own[b, r] = picked[:128]
            out_core[b, r] = picked[128:]

    leg_copy(0).wait()
    permute(0)
    pl.semaphore_wait(barrier, len(near))
    core_copy(0).start()
    permute(1)
    core_copy(1).start()

    for load in loads:
        load.wait()
    rows = maps * cycles
    coarse = sky.shape[0] // rows
    spectral = spectral_values(rows, coarse, sky, first_buf[...], high_buf[...], low_buf[...], orders)
    out_row = lax.broadcasted_iota(I32, (cycles * channels, rows), 0)
    in_row = lax.broadcasted_iota(I32, (cycles * channels, rows), 1)
    value = jnp.zeros((cycles * channels, orders), F32)
    for q in range(2):
        wanted = (in_row % cycles) * channels + 2 * (in_row // cycles) + q
        pick = jnp.where(out_row == wanted, 1.0, 0.0).astype(BF16)
        value = value + jnp.dot(pick, spectral[:, q * orders : (q + 1) * orders], preferred_element_type=F32)
    four[...] = value.astype(BF16)
    four_copy = remote(four, four_got, four_sem.at[0], four_sem.at[1], partner)
    four_copy.start()

    def coefficients(b):
        every = jnp.concatenate([four[...], four_got[...]], axis=0)
        coefs[b] = lax.dot_general(
            every, hot[b], (((1,), (1,)), ((), ())), preferred_element_type=F32
        )

    def partial(b, g):
        lane = lax.broadcasted_iota(I32, (channels, 128), 1) // 32
        sides = []
        for side in range(2):
            total = jnp.zeros((channels, 128), F32)
            for q in range(4):
                r = side * 4 + q
                piece = coefs[b, r * channels : (r + 1) * channels, :]
                shift = (32 * (q - g)) % 128
                piece = pltpu.roll(piece, shift, 1) if shift else piece
                total = jnp.where(lane == q, piece, total)
            sides.append(total)
        line = jnp.concatenate(sides, axis=1)
        wide = jnp.broadcast_to(line[None], (32, channels, 256)).reshape(256, 256)
        row = lax.broadcasted_iota(I32, (256, 256), 0) // channels
        col = lax.broadcasted_iota(I32, (256, 256), 1) % 32
        left = jnp.where(row == col, wide, 0.0).astype(BF16)
        right = jnp.concatenate(
            [ref[b, r, 32 * g : 32 * (g + 1), :] for ref in (own, got) for r in range(cycles)], axis=0
        )
        return jnp.dot(left, right, preferred_element_type=F32)

    senders, receivers = (s1, s2, s3, s4), (r1, r2, r3, r4)

    def step_copy(k, b):
        gen = look_up([order[k] for order in ORDERS], b)
        device = device_at(*moved(chip, gen), core)
        return remote(senders[k].at[b], receivers[k].at[b], step_send.at[k], step_recv.at[k, b], device)

    def first_step(b):
        core_copy(b).wait_recv()
        coefficients(b)
        for g in (2, 3):
            s1[b, (g - 2) * 256 : (g - 1) * 256] = partial(b, g).astype(BF16)
        step_copy(0, b).start()

    four_copy.wait_recv()

    def front(t, carry):
        @pl.when(t + 1 < tiles)
        def _():
            leg_copy(t + 1).wait()
            for h in range(HALVES):
                b = HALVES * (t + 1) + h
                permute(b)
                core_copy(b).start()

        for h in range(HALVES):
            first_step(HALVES * t + h)
        return carry

    lax.fori_loop(0, tiles, front, 0)

    def second(b, carry):
        low = partial(b, 0)
        high = partial(b, 1)
        step_copy(0, b).wait_recv()
        s2[b] = (high + r1[b, 256:512].astype(F32)).astype(BF16)
        step_copy(1, b).start()
        acc[b] = low + r1[b, 0:256].astype(F32)
        return carry

    lax.fori_loop(0, BLOCKS, second, 0)

    def third(b, carry):
        step_copy(1, b).wait_recv()
        s3[b] = (acc[b, 128:256] + r2[b, 128:256].astype(F32)).astype(BF16)
        step_copy(2, b).start()
        acc[b, 0:128] = acc[b, 0:128] + r2[b, 0:128].astype(F32)
        return carry

    lax.fori_loop(0, BLOCKS, third, 0)

    def fourth(b, carry):
        step_copy(2, b).wait_recv()
        s4[b] = (acc[b, 64:128] + r3[b, 64:128].astype(F32)).astype(BF16)
        step_copy(3, b).start()
        acc[b, 0:64] = acc[b, 0:64] + r3[b, 0:64].astype(F32)
        return carry

    lax.fori_loop(0, BLOCKS, fourth, 0)

    def last_copies(b):
        gens = [look_up([order[k] for order in ORDERS], b) for k in (4, 5)]
        to = [moved(chip, gens[1]), moved(chip, gens[0])]
        to.append(moved(to[0], gens[0]))
        return [
            remote(s5.at[b, i], r5.at[b, i], last_send.at[i], last_recv.at[b, i], device_at(*where, core))
            for i, where in enumerate(to)
        ]

    def fifth(b, carry):
        step_copy(3, b).wait_recv()
        total = acc[b, 16:64] + r4[b, 16:64].astype(F32)
        for i in range(3):
            s5[b, i] = total[16 * i : 16 * (i + 1)].astype(BF16)
        for copy in last_copies(b):
            copy.start()
        acc[b, 0:16] = acc[b, 0:16] + r4[b, 0:16].astype(F32)
        return carry

    lax.fori_loop(0, BLOCKS, fifth, 0)

    def power_copy(c):
        device = device_at(c // 4, c % 4, z, core)
        return remote(power.at[c], power_got.at[place], power_sem.at[0], power_sem.at[1], device)

    def column_copy(n):
        there = (n % 2) * 2 + n // 4
        device = device_at(x, y, there, (n // 2) % 2)
        return remote(column, column_got.at[member], column_sem.at[0], column_sem.at[1], device)

    def finish(t, carry):
        start = pl.multiple_of(t * LANES, LANES)
        ell = start + lax.broadcasted_iota(I32, (2 * channels, LANES), 1)
        total = [None] * maps
        for h in range(HALVES):
            b = HALVES * t + h
            for copy in last_copies(b):
                copy.wait_recv()
            value = acc[b, 0:16]
            for i in range(3):
                value = value + r5[b, i].astype(F32)
            order = owned_ref[16 * h : 16 * (h + 1), 0:1]
            value = jnp.where(ell >= order, value, 0.0)
            for s in range(2):
                for a in range(maps):
                    row = s * channels + 2 * a
                    harm_ref[2 * h + s, a, :, pl.ds(start, LANES)] = value[row : row + 2]
            weighted = jnp.where(order == 0, value, 2.0 * value)
            for s in range(2):
                mode = value[s * channels : (s + 1) * channels]
                heavy = weighted[s * channels : (s + 1) * channels]
                for k in range(maps // 2 + 1):
                    turned = mode if k == 0 else jnp.concatenate([mode[2 * k :], mode[: 2 * k]], axis=0)
                    term = heavy * turned
                    total[k] = term if total[k] is None else total[k] + term
        lines = []
        for i in range(maps):
            for j in range(i, maps):
                k, a = (j - i, i) if j - i <= maps // 2 else (maps - (j - i), j)
                lines.append(total[k][2 * a : 2 * a + 1] + total[k][2 * a + 1 : 2 * a + 2])
        lines.append(jnp.zeros((power.shape[1] - len(lines), LANES), F32))
        block = jnp.concatenate(lines, axis=0)
        for half in range(LANES // 128):
            c = (LANES // 128) * t + half
            power[c] = block[:, 128 * half : 128 * (half + 1)]

            @pl.when(c != place)
            def _():
                power_copy(c).start()

        return carry

    lax.fori_loop(0, tiles, finish, 0)

    others = columns - 1
    remote(
        power.at[0:others], power_got.at[0:others], power_sem.at[0], power_sem.at[1], partner
    ).wait_recv()
    power_got[place] = power[place]
    total = power_got[0]
    for c in range(1, columns):
        total = total + power_got[c]
    column[...] = total
    for n in range(members):

        @pl.when(n != member)
        def _():
            column_copy(n).start()

    others = members - 1
    whole = remote(
        column_got.at[0:others], column_got.at[0:others], column_sem.at[0], column_sem.at[1], partner
    )
    whole.wait_recv()
    column_got[member] = column[...]
    total = column_got[0]
    for n in range(1, members):
        total = total + column_got[n]
    share = spectra_ref.shape[1]
    ell = place * 128 + lax.broadcasted_iota(I32, total.shape, 1)
    total = total / (2 * ell + 1).astype(F32)
    total = pltpu.roll(total, (128 - share * member) % 128, 1)
    spectra_ref[...] = total[: spectra_ref.shape[0], :share]

    whole.wait_send()
    remote(power.at[0 : columns - 1], power.at[0 : columns - 1], power_sem.at[0], power_sem.at[1], partner).wait_send()
    remote(out_core, got, core_send, core_recv.at[0], partner).wait_send()
    four_copy.wait_send()
    for k in range(STEPS):
        remote(senders[k], receivers[k], step_send.at[k], step_recv.at[k, 0], partner).wait_send()
    for i in range(3):
        remote(s5.at[:, i], r5.at[:, i], last_send.at[i], last_recv.at[0, i], partner).wait_send()


def main_call(devices, sky_maps, legendre, table, owned):
    maps, cycles, pixels = sky_maps.shape
    _, orders, ells = legendre.shape
    width = 128
    coarse = pixels // width
    rows = maps * cycles
    channels = 2 * maps
    tiles = ells // LANES
    pairs = maps * (maps + 1) // 2
    first, high, low = fourier_tables(pixels, orders, width)
    hbm = pl.BlockSpec(memory_space=pl.ANY)
    vmem = pl.BlockSpec(memory_space=pltpu.VMEM)

    def steps(rows_of):
        return [pltpu.VMEM((BLOCKS, n, LANES), BF16) for n in rows_of for _ in range(2)]

    return pl.pallas_call(
        functools.partial(main_body, maps, cycles, orders),
        out_shape=[
            jax.ShapeDtypeStruct((4, maps, 2, ells), F32),
            jax.ShapeDtypeStruct((pairs, ells // devices), F32),
        ],
        in_specs=[hbm] * 5 + [vmem] * 2,
        out_specs=[vmem] * 2,
        scratch_shapes=[
            pltpu.VMEM((tiles, cycles, orders, LANES), BF16),
            pltpu.VMEM((rows * coarse, width), F32),
            pltpu.VMEM(first.shape, F32),
            pltpu.VMEM(high.shape, BF16),
            pltpu.VMEM(low.shape, BF16),
            pltpu.VMEM((BLOCKS, 128, orders), BF16),
            pltpu.VMEM((BLOCKS, cycles, 128, LANES), BF16),
            pltpu.VMEM((BLOCKS, cycles, 128, LANES), BF16),
            pltpu.VMEM((BLOCKS, cycles, 128, LANES), BF16),
            pltpu.VMEM((cycles * channels, orders), BF16),
            pltpu.VMEM((cycles * channels, orders), BF16),
            pltpu.VMEM((BLOCKS, 2 * cycles * channels, 128), F32),
            *steps((512, 256, 128, 64)),
            pltpu.VMEM((BLOCKS, 3, 16, LANES), BF16),
            pltpu.VMEM((BLOCKS, 3, 16, LANES), BF16),
            pltpu.VMEM((BLOCKS, 256, LANES), F32),
            pltpu.VMEM((ells // 128, 16, 128), F32),
            pltpu.VMEM((ells // 128, 16, 128), F32),
            pltpu.VMEM((16, 128), F32),
            pltpu.VMEM((8, 16, 128), F32),
            pltpu.SemaphoreType.DMA((tiles,)),
            pltpu.SemaphoreType.DMA((4,)),
            pltpu.SemaphoreType.DMA,
            pltpu.SemaphoreType.DMA((BLOCKS,)),
            pltpu.SemaphoreType.DMA((2,)),
            pltpu.SemaphoreType.DMA((STEPS,)),
            pltpu.SemaphoreType.DMA((STEPS, BLOCKS)),
            pltpu.SemaphoreType.DMA((3,)),
            pltpu.SemaphoreType.DMA((BLOCKS, 3)),
            pltpu.SemaphoreType.DMA((2,)),
            pltpu.SemaphoreType.DMA((2,)),
        ],
        compiler_params=pltpu.CompilerParams(
            collective_id=0, has_side_effects=True, vmem_limit_bytes=58 * MIB
        ),
        cost_estimate=pl.CostEstimate(flops=10_000_000_000, bytes_accessed=16 * MIB, transcendentals=0),
    )(
        legendre,
        sky_maps.reshape(rows * coarse, width),
        jnp.asarray(first),
        jnp.asarray(high),
        jnp.asarray(low),
        table,
        owned,
    )


def per_device(sky_maps, legendre, owner_table):
    maps = sky_maps.shape[0]
    _, order_count, _ = legendre.shape
    devices = lax.axis_size(AXES)
    own_count = order_count // devices
    channels = 2 * maps
    me = lax.axis_index(AXES)
    x, y, z, core = position()

    flips, parts, items = (jnp.asarray(v.T) for v in row_slots())
    chips = (x * 16 + y * 4 + z) ^ flips
    z_of = chips % 4
    device = (((chips // 4) * 2 + z_of % 2) * 2 + (core ^ parts)) * 2 + z_of // 2
    slot = device * own_count + items
    index = lax.iota(I32, order_count)
    table = jnp.sum(jnp.where(slot[:, :, None] == index, owner_table, 0), axis=2)

    owned = lax.dynamic_slice_in_dim(owner_table, me * own_count, own_count)
    owned = jnp.broadcast_to(owned[:, None, None], (own_count, channels, 128)).reshape(-1, 128)
    harmonics, spectra = main_call(devices, sky_maps, legendre, table, owned)
    return (harmonics, spectra)


def solution(mesh):
    return jax.shard_map(
        per_device,
        mesh=mesh,
        in_specs=(P(None, AXES, None), P(AXES, None, None), P()),
        out_specs=(P(AXES, None, None, None), P(None, AXES)),
        check_vma=False,
    )
```

```python
import functools
import math

import jax
import jax.numpy as jnp
import numpy as np
from jax import lax
from jax.experimental import pallas as pl
from jax.experimental.pallas import tpu as pltpu
from jax.sharding import PartitionSpec as P

AXES = ("blk", "grp")
MESH = pl.DeviceIdType.MESH
MIB = 1024 * 1024
F32, BF16, I32 = jnp.float32, jnp.bfloat16, jnp.int32

LANES = 256
HALVES = 2
BLOCKS = 16
STEPS = 4
ORDERS = (
    (0, 4, 3, 2, 1, 5), (1, 4, 5, 0, 2, 3), (2, 3, 4, 1, 0, 5), (3, 1, 2, 5, 4, 0),
    (4, 1, 0, 3, 2, 5), (5, 4, 3, 2, 0, 1), (0, 5, 2, 3, 1, 4), (1, 3, 4, 5, 0, 2),
    (2, 0, 4, 5, 3, 1), (3, 5, 1, 0, 4, 2), (4, 2, 1, 5, 0, 3), (5, 2, 0, 3, 4, 1),
    (0, 5, 1, 3, 2, 4), (1, 0, 5, 4, 2, 3), (2, 4, 0, 1, 3, 5), (3, 5, 2, 4, 0, 1),
)


def split_bf16(values):
    high = values.astype(BF16)
    low = (values - high.astype(F32)).astype(BF16)
    return high, low


def dot3(left, right_high, right_low):
    high, low = split_bf16(left)
    dot = functools.partial(jnp.dot, preferred_element_type=F32)
    return dot(high, right_high) + (dot(high, right_low) + dot(low, right_high))


def fourier_tables(pixels, order_count, width):
    coarse = pixels // width
    k1, m1 = np.meshgrid(np.arange(coarse), np.arange(coarse), indexing="ij")
    angle = 2.0 * math.pi * ((k1 * m1) % coarse) / coarse
    first = np.concatenate([np.cos(angle.T), -np.sin(angle.T)], axis=0)
    k2 = np.arange(width)[:, None]
    m = np.arange(order_count)[None, :]
    angle = 2.0 * math.pi * ((k2 * m) % pixels) / pixels
    cosine, sine = np.cos(angle) / math.sqrt(pixels), np.sin(angle) / math.sqrt(pixels)
    second = np.block([[cosine, -sine], [sine, cosine]]).astype(np.float32)
    high = second.astype(BF16)
    low = (second - high.astype(np.float32)).astype(BF16)
    return first.astype(np.float32), high, low


def position():
    blk, grp = lax.axis_index("blk"), lax.axis_index("grp")
    x, y = blk // 16, (blk // 4) % 4
    z = grp * 2 + (blk // 2) % 2
    return x, y, z, blk % 2


def device_at(x, y, z, core):
    return ((x * 4 + y) * 2 + z % 2) * 2 + core, z // 2


def moved(chip, gen):
    axis, kind = gen % 3, gen // 3
    out = []
    for i, c in enumerate(chip):
        other = jnp.where(kind == 0, c + 1 - 2 * (c % 2), 3 - c)
        out.append(jnp.where(axis == i, other, c))
    return tuple(out)


def look_up(values, index):
    total = jnp.int32(0)
    for i, value in enumerate(values):
        if value:
            total = total + jnp.where(index == i, jnp.int32(value), jnp.int32(0))
    return total


def row_flips():
    out = np.zeros((2 * BLOCKS, 128), np.int32)
    for b, order in enumerate(ORDERS):
        for row in range(256):
            part, rel, j = row // 128, (row % 128) // 2, row % 2
            flips = [0, 0, 0]
            for k, gen in enumerate(order):
                if (rel >> (5 - k)) & 1:
                    flips[gen % 3] ^= 1 if gen // 3 == 0 else 3
            device = ((flips[0] * 4 + flips[1]) * 2 + flips[2] % 2) * 4 + part * 2 + flips[2] // 2
            out[2 * b + part, row % 128] = device * 4 + (b % HALVES) * 2 + j
    return out


def spectral_values(rows, cycles, coarse, x_ref, first, high, low, order_count):
    columns = 2 * order_count
    m1 = lax.broadcasted_iota(I32, (1, coarse, columns), 1)
    col = lax.broadcasted_iota(I32, (1, coarse, columns), 2)
    keep = (col % coarse) == m1
    stages = []
    for b in range(rows):
        stage = jnp.dot(
            first,
            x_ref[b // cycles, b % cycles],
            precision=lax.Precision.HIGHEST,
            preferred_element_type=F32,
        )
        stages.append(jnp.concatenate([stage[:coarse], stage[coarse:]], axis=1))
    full = dot3(jnp.concatenate(stages, axis=0), high, low)
    full = full.reshape(rows, coarse, columns)
    return jnp.sum(jnp.where(keep, full, 0.0), axis=1).astype(BF16)


def main_body(
    maps,
    cycles,
    orders,
    legendre_ref,
    sky_ref,
    first_ref,
    high_ref,
    low_ref,
    flips_ref,
    table_ref,
    owner_ref,
    harm_ref,
    spectra_ref,
    leg,
    sky,
    first_buf,
    high_buf,
    low_buf,
    lines,
    hot,
    own,
    out_core,
    got,
    four,
    four_got,
    coefs,
    s1,
    r1,
    s2,
    r2,
    s3,
    r3,
    s4,
    r4,
    s5,
    r5,
    acc,
    power,
    power_got,
    column,
    column_got,
    leg_sem,
    in_sem,
    core_send,
    core_recv,
    four_sem,
    step_send,
    step_recv,
    last_send,
    last_recv,
    power_sem,
    column_sem,
):
    x, y, z, core = position()
    chip = (x, y, z)
    place = x * 4 + y
    member = ((z % 2) * 2 + core) * 2 + z // 2
    members = 8
    columns = power.shape[0]
    channels = 2 * maps
    tiles = legendre_ref.shape[2] // LANES

    def leg_copy(t):
        return pltpu.make_async_copy(
            legendre_ref.at[:, :, pl.ds(pl.multiple_of(t * LANES, LANES), LANES)], leg.at[t], leg_sem.at[t]
        )

    leg_copy(0).start()
    coarse = sky.shape[2]

    def sky_copy(k, carry):
        lanes = pl.ds(pl.multiple_of(k * 128, 128), 128)
        pltpu.make_async_copy(sky_ref.at[:, :, lanes], sky.at[:, :, k, :], in_sem.at[0]).start()
        return carry

    loads = [
        pltpu.make_async_copy(src, dst, in_sem.at[i + 1])
        for i, (src, dst) in enumerate([(first_ref, first_buf), (high_ref, high_buf), (low_ref, low_buf)])
    ]
    lax.fori_loop(0, coarse, sky_copy, 0)
    for load in loads:
        load.start()
    loads.append(pltpu.make_async_copy(sky, sky, in_sem.at[0]))
    for t in range(1, tiles):
        leg_copy(t).start()

    barrier = pltpu.get_barrier_semaphore()
    partner = device_at(x, y, z, 1 - core)
    near = [partner] + [device_at(*moved(chip, jnp.int32(g)), core) for g in range(6)]
    for device in near:
        pl.semaphore_signal(barrier, inc=1, device_id=device, device_id_type=MESH)

    def remote(src, dst, send, recv, device):
        return pltpu.make_async_remote_copy(
            src_ref=src, dst_ref=dst, send_sem=send, recv_sem=recv, device_id=device, device_id_type=MESH
        )

    def core_copy(b):
        return remote(out_core.at[b], got.at[b], core_send, core_recv.at[b], partner)

    def permute(b):
        t = b // HALVES
        column = jnp.transpose(lines[b])[:, 0:1].astype(I32)
        one_hot = jnp.where(column == lax.broadcasted_iota(I32, (256, orders), 1), 1.0, 0.0).astype(BF16)
        hot[b] = one_hot[:128]
        for r in range(cycles):
            picked = jnp.dot(one_hot, leg[t, r], preferred_element_type=F32).astype(BF16)
            own[b, r] = picked[:128]
            out_core[b, r] = picked[128:]

    base = ((place * 2 + z % 2) * 4 + core * 2 + z // 2) * 4
    digits = jnp.concatenate([table_ref[...] >> 4, table_ref[...] & 15], axis=0).astype(F32).astype(BF16)
    for b in range(BLOCKS):
        slot = jnp.concatenate([flips_ref[2 * b + i : 2 * b + i + 1, :] for i in range(2)], axis=1) ^ base
        spot = jnp.where(lax.broadcasted_iota(I32, (128, 256), 0) == (slot & 127), 1.0, 0.0).astype(BF16)
        found = jnp.dot(digits, spot, preferred_element_type=F32)
        found = found[0:4] * 16.0 + found[4:8]
        found = jnp.where(lax.broadcasted_iota(I32, (4, 256), 0) == (slot >> 7), found, 0.0)
        lines[b] = jnp.broadcast_to(jnp.sum(found, axis=0, keepdims=True), (8, 256))

    leg_copy(0).wait()
    permute(0)
    pl.semaphore_wait(barrier, len(near))
    core_copy(0).start()
    permute(1)
    core_copy(1).start()

    for load in loads:
        load.wait()
    rows = maps * cycles
    spectral = spectral_values(rows, cycles, coarse, sky, first_buf[...], high_buf[...], low_buf[...], orders)
    out_row = lax.broadcasted_iota(I32, (cycles * channels, rows), 0)
    in_row = lax.broadcasted_iota(I32, (cycles * channels, rows), 1)
    value = jnp.zeros((cycles * channels, orders), F32)
    for q in range(2):
        wanted = (in_row % cycles) * channels + 2 * (in_row // cycles) + q
        pick = jnp.where(out_row == wanted, 1.0, 0.0).astype(BF16)
        value = value + jnp.dot(pick, spectral[:, q * orders : (q + 1) * orders], preferred_element_type=F32)
    four[...] = value.astype(BF16)
    four_copy = remote(four, four_got, four_sem.at[0], four_sem.at[1], partner)
    four_copy.start()

    def coefficients(b):
        every = jnp.concatenate([four[...], four_got[...]], axis=0)
        coefs[b] = lax.dot_general(
            every, hot[b], (((1,), (1,)), ((), ())), preferred_element_type=F32
        )

    def partial(b, g):
        lane = lax.broadcasted_iota(I32, (channels, 128), 1) // 32
        sides = []
        for side in range(2):
            total = jnp.zeros((channels, 128), F32)
            for q in range(4):
                r = side * 4 + q
                piece = coefs[b, r * channels : (r + 1) * channels, :]
                shift = (32 * (q - g)) % 128
                piece = pltpu.roll(piece, shift, 1) if shift else piece
                total = jnp.where(lane == q, piece, total)
            sides.append(total)
        line = jnp.concatenate(sides, axis=1)
        wide = jnp.broadcast_to(line[None], (32, channels, 256)).reshape(256, 256)
        row = lax.broadcasted_iota(I32, (256, 256), 0) // channels
        col = lax.broadcasted_iota(I32, (256, 256), 1) % 32
        left = jnp.where(row == col, wide, 0.0).astype(BF16)
        right = jnp.concatenate(
            [ref[b, r, 32 * g : 32 * (g + 1), :] for ref in (own, got) for r in range(cycles)], axis=0
        )
        return jnp.dot(left, right, preferred_element_type=F32)

    senders, receivers = (s1, s2, s3, s4), (r1, r2, r3, r4)

    def step_copy(k, b):
        gen = look_up([order[k] for order in ORDERS], b)
        device = device_at(*moved(chip, gen), core)
        return remote(senders[k].at[b], receivers[k].at[b], step_send.at[k], step_recv.at[k, b], device)

    def first_step(b):
        core_copy(b).wait_recv()
        coefficients(b)
        for g in (2, 3):
            s1[b, (g - 2) * 256 : (g - 1) * 256] = partial(b, g).astype(BF16)
        step_copy(0, b).start()

    four_copy.wait_recv()

    def front(t, carry):
        @pl.when(t + 1 < tiles)
        def _():
            leg_copy(t + 1).wait()
            for h in range(HALVES):
                b = HALVES * (t + 1) + h
                permute(b)
                core_copy(b).start()

        for h in range(HALVES):
            first_step(HALVES * t + h)
        return carry

    lax.fori_loop(0, tiles, front, 0)

    def second(b, carry):
        low = partial(b, 0)
        high = partial(b, 1)
        step_copy(0, b).wait_recv()
        s2[b] = (high + r1[b, 256:512].astype(F32)).astype(BF16)
        step_copy(1, b).start()
        acc[b] = low + r1[b, 0:256].astype(F32)
        return carry

    lax.fori_loop(0, BLOCKS, second, 0)

    def third(b, carry):
        step_copy(1, b).wait_recv()
        s3[b] = (acc[b, 128:256] + r2[b, 128:256].astype(F32)).astype(BF16)
        step_copy(2, b).start()
        acc[b, 0:128] = acc[b, 0:128] + r2[b, 0:128].astype(F32)
        return carry

    lax.fori_loop(0, BLOCKS, third, 0)

    def fourth(b, carry):
        step_copy(2, b).wait_recv()
        s4[b] = (acc[b, 64:128] + r3[b, 64:128].astype(F32)).astype(BF16)
        step_copy(3, b).start()
        acc[b, 0:64] = acc[b, 0:64] + r3[b, 0:64].astype(F32)
        return carry

    lax.fori_loop(0, BLOCKS, fourth, 0)

    def last_copies(b):
        gens = [look_up([order[k] for order in ORDERS], b) for k in (4, 5)]
        to = [moved(chip, gens[1]), moved(chip, gens[0])]
        to.append(moved(to[0], gens[0]))
        return [
            remote(s5.at[b, i], r5.at[b, i], last_send.at[i], last_recv.at[b, i], device_at(*where, core))
            for i, where in enumerate(to)
        ]

    def fifth(b, carry):
        step_copy(3, b).wait_recv()
        total = acc[b, 16:64] + r4[b, 16:64].astype(F32)
        for i in range(3):
            s5[b, i] = total[16 * i : 16 * (i + 1)].astype(BF16)
        for copy in last_copies(b):
            copy.start()
        acc[b, 0:16] = acc[b, 0:16] + r4[b, 0:16].astype(F32)
        return carry

    lax.fori_loop(0, BLOCKS, fifth, 0)

    def power_copy(c):
        device = device_at(c // 4, c % 4, z, core)
        return remote(power.at[c], power_got.at[place], power_sem.at[0], power_sem.at[1], device)

    def column_copy(n):
        there = (n % 2) * 2 + n // 4
        device = device_at(x, y, there, (n // 2) % 2)
        return remote(column, column_got.at[member], column_sem.at[0], column_sem.at[1], device)

    def finish(t, carry):
        start = pl.multiple_of(t * LANES, LANES)
        ell = start + lax.broadcasted_iota(I32, (2 * channels, LANES), 1)
        total = [None] * maps
        for h in range(HALVES):
            b = HALVES * t + h
            for copy in last_copies(b):
                copy.wait_recv()
            value = acc[b, 0:16]
            for i in range(3):
                value = value + r5[b, i].astype(F32)
            pair = [owner_ref[base + 2 * h + s] for s in range(2)]
            order = jnp.where(lax.broadcasted_iota(I32, (2 * channels, 1), 0) < channels, pair[0], pair[1])
            value = jnp.where(ell >= order, value, 0.0)
            for s in range(2):
                for a in range(maps):
                    row = s * channels + 2 * a
                    harm_ref[2 * h + s, a, :, pl.ds(start, LANES)] = value[row : row + 2]
            weighted = jnp.where(order == 0, value, 2.0 * value)
            for s in range(2):
                mode = value[s * channels : (s + 1) * channels]
                heavy = weighted[s * channels : (s + 1) * channels]
                for k in range(maps // 2 + 1):
                    turned = mode if k == 0 else jnp.concatenate([mode[2 * k :], mode[: 2 * k]], axis=0)
                    term = heavy * turned
                    total[k] = term if total[k] is None else total[k] + term
        lines = []
        for i in range(maps):
            for j in range(i, maps):
                k, a = (j - i, i) if j - i <= maps // 2 else (maps - (j - i), j)
                lines.append(total[k][2 * a : 2 * a + 1] + total[k][2 * a + 1 : 2 * a + 2])
        lines.append(jnp.zeros((power.shape[1] - len(lines), LANES), F32))
        block = jnp.concatenate(lines, axis=0)
        for half in range(LANES // 128):
            c = (LANES // 128) * t + half
            power[c] = block[:, 128 * half : 128 * (half + 1)]

            @pl.when(c != place)
            def _():
                power_copy(c).start()

        return carry

    lax.fori_loop(0, tiles, finish, 0)

    others = columns - 1
    remote(
        power.at[0:others], power_got.at[0:others], power_sem.at[0], power_sem.at[1], partner
    ).wait_recv()
    power_got[place] = power[place]
    total = power_got[0]
    for c in range(1, columns):
        total = total + power_got[c]
    column[...] = total
    for n in range(members):

        @pl.when(n != member)
        def _():
            column_copy(n).start()

    others = members - 1
    whole = remote(
        column_got.at[0:others], column_got.at[0:others], column_sem.at[0], column_sem.at[1], partner
    )
    whole.wait_recv()
    column_got[member] = column[...]
    total = column_got[0]
    for n in range(1, members):
        total = total + column_got[n]
    share = spectra_ref.shape[1]
    ell = place * 128 + lax.broadcasted_iota(I32, total.shape, 1)
    total = total / (2 * ell + 1).astype(F32)
    total = pltpu.roll(total, (128 - share * member) % 128, 1)
    spectra_ref[...] = total[: spectra_ref.shape[0], :share]

    whole.wait_send()
    remote(power.at[0 : columns - 1], power.at[0 : columns - 1], power_sem.at[0], power_sem.at[1], partner).wait_send()
    remote(out_core, got, core_send, core_recv.at[0], partner).wait_send()
    four_copy.wait_send()
    for k in range(STEPS):
        remote(senders[k], receivers[k], step_send.at[k], step_recv.at[k, 0], partner).wait_send()
    for i in range(3):
        remote(s5.at[:, i], r5.at[:, i], last_send.at[i], last_recv.at[0, i], partner).wait_send()


def main_call(devices, sky_maps, legendre, owner_table):
    maps, cycles, pixels = sky_maps.shape
    _, orders, ells = legendre.shape
    width = 128
    coarse = pixels // width
    channels = 2 * maps
    tiles = ells // LANES
    pairs = maps * (maps + 1) // 2
    first, high, low = fourier_tables(pixels, orders, width)
    hbm = pl.BlockSpec(memory_space=pl.ANY)
    vmem = pl.BlockSpec(memory_space=pltpu.VMEM)

    def steps(rows_of):
        return [pltpu.VMEM((BLOCKS, n, LANES), BF16) for n in rows_of for _ in range(2)]

    return pl.pallas_call(
        functools.partial(main_body, maps, cycles, orders),
        out_shape=[
            jax.ShapeDtypeStruct((4, maps, 2, ells), F32),
            jax.ShapeDtypeStruct((pairs, ells // devices), F32),
        ],
        in_specs=[hbm] * 5 + [vmem] * 2 + [pl.BlockSpec(memory_space=pltpu.SMEM)],
        out_specs=[vmem] * 2,
        scratch_shapes=[
            pltpu.VMEM((tiles, cycles, orders, LANES), BF16),
            pltpu.VMEM((maps, cycles, coarse, width), F32),
            pltpu.VMEM(first.shape, F32),
            pltpu.VMEM(high.shape, BF16),
            pltpu.VMEM(low.shape, BF16),
            pltpu.VMEM((BLOCKS, 8, 256), F32),
            pltpu.VMEM((BLOCKS, 128, orders), BF16),
            pltpu.VMEM((BLOCKS, cycles, 128, LANES), BF16),
            pltpu.VMEM((BLOCKS, cycles, 128, LANES), BF16),
            pltpu.VMEM((BLOCKS, cycles, 128, LANES), BF16),
            pltpu.VMEM((cycles * channels, orders), BF16),
            pltpu.VMEM((cycles * channels, orders), BF16),
            pltpu.VMEM((BLOCKS, 2 * cycles * channels, 128), F32),
            *steps((512, 256, 128, 64)),
            pltpu.VMEM((BLOCKS, 3, 16, LANES), BF16),
            pltpu.VMEM((BLOCKS, 3, 16, LANES), BF16),
            pltpu.VMEM((BLOCKS, 256, LANES), F32),
            pltpu.VMEM((ells // 128, 16, 128), F32),
            pltpu.VMEM((ells // 128, 16, 128), F32),
            pltpu.VMEM((16, 128), F32),
            pltpu.VMEM((8, 16, 128), F32),
            pltpu.SemaphoreType.DMA((tiles,)),
            pltpu.SemaphoreType.DMA((4,)),
            pltpu.SemaphoreType.DMA,
            pltpu.SemaphoreType.DMA((BLOCKS,)),
            pltpu.SemaphoreType.DMA((2,)),
            pltpu.SemaphoreType.DMA((STEPS,)),
            pltpu.SemaphoreType.DMA((STEPS, BLOCKS)),
            pltpu.SemaphoreType.DMA((3,)),
            pltpu.SemaphoreType.DMA((BLOCKS, 3)),
            pltpu.SemaphoreType.DMA((2,)),
            pltpu.SemaphoreType.DMA((2,)),
        ],
        compiler_params=pltpu.CompilerParams(
            collective_id=0, has_side_effects=True, vmem_limit_bytes=58 * MIB
        ),
        cost_estimate=pl.CostEstimate(flops=10_000_000_000, bytes_accessed=16 * MIB, transcendentals=0),
    )(
        legendre,
        sky_maps,
        jnp.asarray(first),
        jnp.asarray(high),
        jnp.asarray(low),
        jnp.asarray(row_flips()),
        owner_table.reshape(4, 128),
        owner_table,
    )


def per_device(sky_maps, legendre, owner_table):
    devices = lax.axis_size(AXES)
    harmonics, spectra = main_call(devices, sky_maps, legendre, owner_table)
    return (harmonics, spectra)


def solution(mesh):
    return jax.shard_map(
        per_device,
        mesh=mesh,
        in_specs=(P(None, AXES, None), P(AXES, None, None), P()),
        out_specs=(P(AXES, None, None, None), P(None, AXES)),
        check_vma=False,
    )
```

```python
import functools
import math

import jax
import jax.numpy as jnp
import numpy as np
from jax import lax
from jax.experimental import pallas as pl
from jax.experimental.pallas import tpu as pltpu
from jax.sharding import PartitionSpec as P

AXES = ("blk", "grp")
MESH = pl.DeviceIdType.MESH
MIB = 1024 * 1024
F32, BF16, I32 = jnp.float32, jnp.bfloat16, jnp.int32

LANES = 256
HALVES = 2
BLOCKS = 16
STEPS = 4
ORDERS = (
    (0, 4, 3, 2, 1, 5), (1, 4, 5, 0, 2, 3), (2, 3, 4, 1, 0, 5), (3, 1, 2, 5, 4, 0),
    (4, 1, 0, 3, 2, 5), (5, 4, 3, 2, 0, 1), (0, 5, 2, 3, 1, 4), (1, 3, 4, 5, 0, 2),
    (2, 0, 4, 5, 3, 1), (3, 5, 1, 0, 4, 2), (4, 2, 1, 5, 0, 3), (5, 2, 0, 3, 4, 1),
    (0, 5, 1, 3, 2, 4), (1, 0, 5, 4, 2, 3), (2, 4, 0, 1, 3, 5), (3, 5, 2, 4, 0, 1),
)


def split_bf16(values):
    high = values.astype(BF16)
    low = (values - high.astype(F32)).astype(BF16)
    return high, low


def dot3(left, right_high, right_low):
    high, low = split_bf16(left)
    dot = functools.partial(jnp.dot, preferred_element_type=F32)
    return dot(high, right_high) + (dot(high, right_low) + dot(low, right_high))


def fourier_tables(pixels, order_count, width):
    coarse = pixels // width
    k1, m1 = np.meshgrid(np.arange(coarse), np.arange(coarse), indexing="ij")
    angle = 2.0 * math.pi * ((k1 * m1) % coarse) / coarse
    first = np.concatenate([np.cos(angle.T), -np.sin(angle.T)], axis=0)
    k2 = np.arange(width)[:, None]
    m = np.arange(order_count)[None, :]
    angle = 2.0 * math.pi * ((k2 * m) % pixels) / pixels
    cosine, sine = np.cos(angle) / math.sqrt(pixels), np.sin(angle) / math.sqrt(pixels)
    second = np.block([[cosine, -sine], [sine, cosine]]).astype(np.float32)
    high = second.astype(BF16)
    low = (second - high.astype(np.float32)).astype(BF16)
    first = first.astype(np.float32)
    first_high = first.astype(BF16)
    first_low = (first - first_high.astype(np.float32)).astype(BF16)
    return np.stack([first_high, first_low]), high, low


def position():
    blk, grp = lax.axis_index("blk"), lax.axis_index("grp")
    x, y = blk // 16, (blk // 4) % 4
    z = grp * 2 + (blk // 2) % 2
    return x, y, z, blk % 2


def device_at(x, y, z, core):
    return ((x * 4 + y) * 2 + z % 2) * 2 + core, z // 2


def moved(chip, gen):
    axis, kind = gen % 3, gen // 3
    out = []
    for i, c in enumerate(chip):
        if isinstance(gen, int):
            out.append((c + 1 - 2 * (c % 2) if kind == 0 else 3 - c) if axis == i else c)
            continue
        other = jnp.where(kind == 0, c + 1 - 2 * (c % 2), 3 - c)
        out.append(jnp.where(axis == i, other, c))
    return tuple(out)


def look_up(values, index):
    total = jnp.int32(0)
    for i, value in enumerate(values):
        if value:
            total = total + jnp.where(index == i, jnp.int32(value), jnp.int32(0))
    return total


def row_flips():
    out = np.zeros((2, BLOCKS // HALVES, HALVES, 2, 32, 2), np.int32)
    for half, t, h, part, low, j in np.ndindex(*out.shape):
        flips = [0, 0, 0]
        for k, gen in enumerate(ORDERS[HALVES * t + h]):
            if ((half * 32 + low) >> (5 - k)) & 1:
                flips[gen % 3] ^= 1 if gen // 3 == 0 else 3
        device = ((flips[0] * 4 + flips[1]) * 2 + flips[2] % 2) * 4 + part * 2 + flips[2] // 2
        out[half, t, h, part, low, j] = device * 4 + h * 2 + j
    return out.reshape(-1, 256)


def spectral_values(x_ref, first, high, low):
    maps, cycles, coarse, width = x_ref.shape
    rows = maps * cycles
    columns = high.shape[1]
    x_high, x_low = split_bf16(jnp.concatenate([x_ref[i // cycles, i % cycles] for i in range(rows)], axis=1))
    dot = functools.partial(jnp.dot, preferred_element_type=F32)
    stage = dot(first[0], x_high) + (dot(first[0], x_low) + dot(first[1], x_high))
    stages = []
    for i in range(rows):
        piece = stage[:, i * width : (i + 1) * width]
        stages.append(jnp.concatenate([piece[:coarse], piece[coarse:]], axis=1))
    full = dot3(jnp.concatenate(stages, axis=0), high, low)
    m1 = lax.broadcasted_iota(I32, (1, coarse, columns), 1)
    col = lax.broadcasted_iota(I32, (1, coarse, columns), 2)
    full = jnp.where((col % coarse) == m1, full.reshape(rows, coarse, columns), 0.0)
    return jnp.sum(full, axis=1).astype(BF16)


def main_body(
    maps,
    cycles,
    orders,
    legendre_ref,
    sky_ref,
    first_ref,
    high_ref,
    low_ref,
    flips_ref,
    table_ref,
    owner_ref,
    harm_ref,
    spectra_ref,
    leg,
    sky,
    first_buf,
    high_buf,
    low_buf,
    lines,
    hot,
    own,
    out_core,
    got,
    four,
    four_got,
    s1,
    r1,
    s2,
    r2,
    s3,
    r3,
    s4,
    r4,
    s5,
    r5,
    acc,
    power,
    power_got,
    column,
    column_got,
    leg_sem,
    in_sem,
    core_send,
    core_recv,
    four_sem,
    step_send,
    step_recv,
    last_send,
    last_recv,
    power_sem,
    column_sem,
):
    x, y, z, core = position()
    chip = (x, y, z)
    place = x * 4 + y
    member = ((z % 2) * 2 + core) * 2 + z // 2
    members = 8
    columns = power.shape[0]
    channels = 2 * maps
    tiles = legendre_ref.shape[2] // LANES

    def leg_copy(t):
        return pltpu.make_async_copy(
            legendre_ref.at[:, :, pl.ds(pl.multiple_of(t * LANES, LANES), LANES)], leg.at[t], leg_sem.at[t]
        )

    leg_copy(0).start()
    coarse = sky.shape[2]

    def sky_copy(k, carry):
        lanes = pl.ds(pl.multiple_of(k * 128, 128), 128)
        pltpu.make_async_copy(sky_ref.at[:, :, lanes], sky.at[:, :, k, :], in_sem.at[0]).start()
        return carry

    loads = [
        pltpu.make_async_copy(src, dst, in_sem.at[i + 1])
        for i, (src, dst) in enumerate([(first_ref, first_buf), (high_ref, high_buf), (low_ref, low_buf)])
    ]
    lax.fori_loop(0, coarse, sky_copy, 0)
    for load in loads:
        load.start()
    loads.append(pltpu.make_async_copy(sky, sky, in_sem.at[0]))
    for t in range(1, tiles):
        leg_copy(t).start()

    barrier = pltpu.get_barrier_semaphore()
    partner = device_at(x, y, z, 1 - core)
    across = [device_at(*moved(chip, g), core) for g in range(6)]
    near = [partner] + across
    for device in near:
        pl.semaphore_signal(barrier, inc=1, device_id=device, device_id_type=MESH)

    def remote(src, dst, send, recv, device):
        return pltpu.make_async_remote_copy(
            src_ref=src, dst_ref=dst, send_sem=send, recv_sem=recv, device_id=device, device_id_type=MESH
        )

    def core_copy(half, t):
        return remote(out_core.at[half, t], got.at[half, t], core_send, core_recv.at[half, t], partner)

    def make_hot(half, t):
        column = jnp.transpose(lines[half * tiles + t])[:, 0:1].astype(I32)
        lane = lax.broadcasted_iota(I32, (256, orders), 1)
        hot[half, t] = jnp.where(column == lane, 1.0, 0.0).astype(BF16)

    def permute(half, t):
        one_hot = hot[half, t]
        for r in range(cycles):
            picked = jnp.dot(one_hot, leg[t, r], preferred_element_type=F32).astype(BF16)
            for h in range(HALVES):
                own[half, t, h, r] = picked[128 * h : 128 * h + 64]
                out_core[half, t, h, r] = picked[128 * h + 64 : 128 * (h + 1)]

    base = ((place * 2 + z % 2) * 4 + core * 2 + z // 2) * 4
    digits = jnp.concatenate([table_ref[...] >> 4, table_ref[...] & 15], axis=0).astype(F32).astype(BF16)
    for i in range(2 * tiles):
        slot = flips_ref[i : i + 1, :] ^ base
        spot = jnp.where(lax.broadcasted_iota(I32, (128, 256), 0) == (slot & 127), 1.0, 0.0).astype(BF16)
        found = jnp.dot(digits, spot, preferred_element_type=F32)
        found = found[0:4] * 16.0 + found[4:8]
        found = jnp.where(lax.broadcasted_iota(I32, (4, 256), 0) == (slot >> 7), found, 0.0)
        lines[i] = jnp.broadcast_to(jnp.sum(found, axis=0, keepdims=True), (8, 256))
    for t in range(2):
        make_hot(1, t)

    for load in loads:
        load.wait()
    spectral = spectral_values(sky, first_buf, high_buf[...], low_buf[...])
    rows = maps * cycles
    out_row = lax.broadcasted_iota(I32, (cycles * channels, rows), 0)
    in_row = lax.broadcasted_iota(I32, (cycles * channels, rows), 1)
    value = jnp.zeros((cycles * channels, orders), F32)
    for q in range(2):
        wanted = (in_row % cycles) * channels + 2 * (in_row // cycles) + q
        pick = jnp.where(out_row == wanted, 1.0, 0.0).astype(BF16)
        value = value + jnp.dot(pick, spectral[:, q * orders : (q + 1) * orders], preferred_element_type=F32)
    four[...] = value.astype(BF16)
    pl.semaphore_wait(barrier, len(near))
    four_copy = remote(four, four_got, four_sem.at[0], four_sem.at[1], partner)
    four_copy.start()
    leg_copy(0).wait()
    permute(1, 0)
    core_copy(1, 0).start()

    def coefficients(half, t):
        every = jnp.concatenate([four[...], four_got[...]], axis=0)
        mine = jnp.concatenate([hot[half, t, 128 * h : 128 * h + 64, :] for h in range(HALVES)], axis=0)
        return lax.dot_general(every, mine, (((1,), (1,)), ((), ())), preferred_element_type=F32)

    def partial(half, t, coefs, g):
        lane = lax.broadcasted_iota(I32, (channels, 128), 1) // 32
        sides = []
        for side in range(2):
            total = jnp.zeros((channels, 128), F32)
            for q in range(4):
                r = side * 4 + q
                piece = coefs[r * channels : (r + 1) * channels, :]
                shift = (32 * (q - g)) % 128
                piece = pltpu.roll(piece, shift, 1) if shift else piece
                total = jnp.where(lane == q, piece, total)
            sides.append(total)
        line = jnp.concatenate(sides, axis=1)
        wide = jnp.broadcast_to(line[None], (32, channels, 256)).reshape(256, 256)
        row = lax.broadcasted_iota(I32, (256, 256), 0) // channels
        col = lax.broadcasted_iota(I32, (256, 256), 1) % 32
        left = jnp.where(row == col, wide, 0.0).astype(BF16)
        at = slice(32 * (g % 2), 32 * (g % 2) + 32)
        right = jnp.concatenate(
            [ref[half, t, g // 2, r, at, :] for ref in (own, got) for r in range(cycles)], axis=0
        )
        return jnp.dot(left, right, preferred_element_type=F32)

    senders, receivers = (s1, s2, s3, s4), (r1, r2, r3, r4)

    def step_copy(k, b):
        if isinstance(b, int):
            device = across[ORDERS[b][k]]
        else:
            device = device_at(*moved(chip, look_up([order[k] for order in ORDERS], b)), core)
        return remote(senders[k].at[b], receivers[k].at[b], step_send.at[k], step_recv.at[k, b], device)

    four_copy.wait_recv()

    def front(t, carry):
        @pl.when(t + 1 < tiles)
        def _():
            leg_copy(t + 1).wait()
            permute(1, t + 1)
            core_copy(1, t + 1).start()

        core_copy(1, t).wait_recv()
        coefs = coefficients(1, t)
        for g in range(4):
            s1[HALVES * t + g // 2, (g % 2) * 256 : (g % 2 + 1) * 256] = partial(1, t, coefs, g).astype(BF16)
        ahead = t + 2
        make_hot(jnp.where(ahead < tiles, 1, 0), ahead % tiles)
        for h in range(HALVES):
            step_copy(0, HALVES * t + h).start()
        return carry

    lax.fori_loop(0, tiles, front, 0)

    permute(0, 0)
    core_copy(0, 0).start()

    def second(t, carry):
        @pl.when(t + 1 < tiles)
        def _():
            permute(0, t + 1)
            core_copy(0, t + 1).start()

        core_copy(0, t).wait_recv()
        coefs = coefficients(0, t)
        for g in range(4):
            acc[HALVES * t + g // 2, (g % 2) * 256 : (g % 2 + 1) * 256] = partial(0, t, coefs, g)
        make_hot(0, (t + 2) % tiles)
        for h in range(HALVES):
            b = HALVES * t + h
            step_copy(0, b).wait_recv()
            s2[b] = (acc[b, 256:512] + r1[b, 256:512].astype(F32)).astype(BF16)
            step_copy(1, b).start()
            acc[b, 0:256] = acc[b, 0:256] + r1[b, 0:256].astype(F32)
        return carry

    lax.fori_loop(0, tiles, second, 0)

    for k in (2, 3):
        n = 512 >> k
        for b in range(BLOCKS):
            step_copy(k - 1, b).wait_recv()
            got_ref = receivers[k - 1]
            senders[k][b] = (acc[b, n : 2 * n] + got_ref[b, n : 2 * n].astype(F32)).astype(BF16)
            step_copy(k, b).start()
            acc[b, 0:n] = acc[b, 0:n] + got_ref[b, 0:n].astype(F32)

    def last_copies(b):
        near, far = ORDERS[b][5], ORDERS[b][4]
        to = [across[near], across[far], device_at(*moved(moved(chip, near), far), core)]
        return [
            remote(s5.at[b, i], r5.at[b, i], last_send.at[i], last_recv.at[b, i], device)
            for i, device in enumerate(to)
        ]

    for b in range(BLOCKS):
        step_copy(3, b).wait_recv()
        total = acc[b, 16:64] + r4[b, 16:64].astype(F32)
        for i in range(3):
            s5[b, i] = total[16 * i : 16 * (i + 1)].astype(BF16)
        for copy in last_copies(b):
            copy.start()
        acc[b, 0:16] = acc[b, 0:16] + r4[b, 0:16].astype(F32)

    def power_copy(c):
        device = device_at(c // 4, c % 4, z, core)
        return remote(power.at[c], power_got.at[place], power_sem.at[0], power_sem.at[1], device)

    def column_copy(n):
        there = (n % 2) * 2 + n // 4
        device = device_at(x, y, there, (n // 2) % 2)
        return remote(column, column_got.at[member], column_sem.at[0], column_sem.at[1], device)

    def finish(t):
        lanes = slice(t * LANES, (t + 1) * LANES)
        ell = t * LANES + lax.broadcasted_iota(I32, (2 * channels, LANES), 1)
        total = [None] * maps
        for h in range(HALVES):
            b = HALVES * t + h
            for copy in last_copies(b):
                copy.wait_recv()
            value = acc[b, 0:16]
            for i in range(3):
                value = value + r5[b, i].astype(F32)
            pair = [owner_ref[base + 2 * h + s] for s in range(2)]
            order = jnp.where(lax.broadcasted_iota(I32, (2 * channels, 1), 0) < channels, pair[0], pair[1])
            value = jnp.where(ell >= order, value, 0.0)
            for s in range(2):
                for a in range(maps):
                    row = s * channels + 2 * a
                    harm_ref[2 * h + s, a, :, lanes] = value[row : row + 2]
            weighted = jnp.where(order == 0, value, 2.0 * value)
            for s in range(2):
                mode = value[s * channels : (s + 1) * channels]
                heavy = weighted[s * channels : (s + 1) * channels]
                for k in range(maps // 2 + 1):
                    turned = mode if k == 0 else jnp.concatenate([mode[2 * k :], mode[: 2 * k]], axis=0)
                    term = heavy * turned
                    total[k] = term if total[k] is None else total[k] + term
        rows = []
        for i in range(maps):
            for j in range(i, maps):
                k, a = (j - i, i) if j - i <= maps // 2 else (maps - (j - i), j)
                rows.append(total[k][2 * a : 2 * a + 1] + total[k][2 * a + 1 : 2 * a + 2])
        rows.append(jnp.zeros((power.shape[1] - len(rows), LANES), F32))
        block = jnp.concatenate(rows, axis=0)
        for half in range(LANES // 128):
            c = (LANES // 128) * t + half
            power[c] = block[:, 128 * half : 128 * (half + 1)]

            @pl.when(c != place)
            def _():
                power_copy(c).start()

    for t in range(tiles):
        finish(t)

    others = columns - 1
    remote(
        power.at[0:others], power_got.at[0:others], power_sem.at[0], power_sem.at[1], partner
    ).wait_recv()
    power_got[place] = power[place]
    total = power_got[0]
    for c in range(1, columns):
        total = total + power_got[c]
    column[...] = total
    for n in range(members):

        @pl.when(n != member)
        def _():
            column_copy(n).start()

    others = members - 1
    whole = remote(
        column_got.at[0:others], column_got.at[0:others], column_sem.at[0], column_sem.at[1], partner
    )
    whole.wait_recv()
    column_got[member] = column[...]
    total = column_got[0]
    for n in range(1, members):
        total = total + column_got[n]
    share = spectra_ref.shape[1]
    ell = place * 128 + lax.broadcasted_iota(I32, total.shape, 1)
    total = total / (2 * ell + 1).astype(F32)
    total = pltpu.roll(total, (128 - share * member) % 128, 1)
    spectra_ref[...] = total[: spectra_ref.shape[0], :share]

    whole.wait_send()
    others = columns - 1
    remote(
        power.at[0:others], power_got.at[0:others], power_sem.at[0], power_sem.at[1], partner
    ).wait_send()
    remote(out_core, got, core_send, core_recv.at[0, 0], partner).wait_send()
    four_copy.wait_send()
    for k in range(STEPS):
        remote(senders[k], receivers[k], step_send.at[k], step_recv.at[k, 0], partner).wait_send()
    for i in range(3):
        remote(s5.at[:, i], r5.at[:, i], last_send.at[i], last_recv.at[0, i], partner).wait_send()


def main_call(devices, sky_maps, legendre, owner_table):
    maps, cycles, pixels = sky_maps.shape
    _, orders, ells = legendre.shape
    width = 128
    coarse = pixels // width
    channels = 2 * maps
    tiles = ells // LANES
    pairs = maps * (maps + 1) // 2
    first, high, low = fourier_tables(pixels, orders, width)
    hbm = pl.BlockSpec(memory_space=pl.ANY)
    vmem = pl.BlockSpec(memory_space=pltpu.VMEM)

    def steps(rows_of):
        return [pltpu.VMEM((BLOCKS, n, LANES), BF16) for n in rows_of for _ in range(2)]

    return pl.pallas_call(
        functools.partial(main_body, maps, cycles, orders),
        out_shape=[
            jax.ShapeDtypeStruct((4, maps, 2, ells), F32),
            jax.ShapeDtypeStruct((pairs, ells // devices), F32),
        ],
        in_specs=[hbm] * 5 + [vmem] * 2 + [pl.BlockSpec(memory_space=pltpu.SMEM)],
        out_specs=[vmem] * 2,
        scratch_shapes=[
            pltpu.VMEM((tiles, cycles, orders, LANES), BF16),
            pltpu.VMEM((maps, cycles, coarse, width), F32),
            pltpu.VMEM(first.shape, BF16),
            pltpu.VMEM(high.shape, BF16),
            pltpu.VMEM(low.shape, BF16),
            pltpu.VMEM((2 * tiles, 8, 256), F32),
            pltpu.VMEM((2, tiles, 256, orders), BF16),
            pltpu.VMEM((2, tiles, HALVES, cycles, 64, LANES), BF16),
            pltpu.VMEM((2, tiles, HALVES, cycles, 64, LANES), BF16),
            pltpu.VMEM((2, tiles, HALVES, cycles, 64, LANES), BF16),
            pltpu.VMEM((cycles * channels, orders), BF16),
            pltpu.VMEM((cycles * channels, orders), BF16),
            *steps((512, 256, 128, 64)),
            pltpu.VMEM((BLOCKS, 3, 16, LANES), BF16),
            pltpu.VMEM((BLOCKS, 3, 16, LANES), BF16),
            pltpu.VMEM((BLOCKS, 512, LANES), F32),
            pltpu.VMEM((ells // 128, 16, 128), F32),
            pltpu.VMEM((ells // 128, 16, 128), F32),
            pltpu.VMEM((16, 128), F32),
            pltpu.VMEM((8, 16, 128), F32),
            pltpu.SemaphoreType.DMA((tiles,)),
            pltpu.SemaphoreType.DMA((4,)),
            pltpu.SemaphoreType.DMA,
            pltpu.SemaphoreType.DMA((2, tiles)),
            pltpu.SemaphoreType.DMA((2,)),
            pltpu.SemaphoreType.DMA((STEPS,)),
            pltpu.SemaphoreType.DMA((STEPS, BLOCKS)),
            pltpu.SemaphoreType.DMA((3,)),
            pltpu.SemaphoreType.DMA((BLOCKS, 3)),
            pltpu.SemaphoreType.DMA((2,)),
            pltpu.SemaphoreType.DMA((2,)),
        ],
        compiler_params=pltpu.CompilerParams(
            collective_id=0, has_side_effects=True, vmem_limit_bytes=58 * MIB
        ),
        cost_estimate=pl.CostEstimate(flops=10_000_000_000, bytes_accessed=16 * MIB, transcendentals=0),
    )(
        legendre,
        sky_maps,
        jnp.asarray(first),
        jnp.asarray(high),
        jnp.asarray(low),
        jnp.asarray(row_flips()),
        owner_table.reshape(4, 128),
        owner_table,
    )


def per_device(sky_maps, legendre, owner_table):
    devices = lax.axis_size(AXES)
    harmonics, spectra = main_call(devices, sky_maps, legendre, owner_table)
    return (harmonics, spectra)


def solution(mesh):
    return jax.shard_map(
        per_device,
        mesh=mesh,
        in_specs=(P(None, AXES, None), P(AXES, None, None), P()),
        out_specs=(P(AXES, None, None, None), P(None, AXES)),
        check_vma=False,
    )
```

```python
import functools
import math

import jax
import jax.numpy as jnp
import numpy as np
from jax import lax
from jax.experimental import pallas as pl
from jax.experimental.pallas import tpu as pltpu
from jax.sharding import PartitionSpec as P

AXES = ("blk", "grp")
MESH = pl.DeviceIdType.MESH
MIB = 1024 * 1024
F32, BF16, I32 = jnp.float32, jnp.bfloat16, jnp.int32

LANES = 256
HALVES = 2
BLOCKS = 16
STEPS = 4
ORDERS = (
    (5, 4, 1, 2, 3, 0), (0, 1, 3, 5, 4, 2), (5, 0, 3, 1, 4, 2), (1, 3, 5, 0, 2, 4),
    (0, 4, 2, 3, 1, 5), (3, 1, 2, 4, 0, 5), (1, 0, 3, 2, 4, 5), (4, 2, 5, 3, 1, 0),
    (1, 4, 5, 0, 2, 3), (2, 5, 1, 0, 4, 3), (3, 5, 1, 2, 0, 4), (5, 2, 0, 3, 4, 1),
    (2, 3, 1, 0, 4, 5), (3, 2, 5, 1, 0, 4), (0, 2, 1, 3, 4, 5), (4, 1, 3, 2, 5, 0),
)

PROGRAM = (
    ("F", 0, 0), ("F", 1, 0), ("F", 2, 0), ("F", 3, 0), ("F", 4, 0), ("F", 5, 0), ("F", 6, 0), ("F", 7, 0),
    ("K", 0, 0), ("S", 0, 0), ("S", 1, 0), ("K", 1, 0), ("S", 3, 0), ("K", 2, 0), ("K", 3, 0), ("S", 5, 0),
    ("S", 2, 0), ("K", 4, 0), ("S", 7, 0), ("K", 5, 0), ("S", 4, 0), ("S", 9, 0), ("K", 6, 0), ("S", 6, 0),
    ("K", 7, 0), ("S", 10, 0), ("S", 11, 0), ("S", 15, 0), ("S", 12, 0), ("S", 14, 0), ("S", 8, 0), ("S", 9, 1),
    ("S", 0, 1), ("S", 7, 1), ("S", 2, 1), ("S", 13, 0), ("S", 1, 1), ("S", 10, 1), ("S", 4, 1), ("S", 11, 1),
    ("S", 6, 1), ("S", 3, 1), ("S", 7, 2), ("S", 5, 1), ("S", 14, 1), ("S", 8, 1), ("S", 12, 1), ("S", 13, 1),
    ("S", 15, 1), ("S", 11, 2), ("S", 2, 2), ("S", 9, 2), ("S", 4, 2), ("S", 1, 2), ("S", 0, 2), ("S", 3, 2),
    ("S", 6, 2), ("S", 10, 2), ("S", 5, 2), ("S", 7, 3), ("S", 8, 2), ("S", 14, 2), ("S", 15, 2), ("S", 13, 2),
    ("S", 12, 2), ("S", 2, 3), ("S", 9, 3), ("S", 11, 3), ("S", 1, 3), ("S", 4, 3), ("S", 0, 3), ("S", 3, 3),
    ("S", 6, 3), ("S", 10, 3), ("S", 5, 3), ("S", 8, 3), ("S", 14, 3), ("S", 15, 3), ("S", 13, 3), ("S", 12, 3),
    ("E", 0, 0), ("E", 1, 0), ("E", 3, 0), ("E", 5, 0), ("E", 2, 0), ("E", 4, 0), ("E", 7, 0), ("E", 6, 0),
)


def split_bf16(values):
    high = values.astype(BF16)
    low = (values - high.astype(F32)).astype(BF16)
    return high, low


def dot3(left, right_high, right_low):
    high, low = split_bf16(left)
    dot = functools.partial(jnp.dot, preferred_element_type=F32)
    return dot(high, right_high) + (dot(high, right_low) + dot(low, right_high))


def fourier_tables(pixels, order_count, width):
    coarse = pixels // width
    k1, m1 = np.meshgrid(np.arange(coarse), np.arange(coarse), indexing="ij")
    angle = 2.0 * math.pi * ((k1 * m1) % coarse) / coarse
    first = np.concatenate([np.cos(angle.T), -np.sin(angle.T)], axis=0)
    k2 = np.arange(width)[:, None]
    m = np.arange(order_count)[None, :]
    angle = 2.0 * math.pi * ((k2 * m) % pixels) / pixels
    cosine, sine = np.cos(angle) / math.sqrt(pixels), np.sin(angle) / math.sqrt(pixels)
    second = np.block([[cosine, -sine], [sine, cosine]]).astype(np.float32)
    high = second.astype(BF16)
    low = (second - high.astype(np.float32)).astype(BF16)
    first = first.astype(np.float32)
    first_high = first.astype(BF16)
    first_low = (first - first_high.astype(np.float32)).astype(BF16)
    return np.stack([first_high, first_low]), high, low


def position():
    blk, grp = lax.axis_index("blk"), lax.axis_index("grp")
    x, y = blk // 16, (blk // 4) % 4
    z = grp * 2 + (blk // 2) % 2
    return x, y, z, blk % 2


def device_at(x, y, z, core):
    return ((x * 4 + y) * 2 + z % 2) * 2 + core, z // 2


def moved(chip, core, gen):
    axis, c = gen % 3, chip[gen % 3]
    other = jnp.where((gen // 3 + core) % 2 == 0, c + 1 - 2 * (c % 2), 3 - c)
    return chip[:axis] + (other,) + chip[axis + 1 :]


def row_flips():
    out = np.zeros((2, 2, BLOCKS // HALVES, HALVES, 2, 32, 2), np.int32)
    for core, half, t, h, part, low, j in np.ndindex(*out.shape):
        flips = [0, 0, 0]
        for k, gen in enumerate(ORDERS[HALVES * t + h]):
            if ((half * 32 + low) >> (5 - k)) & 1:
                flips[gen % 3] ^= 1 if (gen // 3 + core + part) % 2 == 0 else 3
        device = ((flips[0] * 4 + flips[1]) * 2 + flips[2] % 2) * 4 + part * 2 + flips[2] // 2
        out[core, half, t, h, part, low, j] = device * 4 + h * 2 + j
    return out.reshape(2, -1, 256)


def spectral_values(x_ref, first, high, low):
    maps, cycles, coarse, width = x_ref.shape
    rows = maps * cycles
    columns = high.shape[1]
    x_high, x_low = split_bf16(jnp.concatenate([x_ref[i // cycles, i % cycles] for i in range(rows)], axis=1))
    dot = functools.partial(jnp.dot, preferred_element_type=F32)
    stage = dot(first[0], x_high) + (dot(first[0], x_low) + dot(first[1], x_high))
    stages = []
    for i in range(rows):
        piece = stage[:, i * width : (i + 1) * width]
        stages.append(jnp.concatenate([piece[:coarse], piece[coarse:]], axis=1))
    full = dot3(jnp.concatenate(stages, axis=0), high, low)
    m1 = lax.broadcasted_iota(I32, (1, coarse, columns), 1)
    col = lax.broadcasted_iota(I32, (1, coarse, columns), 2)
    full = jnp.where((col % coarse) == m1, full.reshape(rows, coarse, columns), 0.0)
    return jnp.sum(full, axis=1).astype(BF16)


def main_body(
    maps,
    cycles,
    orders,
    legendre_ref,
    sky_ref,
    first_ref,
    high_ref,
    low_ref,
    flips_ref,
    table_ref,
    owner_ref,
    harm_ref,
    spectra_ref,
    leg,
    sky,
    first_buf,
    high_buf,
    low_buf,
    flips,
    table,
    harm,
    lines,
    coefs,
    hot,
    own,
    out_core,
    got,
    four,
    four_got,
    s1,
    r1,
    s2,
    r2,
    s3,
    r3,
    s4,
    r4,
    s5,
    r5,
    acc,
    power,
    power_got,
    column,
    column_got,
    leg_sem,
    in_sem,
    out_sem,
    core_send,
    core_recv,
    four_sem,
    step_send,
    step_recv,
    last_send,
    last_recv,
    power_sem,
    column_sem,
):
    x, y, z, core = position()
    chip = (x, y, z)
    place = x * 4 + y
    member = ((z % 2) * 2 + core) * 2 + z // 2
    members = 8
    columns = power.shape[0]
    channels = 2 * maps
    tiles = legendre_ref.shape[2] // LANES

    def leg_copy(t):
        return pltpu.make_async_copy(
            legendre_ref.at[:, :, pl.ds(pl.multiple_of(t * LANES, LANES), LANES)], leg.at[t], leg_sem.at[t]
        )

    coarse = sky.shape[2]
    small = [
        pltpu.make_async_copy(flips_ref.at[core], flips, in_sem.at[1]),
        pltpu.make_async_copy(table_ref, table, in_sem.at[2]),
    ]
    for load in small:
        load.start()

    def sky_copy(k, carry):
        lanes = pl.ds(pl.multiple_of(k * 128, 128), 128)
        pltpu.make_async_copy(sky_ref.at[:, :, lanes], sky.at[:, :, k, :], in_sem.at[0]).start()
        return carry

    loads = [
        pltpu.make_async_copy(src, dst, in_sem.at[i + 3])
        for i, (src, dst) in enumerate([(first_ref, first_buf), (high_ref, high_buf), (low_ref, low_buf)])
    ]
    lax.fori_loop(0, coarse, sky_copy, 0)
    for load in loads:
        load.start()
    loads.append(pltpu.make_async_copy(sky, sky, in_sem.at[0]))
    leg_copy(0).start()

    barrier = pltpu.get_barrier_semaphore()
    partner = device_at(x, y, z, 1 - core)
    across = [device_at(*moved(chip, core, g), core) for g in range(6)]
    near = [partner] + across
    for device in near:
        pl.semaphore_signal(barrier, inc=1, device_id=device, device_id_type=MESH)

    def remote(src, dst, send, recv, device):
        return pltpu.make_async_remote_copy(
            src_ref=src, dst_ref=dst, send_sem=send, recv_sem=recv, device_id=device, device_id_type=MESH
        )

    def core_copy(half, t):
        return remote(out_core.at[half, t], got.at[half, t], core_send, core_recv.at[half, t], partner)

    def make_hot(i):
        column = jnp.transpose(lines[i])[:, 0:1].astype(I32)
        lane = lax.broadcasted_iota(I32, (256, orders), 1)
        hot[i % 3] = jnp.where(column == lane, 1.0, 0.0).astype(BF16)

    def permute(i):
        half, t = 1 - i // tiles, i % tiles
        if half:
            leg_copy(t).wait()
        one_hot = hot[i % 3]
        for r in range(cycles):
            picked = jnp.dot(one_hot, leg[t, r], preferred_element_type=F32).astype(BF16)
            for h in range(HALVES):
                own[half, t, h, r] = picked[128 * h : 128 * h + 64]
                out_core[half, t, h, r] = picked[128 * h + 64 : 128 * (h + 1)]
        core_copy(half, t).start()

    base = ((place * 2 + z % 2) * 4 + core * 2 + z // 2) * 4
    for load in small:
        load.wait()
    digits = jnp.concatenate([table[...] >> 4, table[...] & 15], axis=0).astype(F32).astype(BF16)
    for i in range(2 * tiles):
        row = (1 - i // tiles) * tiles + i % tiles
        slot = flips[row : row + 1, :] ^ base
        spot = jnp.where(lax.broadcasted_iota(I32, (128, 256), 0) == (slot & 127), 1.0, 0.0).astype(BF16)
        found = jnp.dot(digits, spot, preferred_element_type=F32)
        found = found[0:4] * 16.0 + found[4:8]
        found = jnp.where(lax.broadcasted_iota(I32, (4, 256), 0) == (slot >> 7), found, 0.0)
        lines[i] = jnp.broadcast_to(jnp.sum(found, axis=0, keepdims=True), (8, 256))
    for i in range(2):
        make_hot(i)

    for load in loads:
        load.wait()
    for t in range(1, tiles):
        leg_copy(t).start()
    spectral = spectral_values(sky, first_buf, high_buf[...], low_buf[...])
    rows = maps * cycles
    out_row = lax.broadcasted_iota(I32, (cycles * channels, rows), 0)
    in_row = lax.broadcasted_iota(I32, (cycles * channels, rows), 1)
    value = jnp.zeros((cycles * channels, orders), F32)
    for q in range(2):
        wanted = (in_row % cycles) * channels + 2 * (in_row // cycles) + q
        pick = jnp.where(out_row == wanted, 1.0, 0.0).astype(BF16)
        value = value + jnp.dot(pick, spectral[:, q * orders : (q + 1) * orders], preferred_element_type=F32)
    four[...] = value.astype(BF16)
    pl.semaphore_wait(barrier, len(near))
    four_copy = remote(four, four_got, four_sem.at[0], four_sem.at[1], partner)
    four_copy.start()
    permute(0)

    def coefficients(i):
        every = jnp.concatenate([four[...], four_got[...]], axis=0)
        mine = jnp.concatenate([hot[i % 3, 128 * h : 128 * h + 64, :] for h in range(HALVES)], axis=0)
        coefs[i] = lax.dot_general(every, mine, (((1,), (1,)), ((), ())), preferred_element_type=F32)

    def partial(i, g):
        lane = lax.broadcasted_iota(I32, (channels, 128), 1) // 32
        sides = []
        for side in range(2):
            total = jnp.zeros((channels, 128), F32)
            for q in range(4):
                r = side * 4 + q
                piece = coefs[i, r * channels : (r + 1) * channels, :]
                shift = (32 * (q - g)) % 128
                piece = pltpu.roll(piece, shift, 1) if shift else piece
                total = jnp.where(lane == q, piece, total)
            sides.append(total)
        line = jnp.concatenate(sides, axis=1)
        wide = jnp.broadcast_to(line[None], (32, channels, 256)).reshape(256, 256)
        row = lax.broadcasted_iota(I32, (256, 256), 0) // channels
        col = lax.broadcasted_iota(I32, (256, 256), 1) % 32
        left = jnp.where(row == col, wide, 0.0).astype(BF16)
        at = slice(32 * (g % 2), 32 * (g % 2) + 32)
        right = jnp.concatenate(
            [ref[1 - i // tiles, i % tiles, g // 2, r, at, :] for ref in (own, got) for r in range(cycles)], axis=0
        )
        return jnp.dot(left, right, preferred_element_type=F32)

    senders, receivers = (s1, s2, s3, s4), (r1, r2, r3, r4)

    def step_copy(k, b):
        device = across[ORDERS[b][k]]
        return remote(senders[k].at[b], receivers[k].at[b], step_send.at[k], step_recv.at[k, b], device)

    four_copy.wait_recv()
    coefficients(0)

    def sums(i):
        half, t = 1 - i // tiles, i % tiles
        if i + 1 < 2 * tiles:
            permute(i + 1)
        core_copy(half, t).wait_recv()
        for g in range(4):
            b, at = HALVES * t + g // 2, slice((g % 2) * 256, (g % 2 + 1) * 256)
            value = partial(i, g)
            if half:
                s1[b, at] = value.astype(BF16)
            else:
                acc[b, at] = value
        if i + 1 < 2 * tiles:
            coefficients(i + 1)
        if i + 2 < 2 * tiles:
            make_hot(i + 2)
        if half:
            for h in range(HALVES):
                step_copy(0, HALVES * t + h).start()

    def last_copies(b):
        low, high = ORDERS[b][5], ORDERS[b][4]
        both = device_at(*moved(moved(chip, core, low), core, high), core)
        return [
            remote(s5.at[b, i], r5.at[b, i], last_send.at[i], last_recv.at[b, i], device)
            for i, device in enumerate([across[low], across[high], both])
        ]

    def reduce_step(k, b):
        step_copy(k, b).wait_recv()
        arrived = receivers[k]
        if k + 1 < STEPS:
            n = 256 >> k
            senders[k + 1][b] = (acc[b, n : 2 * n] + arrived[b, n : 2 * n].astype(F32)).astype(BF16)
            step_copy(k + 1, b).start()
        else:
            n = 16
            total = acc[b, n : 4 * n] + arrived[b, n : 4 * n].astype(F32)
            for i in range(3):
                s5[b, i] = total[n * i : n * (i + 1)].astype(BF16)
            for copy in last_copies(b):
                copy.start()
        acc[b, 0:n] = acc[b, 0:n] + arrived[b, 0:n].astype(F32)

    def power_copy(c):
        device = device_at(c // 4, c % 4, z, core)
        return remote(power.at[c], power_got.at[place], power_sem.at[0], power_sem.at[1], device)

    def column_copy(n):
        there = (n % 2) * 2 + n // 4
        device = device_at(x, y, there, (n // 2) % 2)
        return remote(column, column_got.at[member], column_sem.at[0], column_sem.at[1], device)

    def finish(t):
        lanes = slice(t * LANES, (t + 1) * LANES)
        ell = t * LANES + lax.broadcasted_iota(I32, (2 * channels, LANES), 1)
        total = [None] * maps
        for h in range(HALVES):
            b = HALVES * t + h
            for copy in last_copies(b):
                copy.wait_recv()
            value = acc[b, 0:16]
            for i in range(3):
                value = value + r5[b, i].astype(F32)
            pair = [owner_ref[base + 2 * h + s] for s in range(2)]
            order = jnp.where(lax.broadcasted_iota(I32, (2 * channels, 1), 0) < channels, pair[0], pair[1])
            value = jnp.where(ell >= order, value, 0.0)
            for s in range(2):
                for a in range(maps):
                    row = s * channels + 2 * a
                    harm[2 * h + s, a, :, lanes] = value[row : row + 2]
            weighted = jnp.where(order == 0, value, 2.0 * value)
            for s in range(2):
                mode = value[s * channels : (s + 1) * channels]
                heavy = weighted[s * channels : (s + 1) * channels]
                for k in range(maps // 2 + 1):
                    turned = mode if k == 0 else jnp.concatenate([mode[2 * k :], mode[: 2 * k]], axis=0)
                    term = heavy * turned
                    total[k] = term if total[k] is None else total[k] + term
        rows = []
        for i in range(maps):
            for j in range(i, maps):
                k, a = (j - i, i) if j - i <= maps // 2 else (maps - (j - i), j)
                rows.append(total[k][2 * a : 2 * a + 1] + total[k][2 * a + 1 : 2 * a + 2])
        rows.append(jnp.zeros((power.shape[1] - len(rows), LANES), F32))
        block = jnp.concatenate(rows, axis=0)
        for half in range(LANES // 128):
            c = (LANES // 128) * t + half
            power[c] = block[:, 128 * half : 128 * (half + 1)]

            @pl.when(c != place)
            def _():
                power_copy(c).start()

    for kind, which, k in PROGRAM:
        if kind == "F":
            sums(which)
        elif kind == "K":
            sums(tiles + which)
        elif kind == "S":
            reduce_step(k, which)
        else:
            finish(which)
    harm_copy = pltpu.make_async_copy(harm, harm_ref, out_sem.at[0])
    harm_copy.start()

    others = columns - 1
    remote(
        power.at[0:others], power_got.at[0:others], power_sem.at[0], power_sem.at[1], partner
    ).wait_recv()
    power_got[place] = power[place]
    total = power_got[0]
    for c in range(1, columns):
        total = total + power_got[c]
    column[...] = total
    for n in range(members):

        @pl.when(n != member)
        def _():
            column_copy(n).start()

    others = members - 1
    whole = remote(
        column_got.at[0:others], column_got.at[0:others], column_sem.at[0], column_sem.at[1], partner
    )
    whole.wait_recv()
    column_got[member] = column[...]
    total = column_got[0]
    for n in range(1, members):
        total = total + column_got[n]
    share = spectra_ref.shape[1]
    ell = place * 128 + lax.broadcasted_iota(I32, total.shape, 1)
    total = total / (2 * ell + 1).astype(F32)
    total = pltpu.roll(total, (128 - share * member) % 128, 1)
    spectra_ref[...] = total[: spectra_ref.shape[0], :share]

    harm_copy.wait()
    whole.wait_send()
    others = columns - 1
    remote(
        power.at[0:others], power_got.at[0:others], power_sem.at[0], power_sem.at[1], partner
    ).wait_send()
    remote(out_core, got, core_send, core_recv.at[0, 0], partner).wait_send()
    four_copy.wait_send()
    for k in range(STEPS):
        remote(senders[k], receivers[k], step_send.at[k], step_recv.at[k, 0], partner).wait_send()
    for i in range(3):
        remote(s5.at[:, i], r5.at[:, i], last_send.at[i], last_recv.at[0, i], partner).wait_send()


def main_call(devices, sky_maps, legendre, owner_table):
    maps, cycles, pixels = sky_maps.shape
    _, orders, ells = legendre.shape
    width = 128
    coarse = pixels // width
    channels = 2 * maps
    tiles = ells // LANES
    pairs = maps * (maps + 1) // 2
    first, high, low = fourier_tables(pixels, orders, width)
    hbm = pl.BlockSpec(memory_space=pl.ANY)
    vmem = pl.BlockSpec(memory_space=pltpu.VMEM)

    def steps(rows_of):
        return [pltpu.VMEM((BLOCKS, n, LANES), BF16) for n in rows_of for _ in range(2)]

    return pl.pallas_call(
        functools.partial(main_body, maps, cycles, orders),
        out_shape=[
            jax.ShapeDtypeStruct((4, maps, 2, ells), F32),
            jax.ShapeDtypeStruct((pairs, ells // devices), F32),
        ],
        in_specs=[hbm] * 7 + [pl.BlockSpec(memory_space=pltpu.SMEM)],
        out_specs=[hbm, vmem],
        scratch_shapes=[
            pltpu.VMEM((tiles, cycles, orders, LANES), BF16),
            pltpu.VMEM((maps, cycles, coarse, width), F32),
            pltpu.VMEM(first.shape, BF16),
            pltpu.VMEM(high.shape, BF16),
            pltpu.VMEM(low.shape, BF16),
            pltpu.VMEM((2 * tiles, 256), I32),
            pltpu.VMEM((4, 128), I32),
            pltpu.VMEM((4, maps, 2, ells), F32),
            pltpu.VMEM((2 * tiles, 8, 256), F32),
            pltpu.VMEM((2 * tiles, 2 * cycles * channels, 128), F32),
            pltpu.VMEM((3, 256, orders), BF16),
            pltpu.VMEM((2, tiles, HALVES, cycles, 64, LANES), BF16),
            pltpu.VMEM((2, tiles, HALVES, cycles, 64, LANES), BF16),
            pltpu.VMEM((2, tiles, HALVES, cycles, 64, LANES), BF16),
            pltpu.VMEM((cycles * channels, orders), BF16),
            pltpu.VMEM((cycles * channels, orders), BF16),
            *steps((512, 256, 128, 64)),
            pltpu.VMEM((BLOCKS, 3, 16, LANES), BF16),
            pltpu.VMEM((BLOCKS, 3, 16, LANES), BF16),
            pltpu.VMEM((BLOCKS, 512, LANES), F32),
            pltpu.VMEM((ells // 128, 16, 128), F32),
            pltpu.VMEM((ells // 128, 16, 128), F32),
            pltpu.VMEM((16, 128), F32),
            pltpu.VMEM((8, 16, 128), F32),
            pltpu.SemaphoreType.DMA((tiles,)),
            pltpu.SemaphoreType.DMA((6,)),
            pltpu.SemaphoreType.DMA((1,)),
            pltpu.SemaphoreType.DMA,
            pltpu.SemaphoreType.DMA((2, tiles)),
            pltpu.SemaphoreType.DMA((2,)),
            pltpu.SemaphoreType.DMA((STEPS,)),
            pltpu.SemaphoreType.DMA((STEPS, BLOCKS)),
            pltpu.SemaphoreType.DMA((3,)),
            pltpu.SemaphoreType.DMA((BLOCKS, 3)),
            pltpu.SemaphoreType.DMA((2,)),
            pltpu.SemaphoreType.DMA((2,)),
        ],
        compiler_params=pltpu.CompilerParams(
            collective_id=0, has_side_effects=True, vmem_limit_bytes=58 * MIB
        ),
        cost_estimate=pl.CostEstimate(flops=10_000_000_000, bytes_accessed=16 * MIB, transcendentals=0),
    )(
        legendre,
        sky_maps,
        jnp.asarray(first),
        jnp.asarray(high),
        jnp.asarray(low),
        jnp.asarray(row_flips()),
        owner_table.reshape(4, 128),
        owner_table,
    )


def per_device(sky_maps, legendre, owner_table):
    devices = lax.axis_size(AXES)
    harmonics, spectra = main_call(devices, sky_maps, legendre, owner_table)
    return (harmonics, spectra)


def solution(mesh):
    return jax.shard_map(
        per_device,
        mesh=mesh,
        in_specs=(P(None, AXES, None), P(AXES, None, None), P()),
        out_specs=(P(AXES, None, None, None), P(None, AXES)),
        check_vma=False,
    )
```

```python
import functools
import math

import jax
import jax.numpy as jnp
import numpy as np
from jax import lax
from jax.experimental import pallas as pl
from jax.experimental.pallas import tpu as pltpu
from jax.sharding import PartitionSpec as P

AXES = ("blk", "grp")
MESH = pl.DeviceIdType.MESH
MIB = 1024 * 1024
F32, BF16, I32 = jnp.float32, jnp.bfloat16, jnp.int32

LANES = 256
HALVES = 2
BLOCKS = 16
STEPS = 4
ORDERS = (
    (5, 4, 1, 2, 3, 0), (0, 1, 3, 5, 4, 2), (5, 0, 3, 1, 4, 2), (1, 3, 5, 0, 2, 4),
    (0, 4, 2, 3, 1, 5), (3, 1, 2, 4, 0, 5), (1, 0, 3, 2, 4, 5), (4, 2, 5, 3, 1, 0),
    (1, 4, 5, 0, 2, 3), (2, 5, 1, 0, 4, 3), (3, 5, 1, 2, 0, 4), (5, 2, 0, 3, 4, 1),
    (2, 3, 1, 0, 4, 5), (3, 2, 5, 1, 0, 4), (0, 2, 1, 3, 4, 5), (4, 1, 3, 2, 5, 0),
)

PROGRAM = (
    ("F", 0, 0), ("F", 1, 0), ("F", 2, 0), ("F", 3, 0), ("F", 4, 0), ("F", 5, 0), ("F", 6, 0), ("F", 7, 0),
    ("K", 0, 0), ("S", 0, 0), ("S", 1, 0), ("K", 1, 0), ("S", 3, 0), ("K", 2, 0), ("K", 3, 0), ("S", 5, 0),
    ("S", 2, 0), ("K", 4, 0), ("S", 7, 0), ("K", 5, 0), ("S", 4, 0), ("S", 9, 0), ("K", 6, 0), ("S", 6, 0),
    ("K", 7, 0), ("S", 10, 0), ("S", 11, 0), ("S", 15, 0), ("S", 12, 0), ("S", 14, 0), ("S", 8, 0), ("S", 9, 1),
    ("S", 0, 1), ("S", 7, 1), ("S", 2, 1), ("S", 13, 0), ("S", 1, 1), ("S", 10, 1), ("S", 4, 1), ("S", 11, 1),
    ("S", 6, 1), ("S", 3, 1), ("S", 7, 2), ("S", 5, 1), ("S", 14, 1), ("S", 8, 1), ("S", 12, 1), ("S", 13, 1),
    ("S", 15, 1), ("S", 11, 2), ("S", 2, 2), ("S", 9, 2), ("S", 4, 2), ("S", 1, 2), ("S", 0, 2), ("S", 3, 2),
    ("S", 6, 2), ("S", 10, 2), ("S", 5, 2), ("S", 7, 3), ("S", 8, 2), ("S", 14, 2), ("S", 15, 2), ("S", 13, 2),
    ("S", 12, 2), ("S", 2, 3), ("S", 9, 3), ("S", 11, 3), ("S", 1, 3), ("S", 4, 3), ("S", 0, 3), ("S", 3, 3),
    ("S", 6, 3), ("S", 10, 3), ("S", 5, 3), ("S", 8, 3), ("S", 14, 3), ("S", 15, 3), ("S", 13, 3), ("S", 12, 3),
    ("E", 0, 0), ("E", 1, 0), ("E", 3, 0), ("E", 5, 0), ("E", 2, 0), ("E", 4, 0), ("E", 7, 0), ("E", 6, 0),
)


def split_bf16(values):
    high = values.astype(BF16)
    low = (values - high.astype(F32)).astype(BF16)
    return high, low


def dot3(left, right_high, right_low):
    high, low = split_bf16(left)
    dot = functools.partial(jnp.dot, preferred_element_type=F32)
    return dot(high, right_high) + (dot(high, right_low) + dot(low, right_high))


def tables(pixels, order_count, width):
    coarse = pixels // width
    k1, m1 = np.meshgrid(np.arange(coarse), np.arange(coarse), indexing="ij")
    angle = 2.0 * math.pi * ((k1 * m1) % coarse) / coarse
    first = np.concatenate([np.cos(angle.T), -np.sin(angle.T)], axis=0)
    k2 = np.arange(width)[:, None]
    m = np.arange(order_count)[None, :]
    angle = 2.0 * math.pi * ((k2 * m) % pixels) / pixels
    cosine, sine = np.cos(angle) / math.sqrt(pixels), np.sin(angle) / math.sqrt(pixels)
    second = np.block([[cosine, -sine], [sine, cosine]])
    out = np.zeros((second.shape[0] + first.shape[0], second.shape[1]), np.float32)
    out[: second.shape[0]] = second
    out[second.shape[0] :, :coarse] = first
    flips = row_flips()
    for core in range(2):
        out[second.shape[0] : second.shape[0] + flips.shape[1], 256 * (core + 1) : 256 * (core + 2)] = flips[core]
    return out


def position():
    blk, grp = lax.axis_index("blk"), lax.axis_index("grp")
    x, y = blk // 16, (blk // 4) % 4
    z = grp * 2 + (blk // 2) % 2
    return x, y, z, blk % 2


def device_at(x, y, z, core):
    return ((x * 4 + y) * 2 + z % 2) * 2 + core, z // 2


def moved(chip, core, gen):
    axis, c = gen % 3, chip[gen % 3]
    other = jnp.where((gen // 3 + core) % 2 == 0, c + 1 - 2 * (c % 2), 3 - c)
    return chip[:axis] + (other,) + chip[axis + 1 :]


def row_flips():
    out = np.zeros((2, 2, BLOCKS // HALVES, HALVES, 2, 32, 2), np.int32)
    for core, half, t, h, part, low, j in np.ndindex(*out.shape):
        flips = [0, 0, 0]
        for k, gen in enumerate(ORDERS[HALVES * t + h]):
            if ((half * 32 + low) >> (5 - k)) & 1:
                flips[gen % 3] ^= 1 if (gen // 3 + core + part) % 2 == 0 else 3
        device = ((flips[0] * 4 + flips[1]) * 2 + flips[2] % 2) * 4 + part * 2 + flips[2] // 2
        out[core, half, t, h, part, low, j] = device * 4 + h * 2 + j
    return out.reshape(2, -1, 256)


def spectral_values(x_ref, first, second):
    maps, cycles, coarse, width = x_ref.shape
    rows = maps * cycles
    columns = second.shape[1]
    spread = jnp.concatenate([x_ref[i // cycles, i % cycles] for i in range(rows)], axis=1)
    stage = dot3(first[:, :coarse], *split_bf16(spread))
    stages = []
    for i in range(rows):
        piece = stage[:, i * width : (i + 1) * width]
        stages.append(jnp.concatenate([piece[:coarse], piece[coarse:]], axis=1))
    full = dot3(jnp.concatenate(stages, axis=0), *split_bf16(second))
    m1 = lax.broadcasted_iota(I32, (1, coarse, columns), 1)
    col = lax.broadcasted_iota(I32, (1, coarse, columns), 2)
    full = jnp.where((col % coarse) == m1, full.reshape(rows, coarse, columns), 0.0)
    return jnp.sum(full, axis=1).astype(BF16)


def main_body(
    maps,
    cycles,
    orders,
    legendre_ref,
    sky_ref,
    tables_ref,
    table_ref,
    owner_ref,
    harm_ref,
    spectra_ref,
    leg,
    sky,
    second_buf,
    first_buf,
    flips,
    table,
    owner,
    lines,
    coefs,
    hot,
    own,
    out_core,
    got,
    four,
    four_got,
    s1,
    r1,
    s2,
    r2,
    s3,
    r3,
    s4,
    r4,
    s5,
    r5,
    acc,
    power,
    power_got,
    column,
    column_got,
    leg_sem,
    in_sem,
    core_send,
    core_recv,
    four_sem,
    step_send,
    step_recv,
    last_send,
    last_recv,
    power_sem,
    column_sem,
):
    x, y, z, core = position()
    chip = (x, y, z)
    place = x * 4 + y
    member = ((z % 2) * 2 + core) * 2 + z // 2
    members = 8
    columns = power.shape[0]
    channels = 2 * maps
    tiles = legendre_ref.shape[2] // LANES

    def leg_copy(t):
        return pltpu.make_async_copy(
            legendre_ref.at[:, :, pl.ds(pl.multiple_of(t * LANES, LANES), LANES)], leg.at[t], leg_sem.at[t]
        )

    coarse = sky.shape[2]
    depth = second_buf.shape[0]
    mine = pl.ds(pl.multiple_of(256 * (core + 1), 256), 256)
    small = [
        pltpu.make_async_copy(tables_ref.at[pl.ds(depth, 2 * tiles), mine], flips, in_sem.at[1]),
        pltpu.make_async_copy(table_ref, table, in_sem.at[2]),
    ]
    loads = [
        pltpu.make_async_copy(tables_ref.at[pl.ds(0, depth)], second_buf, in_sem.at[3]),
        pltpu.make_async_copy(tables_ref.at[pl.ds(depth, first_buf.shape[0]), pl.ds(0, 128)], first_buf, in_sem.at[4]),
        pltpu.make_async_copy(owner_ref, owner, in_sem.at[5]),
    ]
    for load in small:
        load.start()
    leg_copy(0).start()

    def sky_copy(k, carry):
        lanes = pl.ds(pl.multiple_of(k * 128, 128), 128)
        pltpu.make_async_copy(sky_ref.at[:, :, lanes], sky.at[:, :, k, :], in_sem.at[0]).start()
        return carry

    lax.fori_loop(0, coarse, sky_copy, 0)
    for load in loads:
        load.start()
    loads.append(pltpu.make_async_copy(sky, sky, in_sem.at[0]))

    barrier = pltpu.get_barrier_semaphore()
    partner = device_at(x, y, z, 1 - core)
    across = [device_at(*moved(chip, core, g), core) for g in range(6)]
    near = [partner] + across
    for device in near:
        pl.semaphore_signal(barrier, inc=1, device_id=device, device_id_type=MESH)

    def remote(src, dst, send, recv, device):
        return pltpu.make_async_remote_copy(
            src_ref=src, dst_ref=dst, send_sem=send, recv_sem=recv, device_id=device, device_id_type=MESH
        )

    def core_copy(half, t):
        return remote(out_core.at[half, t], got.at[half, t], core_send, core_recv.at[half, t], partner)

    def make_hot(i):
        column = jnp.transpose(lines[i])[:, 0:1].astype(I32)
        lane = lax.broadcasted_iota(I32, (256, orders), 1)
        hot[i % 3] = jnp.where(column == lane, 1.0, 0.0).astype(BF16)

    def permute(i):
        half, t = 1 - i // tiles, i % tiles
        if half:
            leg_copy(t).wait()
        one_hot = hot[i % 3]
        for r in range(cycles):
            picked = jnp.dot(one_hot, leg[t, r], preferred_element_type=F32).astype(BF16)
            for h in range(HALVES):
                own[half, t, h, r] = picked[128 * h : 128 * h + 64]
                out_core[half, t, h, r] = picked[128 * h + 64 : 128 * (h + 1)]
        core_copy(half, t).start()

    base = ((place * 2 + z % 2) * 4 + core * 2 + z // 2) * 4
    for load in small:
        load.wait()
    digits = jnp.concatenate([table[...] >> 4, table[...] & 15], axis=0).astype(F32).astype(BF16)
    for i in range(2 * tiles):
        row = (1 - i // tiles) * tiles + i % tiles
        slot = flips[row : row + 1, :].astype(I32) ^ base
        spot = jnp.where(lax.broadcasted_iota(I32, (128, 256), 0) == (slot & 127), 1.0, 0.0).astype(BF16)
        found = jnp.dot(digits, spot, preferred_element_type=F32)
        found = found[0:4] * 16.0 + found[4:8]
        found = jnp.where(lax.broadcasted_iota(I32, (4, 256), 0) == (slot >> 7), found, 0.0)
        lines[i] = jnp.broadcast_to(jnp.sum(found, axis=0, keepdims=True), (8, 256))
    for i in range(2):
        make_hot(i)

    pl.semaphore_wait(barrier, len(near))
    permute(0)
    for load in loads:
        load.wait()
    for t in range(1, tiles):
        leg_copy(t).start()
    spectral = spectral_values(sky, first_buf[...], second_buf[...])
    rows = maps * cycles
    out_row = lax.broadcasted_iota(I32, (cycles * channels, rows), 0)
    in_row = lax.broadcasted_iota(I32, (cycles * channels, rows), 1)
    value = jnp.zeros((cycles * channels, orders), F32)
    for q in range(2):
        wanted = (in_row % cycles) * channels + 2 * (in_row // cycles) + q
        pick = jnp.where(out_row == wanted, 1.0, 0.0).astype(BF16)
        value = value + jnp.dot(pick, spectral[:, q * orders : (q + 1) * orders], preferred_element_type=F32)
    four[...] = value.astype(BF16)
    four_copy = remote(four, four_got, four_sem.at[0], four_sem.at[1], partner)
    four_copy.start()

    def coefficients(i):
        every = jnp.concatenate([four[...], four_got[...]], axis=0)
        mine = jnp.concatenate([hot[i % 3, 128 * h : 128 * h + 64, :] for h in range(HALVES)], axis=0)
        coefs[i] = lax.dot_general(every, mine, (((1,), (1,)), ((), ())), preferred_element_type=F32)

    def partial(i, g):
        lane = lax.broadcasted_iota(I32, (channels, 128), 1) // 32
        sides = []
        for side in range(2):
            total = jnp.zeros((channels, 128), F32)
            for q in range(4):
                r = side * 4 + q
                piece = coefs[i, r * channels : (r + 1) * channels, :]
                shift = (32 * (q - g)) % 128
                piece = pltpu.roll(piece, shift, 1) if shift else piece
                total = jnp.where(lane == q, piece, total)
            sides.append(total)
        line = jnp.concatenate(sides, axis=1)
        wide = jnp.broadcast_to(line[None], (32, channels, 256)).reshape(256, 256)
        row = lax.broadcasted_iota(I32, (256, 256), 0) // channels
        col = lax.broadcasted_iota(I32, (256, 256), 1) % 32
        left = jnp.where(row == col, wide, 0.0).astype(BF16)
        at = slice(32 * (g % 2), 32 * (g % 2) + 32)
        right = jnp.concatenate(
            [ref[1 - i // tiles, i % tiles, g // 2, r, at, :] for ref in (own, got) for r in range(cycles)], axis=0
        )
        return jnp.dot(left, right, preferred_element_type=F32)

    senders, receivers = (s1, s2, s3, s4), (r1, r2, r3, r4)

    def step_copy(k, b):
        device = across[ORDERS[b][k]]
        return remote(senders[k].at[b], receivers[k].at[b], step_send.at[k], step_recv.at[k, b], device)

    def sums(i):
        half, t = 1 - i // tiles, i % tiles
        if i + 1 < 2 * tiles:
            permute(i + 1)
        if i == 0:
            four_copy.wait_recv()
            coefficients(0)
        core_copy(half, t).wait_recv()
        for g in range(4):
            b, at = HALVES * t + g // 2, slice((g % 2) * 256, (g % 2 + 1) * 256)
            value = partial(i, g)
            if half:
                s1[b, at] = value.astype(BF16)
            else:
                acc[b, at] = value
        if i + 1 < 2 * tiles:
            coefficients(i + 1)
        if i + 2 < 2 * tiles:
            make_hot(i + 2)
        if half:
            for h in range(HALVES):
                step_copy(0, HALVES * t + h).start()

    def last_copies(b):
        low, high = ORDERS[b][5], ORDERS[b][4]
        both = device_at(*moved(moved(chip, core, low), core, high), core)
        return [
            remote(s5.at[b, i], r5.at[b, i], last_send.at[i], last_recv.at[b, i], device)
            for i, device in enumerate([across[low], across[high], both])
        ]

    def reduce_step(k, b):
        step_copy(k, b).wait_recv()
        arrived = receivers[k]
        if k + 1 < STEPS:
            n = 256 >> k
            senders[k + 1][b] = (acc[b, n : 2 * n] + arrived[b, n : 2 * n].astype(F32)).astype(BF16)
            step_copy(k + 1, b).start()
        else:
            n = 16
            total = acc[b, n : 4 * n] + arrived[b, n : 4 * n].astype(F32)
            for i in range(3):
                s5[b, i] = total[n * i : n * (i + 1)].astype(BF16)
            for copy in last_copies(b):
                copy.start()
        acc[b, 0:n] = acc[b, 0:n] + arrived[b, 0:n].astype(F32)

    def power_copy(c):
        device = device_at(c // 4, c % 4, z, core)
        return remote(power.at[c], power_got.at[place], power_sem.at[0], power_sem.at[1], device)

    def column_copy(n):
        there = (n % 2) * 2 + n // 4
        device = device_at(x, y, there, (n // 2) % 2)
        return remote(column, column_got.at[member], column_sem.at[0], column_sem.at[1], device)

    def finish(t):
        lanes = slice(t * LANES, (t + 1) * LANES)
        ell = t * LANES + lax.broadcasted_iota(I32, (2 * channels, LANES), 1)
        total = [None] * maps
        for h in range(HALVES):
            b = HALVES * t + h
            for copy in last_copies(b):
                copy.wait_recv()
            value = acc[b, 0:16]
            for i in range(3):
                value = value + r5[b, i].astype(F32)
            pair = [owner[base + 2 * h + s] for s in range(2)]
            order = jnp.where(lax.broadcasted_iota(I32, (2 * channels, 1), 0) < channels, pair[0], pair[1])
            value = jnp.where(ell >= order, value, 0.0)
            for s in range(2):
                for a in range(maps):
                    row = s * channels + 2 * a
                    harm_ref[2 * h + s, a, :, lanes] = value[row : row + 2]
            weighted = jnp.where(order == 0, value, 2.0 * value)
            for s in range(2):
                mode = value[s * channels : (s + 1) * channels]
                heavy = weighted[s * channels : (s + 1) * channels]
                for k in range(maps // 2 + 1):
                    turned = mode if k == 0 else jnp.concatenate([mode[2 * k :], mode[: 2 * k]], axis=0)
                    term = heavy * turned
                    total[k] = term if total[k] is None else total[k] + term
        rows = []
        for i in range(maps):
            for j in range(i, maps):
                k, a = (j - i, i) if j - i <= maps // 2 else (maps - (j - i), j)
                rows.append(total[k][2 * a : 2 * a + 1] + total[k][2 * a + 1 : 2 * a + 2])
        rows.append(jnp.zeros((power.shape[1] - len(rows), LANES), F32))
        block = jnp.concatenate(rows, axis=0)
        for half in range(LANES // 128):
            c = (LANES // 128) * t + half
            power[c] = block[:, 128 * half : 128 * (half + 1)]

            @pl.when(c != place)
            def _():
                power_copy(c).start()

    for kind, which, k in PROGRAM:
        if kind == "F":
            sums(which)
        elif kind == "K":
            sums(tiles + which)
        elif kind == "S":
            reduce_step(k, which)
        else:
            finish(which)

    others = columns - 1
    remote(
        power.at[0:others], power_got.at[0:others], power_sem.at[0], power_sem.at[1], partner
    ).wait_recv()
    power_got[place] = power[place]
    total = power_got[0]
    for c in range(1, columns):
        total = total + power_got[c]
    column[...] = total
    for n in range(members):

        @pl.when(n != member)
        def _():
            column_copy(n).start()

    others = members - 1
    whole = remote(
        column_got.at[0:others], column_got.at[0:others], column_sem.at[0], column_sem.at[1], partner
    )
    whole.wait_recv()
    column_got[member] = column[...]
    total = column_got[0]
    for n in range(1, members):
        total = total + column_got[n]
    share = spectra_ref.shape[1]
    ell = place * 128 + lax.broadcasted_iota(I32, total.shape, 1)
    total = total / (2 * ell + 1).astype(F32)
    total = pltpu.roll(total, (128 - share * member) % 128, 1)
    spectra_ref[...] = total[: spectra_ref.shape[0], :share]

    whole.wait_send()
    others = columns - 1
    remote(
        power.at[0:others], power_got.at[0:others], power_sem.at[0], power_sem.at[1], partner
    ).wait_send()
    remote(out_core, got, core_send, core_recv.at[0, 0], partner).wait_send()
    four_copy.wait_send()
    for k in range(STEPS):
        remote(senders[k], receivers[k], step_send.at[k], step_recv.at[k, 0], partner).wait_send()
    for i in range(3):
        remote(s5.at[:, i], r5.at[:, i], last_send.at[i], last_recv.at[0, i], partner).wait_send()


def main_call(devices, sky_maps, legendre, owner_table):
    maps, cycles, pixels = sky_maps.shape
    _, orders, ells = legendre.shape
    width = 128
    coarse = pixels // width
    channels = 2 * maps
    tiles = ells // LANES
    pairs = maps * (maps + 1) // 2
    constants = tables(pixels, orders, width)
    hbm = pl.BlockSpec(memory_space=pltpu.HBM)
    vmem = pl.BlockSpec(memory_space=pltpu.VMEM)

    def steps(rows_of):
        return [pltpu.VMEM((BLOCKS, n, LANES), BF16) for n in rows_of for _ in range(2)]

    return pl.pallas_call(
        functools.partial(main_body, maps, cycles, orders),
        out_shape=[
            jax.ShapeDtypeStruct((4, maps, 2, ells), F32),
            jax.ShapeDtypeStruct((pairs, ells // devices), F32),
        ],
        in_specs=[hbm] * 5,
        out_specs=[vmem] * 2,
        scratch_shapes=[
            pltpu.VMEM((tiles, cycles, orders, LANES), BF16),
            pltpu.VMEM((maps, cycles, coarse, width), F32),
            pltpu.VMEM((2 * width, 2 * orders), F32),
            pltpu.VMEM((2 * coarse, 128), F32),
            pltpu.VMEM((2 * tiles, 256), F32),
            pltpu.VMEM((4, 128), I32),
            pltpu.SMEM((orders,), I32),
            pltpu.VMEM((2 * tiles, 8, 256), F32),
            pltpu.VMEM((2 * tiles, 2 * cycles * channels, 128), F32),
            pltpu.VMEM((3, 256, orders), BF16),
            pltpu.VMEM((2, tiles, HALVES, cycles, 64, LANES), BF16),
            pltpu.VMEM((2, tiles, HALVES, cycles, 64, LANES), BF16),
            pltpu.VMEM((2, tiles, HALVES, cycles, 64, LANES), BF16),
            pltpu.VMEM((cycles * channels, orders), BF16),
            pltpu.VMEM((cycles * channels, orders), BF16),
            *steps((512, 256, 128, 64)),
            pltpu.VMEM((BLOCKS, 3, 16, LANES), BF16),
            pltpu.VMEM((BLOCKS, 3, 16, LANES), BF16),
            pltpu.VMEM((BLOCKS, 512, LANES), F32),
            pltpu.VMEM((ells // 128, 16, 128), F32),
            pltpu.VMEM((ells // 128, 16, 128), F32),
            pltpu.VMEM((16, 128), F32),
            pltpu.VMEM((8, 16, 128), F32),
            pltpu.SemaphoreType.DMA((tiles,)),
            pltpu.SemaphoreType.DMA((6,)),
            pltpu.SemaphoreType.DMA,
            pltpu.SemaphoreType.DMA((2, tiles)),
            pltpu.SemaphoreType.DMA((2,)),
            pltpu.SemaphoreType.DMA((STEPS,)),
            pltpu.SemaphoreType.DMA((STEPS, BLOCKS)),
            pltpu.SemaphoreType.DMA((3,)),
            pltpu.SemaphoreType.DMA((BLOCKS, 3)),
            pltpu.SemaphoreType.DMA((2,)),
            pltpu.SemaphoreType.DMA((2,)),
        ],
        compiler_params=pltpu.CompilerParams(
            collective_id=0, has_side_effects=True, vmem_limit_bytes=int(53.55 * MIB)
        ),
        cost_estimate=pl.CostEstimate(flops=10_000_000_000, bytes_accessed=16 * MIB, transcendentals=0),
    )(
        legendre,
        sky_maps,
        jnp.asarray(constants),
        owner_table.reshape(4, 128),
        owner_table,
    )


def per_device(sky_maps, legendre, owner_table):
    devices = lax.axis_size(AXES)
    harmonics, spectra = main_call(devices, sky_maps, legendre, owner_table)
    return (harmonics, spectra)


def solution(mesh):
    return jax.shard_map(
        per_device,
        mesh=mesh,
        in_specs=(P(None, AXES, None), P(AXES, None, None), P()),
        out_specs=(P(AXES, None, None, None), P(None, AXES)),
        check_vma=False,
    )
```

```python
import functools
import math

import jax
import jax.numpy as jnp
import numpy as np
from jax import lax
from jax.experimental import pallas as pl
from jax.experimental.pallas import tpu as pltpu
from jax.sharding import PartitionSpec as P

AXES = ("blk", "grp")
MESH = pl.DeviceIdType.MESH
MIB = 1024 * 1024
F32, BF16, I32 = jnp.float32, jnp.bfloat16, jnp.int32

LANES = 256
HALVES = 2
BLOCKS = 16
STEPS = 4
ORDERS = (
    (5, 4, 1, 2, 3, 0), (0, 1, 3, 5, 4, 2), (5, 0, 3, 1, 4, 2), (1, 3, 5, 0, 2, 4),
    (0, 4, 2, 3, 1, 5), (3, 1, 2, 4, 0, 5), (1, 0, 3, 2, 4, 5), (4, 2, 5, 3, 1, 0),
    (1, 4, 5, 0, 2, 3), (2, 5, 1, 0, 4, 3), (3, 5, 1, 2, 0, 4), (5, 2, 0, 3, 4, 1),
    (2, 3, 1, 0, 4, 5), (3, 2, 5, 1, 0, 4), (0, 2, 1, 3, 4, 5), (4, 1, 3, 2, 5, 0),
)

PROGRAM = (
    ("F", 0, 0), ("F", 1, 0), ("F", 2, 0), ("F", 3, 0), ("F", 4, 0), ("F", 5, 0), ("F", 6, 0), ("F", 7, 0),
    ("K", 0, 0), ("S", 0, 0), ("S", 1, 0), ("K", 1, 0), ("S", 3, 0), ("K", 2, 0), ("K", 3, 0), ("S", 5, 0),
    ("S", 2, 0), ("K", 4, 0), ("S", 7, 0), ("K", 5, 0), ("S", 4, 0), ("S", 9, 0), ("K", 6, 0), ("S", 6, 0),
    ("K", 7, 0), ("S", 10, 0), ("S", 11, 0), ("S", 15, 0), ("S", 12, 0), ("S", 14, 0), ("S", 8, 0), ("S", 9, 1),
    ("S", 0, 1), ("S", 7, 1), ("S", 2, 1), ("S", 13, 0), ("S", 1, 1), ("S", 10, 1), ("S", 4, 1), ("S", 11, 1),
    ("S", 6, 1), ("S", 3, 1), ("S", 7, 2), ("S", 5, 1), ("S", 14, 1), ("S", 8, 1), ("S", 12, 1), ("S", 13, 1),
    ("S", 15, 1), ("S", 11, 2), ("S", 2, 2), ("S", 9, 2), ("S", 4, 2), ("S", 1, 2), ("S", 0, 2), ("S", 3, 2),
    ("S", 6, 2), ("S", 10, 2), ("S", 5, 2), ("S", 7, 3), ("S", 8, 2), ("S", 14, 2), ("S", 15, 2), ("S", 13, 2),
    ("S", 12, 2), ("S", 2, 3), ("S", 9, 3), ("S", 11, 3), ("S", 1, 3), ("S", 4, 3), ("S", 0, 3), ("S", 3, 3),
    ("S", 6, 3), ("S", 10, 3), ("S", 5, 3), ("S", 8, 3), ("S", 14, 3), ("S", 15, 3), ("S", 13, 3), ("S", 12, 3),
    ("E", 0, 0), ("E", 1, 0), ("E", 3, 0), ("E", 5, 0), ("E", 2, 0), ("E", 4, 0), ("E", 7, 0), ("E", 6, 0),
)


def split_bf16(values):
    high = values.astype(BF16)
    low = (values - high.astype(F32)).astype(BF16)
    return high, low


def dot3(left, right_high, right_low):
    high, low = split_bf16(left)
    dot = functools.partial(jnp.dot, preferred_element_type=F32)
    return dot(high, right_high) + (dot(high, right_low) + dot(low, right_high))


def tables(pixels, order_count, width):
    coarse = pixels // width
    k1, m1 = np.meshgrid(np.arange(coarse), np.arange(coarse), indexing="ij")
    angle = 2.0 * math.pi * ((k1 * m1) % coarse) / coarse
    first = np.concatenate([np.cos(angle.T), -np.sin(angle.T)], axis=0)
    k2 = np.arange(width)[:, None]
    m = np.arange(order_count)[None, :]
    angle = 2.0 * math.pi * ((k2 * m) % pixels) / pixels
    cosine, sine = np.cos(angle) / math.sqrt(pixels), np.sin(angle) / math.sqrt(pixels)
    second = np.block([[cosine, -sine], [sine, cosine]])
    out = np.zeros((second.shape[0] + first.shape[0], second.shape[1]), np.float32)
    out[: second.shape[0]] = second
    out[second.shape[0] :, :coarse] = first
    flips = row_flips()
    for core in range(2):
        out[second.shape[0] : second.shape[0] + flips.shape[1], 256 * (core + 1) : 256 * (core + 2)] = flips[core]
    return out


def position():
    blk, grp = lax.axis_index("blk"), lax.axis_index("grp")
    x, y = blk // 16, (blk // 4) % 4
    z = grp * 2 + (blk // 2) % 2
    return x, y, z, blk % 2


def device_at(x, y, z, core):
    return ((x * 4 + y) * 2 + z % 2) * 2 + core, z // 2


def moved(chip, core, gen):
    axis, c = gen % 3, chip[gen % 3]
    other = jnp.where((gen // 3 + core) % 2 == 0, c + 1 - 2 * (c % 2), 3 - c)
    return chip[:axis] + (other,) + chip[axis + 1 :]


def row_flips():
    out = np.zeros((2, 2, BLOCKS // HALVES, HALVES, 2, 32, 2), np.int32)
    for core, half, t, h, part, low, j in np.ndindex(*out.shape):
        flips = [0, 0, 0]
        for k, gen in enumerate(ORDERS[HALVES * t + h]):
            if ((half * 32 + low) >> (5 - k)) & 1:
                flips[gen % 3] ^= 1 if (gen // 3 + core + part) % 2 == 0 else 3
        device = ((flips[0] * 4 + flips[1]) * 2 + flips[2] % 2) * 4 + part * 2 + flips[2] // 2
        out[core, half, t, h, part, low, j] = device * 4 + h * 2 + j
    return out.reshape(2, -1, 256)


def spectral_values(x_ref, first, second):
    maps, cycles, coarse, width = x_ref.shape
    rows = maps * cycles
    columns = second.shape[1]
    spread = jnp.concatenate([x_ref[i // cycles, i % cycles] for i in range(rows)], axis=1)
    stage = dot3(first[:, :coarse], *split_bf16(spread))
    stages = []
    for i in range(rows):
        piece = stage[:, i * width : (i + 1) * width]
        stages.append(jnp.concatenate([piece[:coarse], piece[coarse:]], axis=1))
    full = dot3(jnp.concatenate(stages, axis=0), *split_bf16(second))
    m1 = lax.broadcasted_iota(I32, (1, coarse, columns), 1)
    col = lax.broadcasted_iota(I32, (1, coarse, columns), 2)
    full = jnp.where((col % coarse) == m1, full.reshape(rows, coarse, columns), 0.0)
    return jnp.sum(full, axis=1).astype(BF16)


def main_body(
    maps,
    cycles,
    orders,
    legendre_ref,
    sky_ref,
    tables_ref,
    table_ref,
    owner_ref,
    harm_ref,
    spectra_ref,
    leg,
    sky,
    second_buf,
    first_buf,
    flips,
    table,
    owner,
    lines,
    coefs,
    hot,
    own,
    out_core,
    got,
    four,
    four_got,
    s1,
    r1,
    s2,
    r2,
    s3,
    r3,
    s4,
    r4,
    s5,
    r5,
    acc,
    power,
    power_got,
    leg_sem,
    in_sem,
    core_send,
    core_recv,
    four_sem,
    step_send,
    step_recv,
    last_send,
    last_recv,
    power_sem,
):
    x, y, z, core = position()
    chip = (x, y, z)
    place = x * 4 + y
    member = ((z % 2) * 2 + core) * 2 + z // 2
    members = power.shape[1]
    me = place * members + member
    channels = 2 * maps
    tiles = legendre_ref.shape[2] // LANES

    def leg_copy(t):
        return pltpu.make_async_copy(
            legendre_ref.at[:, :, pl.ds(pl.multiple_of(t * LANES, LANES), LANES)], leg.at[t], leg_sem.at[t]
        )

    coarse = sky.shape[2]
    depth = second_buf.shape[0]
    mine = pl.ds(pl.multiple_of(256 * (core + 1), 256), 256)
    small = [
        pltpu.make_async_copy(tables_ref.at[pl.ds(depth, 2 * tiles), mine], flips, in_sem.at[1]),
        pltpu.make_async_copy(table_ref, table, in_sem.at[2]),
    ]
    loads = [
        pltpu.make_async_copy(tables_ref.at[pl.ds(0, depth)], second_buf, in_sem.at[3]),
        pltpu.make_async_copy(tables_ref.at[pl.ds(depth, first_buf.shape[0]), pl.ds(0, 128)], first_buf, in_sem.at[4]),
        pltpu.make_async_copy(owner_ref, owner, in_sem.at[5]),
    ]
    for load in small:
        load.start()
    leg_copy(0).start()

    def sky_copy(k, carry):
        lanes = pl.ds(pl.multiple_of(k * 128, 128), 128)
        pltpu.make_async_copy(sky_ref.at[:, :, lanes], sky.at[:, :, k, :], in_sem.at[0]).start()
        return carry

    lax.fori_loop(0, coarse, sky_copy, 0)
    for load in loads:
        load.start()
    loads.append(pltpu.make_async_copy(sky, sky, in_sem.at[0]))

    barrier = pltpu.get_barrier_semaphore()
    partner = device_at(x, y, z, 1 - core)
    across = [device_at(*moved(chip, core, g), core) for g in range(6)]
    near = [partner] + across
    for device in near:
        pl.semaphore_signal(barrier, inc=1, device_id=device, device_id_type=MESH)

    def remote(src, dst, send, recv, device):
        return pltpu.make_async_remote_copy(
            src_ref=src, dst_ref=dst, send_sem=send, recv_sem=recv, device_id=device, device_id_type=MESH
        )

    def core_copy(half, t):
        return remote(out_core.at[half, t], got.at[half, t], core_send, core_recv.at[half, t], partner)

    def make_hot(i):
        column = jnp.transpose(lines[i])[:, 0:1].astype(I32)
        lane = lax.broadcasted_iota(I32, (256, orders), 1)
        hot[i % 3] = jnp.where(column == lane, 1.0, 0.0).astype(BF16)

    def permute(i):
        half, t = 1 - i // tiles, i % tiles
        if half:
            leg_copy(t).wait()
        one_hot = hot[i % 3]
        for r in range(cycles):
            picked = jnp.dot(one_hot, leg[t, r], preferred_element_type=F32).astype(BF16)
            for h in range(HALVES):
                own[half, t, h, r] = picked[128 * h : 128 * h + 64]
                out_core[half, t, h, r] = picked[128 * h + 64 : 128 * (h + 1)]
        core_copy(half, t).start()

    base = ((place * 2 + z % 2) * 4 + core * 2 + z // 2) * 4
    for load in small:
        load.wait()
    digits = jnp.concatenate([table[...] >> 4, table[...] & 15], axis=0).astype(F32).astype(BF16)
    for i in range(2 * tiles):
        row = (1 - i // tiles) * tiles + i % tiles
        slot = flips[row : row + 1, :].astype(I32) ^ base
        spot = jnp.where(lax.broadcasted_iota(I32, (128, 256), 0) == (slot & 127), 1.0, 0.0).astype(BF16)
        found = jnp.dot(digits, spot, preferred_element_type=F32)
        found = found[0:4] * 16.0 + found[4:8]
        found = jnp.where(lax.broadcasted_iota(I32, (4, 256), 0) == (slot >> 7), found, 0.0)
        lines[i] = jnp.broadcast_to(jnp.sum(found, axis=0, keepdims=True), (8, 256))
    for i in range(2):
        make_hot(i)

    pl.semaphore_wait(barrier, len(near))
    permute(0)
    for load in loads:
        load.wait()
    for t in range(1, tiles):
        leg_copy(t).start()
    spectral = spectral_values(sky, first_buf[...], second_buf[...])
    rows = maps * cycles
    out_row = lax.broadcasted_iota(I32, (cycles * channels, rows), 0)
    in_row = lax.broadcasted_iota(I32, (cycles * channels, rows), 1)
    value = jnp.zeros((cycles * channels, orders), F32)
    for q in range(2):
        wanted = (in_row % cycles) * channels + 2 * (in_row // cycles) + q
        pick = jnp.where(out_row == wanted, 1.0, 0.0).astype(BF16)
        value = value + jnp.dot(pick, spectral[:, q * orders : (q + 1) * orders], preferred_element_type=F32)
    four[...] = value.astype(BF16)
    four_copy = remote(four, four_got, four_sem.at[0], four_sem.at[1], partner)
    four_copy.start()

    def coefficients(i):
        every = jnp.concatenate([four[...], four_got[...]], axis=0)
        mine = jnp.concatenate([hot[i % 3, 128 * h : 128 * h + 64, :] for h in range(HALVES)], axis=0)
        coefs[i] = lax.dot_general(every, mine, (((1,), (1,)), ((), ())), preferred_element_type=F32)

    def partial(i, g):
        lane = lax.broadcasted_iota(I32, (channels, 128), 1) // 32
        sides = []
        for side in range(2):
            total = jnp.zeros((channels, 128), F32)
            for q in range(4):
                r = side * 4 + q
                piece = coefs[i, r * channels : (r + 1) * channels, :]
                shift = (32 * (q - g)) % 128
                piece = pltpu.roll(piece, shift, 1) if shift else piece
                total = jnp.where(lane == q, piece, total)
            sides.append(total)
        line = jnp.concatenate(sides, axis=1)
        wide = jnp.broadcast_to(line[None], (32, channels, 256)).reshape(256, 256)
        row = lax.broadcasted_iota(I32, (256, 256), 0) // channels
        col = lax.broadcasted_iota(I32, (256, 256), 1) % 32
        left = jnp.where(row == col, wide, 0.0).astype(BF16)
        at = slice(32 * (g % 2), 32 * (g % 2) + 32)
        right = jnp.concatenate(
            [ref[1 - i // tiles, i % tiles, g // 2, r, at, :] for ref in (own, got) for r in range(cycles)], axis=0
        )
        return jnp.dot(left, right, preferred_element_type=F32)

    senders, receivers = (s1, s2, s3, s4), (r1, r2, r3, r4)

    def step_copy(k, b):
        device = across[ORDERS[b][k]]
        return remote(senders[k].at[b], receivers[k].at[b], step_send.at[k], step_recv.at[k, b], device)

    def sums(i):
        half, t = 1 - i // tiles, i % tiles
        if i + 1 < 2 * tiles:
            permute(i + 1)
        if i == 0:
            four_copy.wait_recv()
            coefficients(0)
        core_copy(half, t).wait_recv()
        for g in range(4):
            b, at = HALVES * t + g // 2, slice((g % 2) * 256, (g % 2 + 1) * 256)
            value = partial(i, g)
            if half:
                s1[b, at] = value.astype(BF16)
            else:
                acc[b, at] = value
        if i + 1 < 2 * tiles:
            coefficients(i + 1)
        if i + 2 < 2 * tiles:
            make_hot(i + 2)
        if half:
            for h in range(HALVES):
                step_copy(0, HALVES * t + h).start()

    def last_copies(b):
        low, high = ORDERS[b][5], ORDERS[b][4]
        both = device_at(*moved(moved(chip, core, low), core, high), core)
        return [
            remote(s5.at[b, i], r5.at[b, i], last_send.at[i], last_recv.at[b], device)
            for i, device in enumerate([across[low], across[high], both])
        ]

    def reduce_step(k, b):
        step_copy(k, b).wait_recv()
        arrived = receivers[k]
        if k + 1 < STEPS:
            n = 256 >> k
            senders[k + 1][b] = (acc[b, n : 2 * n] + arrived[b, n : 2 * n].astype(F32)).astype(BF16)
            step_copy(k + 1, b).start()
        else:
            n = 16
            total = acc[b, n : 4 * n] + arrived[b, n : 4 * n].astype(F32)
            for i in range(3):
                s5[b, i] = total[n * i : n * (i + 1)].astype(BF16)
            for copy in last_copies(b):
                copy.start()
        acc[b, 0:n] = acc[b, 0:n] + arrived[b, 0:n].astype(F32)

    def power_copy(c, m):
        there = device_at(c // 4, c % 4, (m % 2) * 2 + m // 4, (m // 2) % 2)
        self = me == c * members + m
        device = tuple(jnp.where(self, other, value) for value, other in zip(there, partner))
        row = jnp.where(self, power_got.shape[0] - 1, me)
        return remote(power.at[c, m], power_got.at[row], power_sem.at[0], power_sem.at[1], device)

    share = spectra_ref.shape[1]

    def finish(t):
        lanes = slice(t * LANES, (t + 1) * LANES)
        ell = t * LANES + lax.broadcasted_iota(I32, (2 * channels, LANES), 1)
        total = [None] * maps
        for h in range(HALVES):
            b = HALVES * t + h
            remote(s5.at[b], r5.at[b], last_send.at[0], last_recv.at[b], partner).wait_recv()
            value = acc[b, 0:16]
            for i in range(3):
                value = value + r5[b, i].astype(F32)
            pair = [owner[base + 2 * h + s] for s in range(2)]
            order = jnp.where(lax.broadcasted_iota(I32, (2 * channels, 1), 0) < channels, pair[0], pair[1])
            value = jnp.where(ell >= order, value, 0.0)
            for s in range(2):
                for a in range(maps):
                    row = s * channels + 2 * a
                    harm_ref[2 * h + s, a, :, lanes] = value[row : row + 2]
            weighted = jnp.where(order == 0, value, 2.0 * value)
            for s in range(2):
                mode = value[s * channels : (s + 1) * channels]
                heavy = weighted[s * channels : (s + 1) * channels]
                for k in range(maps // 2 + 1):
                    turned = mode if k == 0 else jnp.concatenate([mode[2 * k :], mode[: 2 * k]], axis=0)
                    term = heavy * turned
                    total[k] = term if total[k] is None else total[k] + term
        rows = []
        for i in range(maps):
            for j in range(i, maps):
                k, a = (j - i, i) if j - i <= maps // 2 else (maps - (j - i), j)
                rows.append(total[k][2 * a : 2 * a + 1] + total[k][2 * a + 1 : 2 * a + 2])
        group = lax.broadcasted_iota(I32, (members, 128), 1) // share
        own_group = group == lax.broadcasted_iota(I32, (members, 128), 0)
        for half in range(LANES // 128):
            c = (LANES // 128) * t + half
            sides = [None] * (LANES // 128)
            for p, row in enumerate(rows):
                piece = jnp.where(own_group, row[:, 128 * half : 128 * (half + 1)], 0.0)
                shift = (share * p) % 128
                piece = pltpu.roll(piece, shift, 1) if shift else piece
                side = share * p // 128
                sides[side] = piece if sides[side] is None else sides[side] + piece
            block = jnp.concatenate(sides, axis=1)
            for m in range(members):
                power[c, m] = block[m : m + 1]
            for m in range(members):
                power_copy(c, m).start()

    for kind, which, k in PROGRAM:
        if kind == "F":
            sums(which)
        elif kind == "K":
            sums(tiles + which)
        elif kind == "S":
            reduce_step(k, which)
        else:
            finish(which)

    others = power_got.shape[0] - 1
    whole = remote(power_got.at[0:others], power_got.at[0:others], power_sem.at[0], power_sem.at[1], partner)
    whole.wait_recv()
    power_got[me] = power[place, member]
    total = jnp.sum(power_got[0:others], axis=0)
    ell = share * me + lax.broadcasted_iota(I32, (1, 128), 1) % share
    for side in range(total.shape[1] // 128):
        line = total[:, 128 * side : 128 * (side + 1)] / (2 * ell + 1).astype(F32)
        line = pltpu.roll(line, (128 - share * member) % 128, 1)
        for p in range(128 // share * side, min(128 // share * (side + 1), spectra_ref.shape[0])):
            shift = (128 - share * p) % 128
            spectra_ref[p : p + 1, :] = (pltpu.roll(line, shift, 1) if shift else line)[:, :share]

    whole.wait_send()
    remote(out_core, got, core_send, core_recv.at[0, 0], partner).wait_send()
    four_copy.wait_send()
    for k in range(STEPS):
        remote(senders[k], receivers[k], step_send.at[k], step_recv.at[k, 0], partner).wait_send()
    for i in range(3):
        remote(s5.at[:, i], r5.at[:, i], last_send.at[i], last_recv.at[0], partner).wait_send()


def main_call(devices, sky_maps, legendre, owner_table):
    maps, cycles, pixels = sky_maps.shape
    _, orders, ells = legendre.shape
    width = 128
    coarse = pixels // width
    channels = 2 * maps
    tiles = ells // LANES
    pairs = maps * (maps + 1) // 2
    constants = tables(pixels, orders, width)
    hbm = pl.BlockSpec(memory_space=pltpu.HBM)
    vmem = pl.BlockSpec(memory_space=pltpu.VMEM)

    def steps(rows_of):
        return [pltpu.VMEM((BLOCKS, n, LANES), BF16) for n in rows_of for _ in range(2)]

    return pl.pallas_call(
        functools.partial(main_body, maps, cycles, orders),
        out_shape=[
            jax.ShapeDtypeStruct((4, maps, 2, ells), F32),
            jax.ShapeDtypeStruct((pairs, ells // devices), F32),
        ],
        in_specs=[hbm] * 5,
        out_specs=[vmem] * 2,
        scratch_shapes=[
            pltpu.VMEM((tiles, cycles, orders, LANES), BF16),
            pltpu.VMEM((maps, cycles, coarse, width), F32),
            pltpu.VMEM((2 * width, 2 * orders), F32),
            pltpu.VMEM((2 * coarse, 128), F32),
            pltpu.VMEM((2 * tiles, 256), F32),
            pltpu.VMEM((4, 128), I32),
            pltpu.SMEM((orders,), I32),
            pltpu.VMEM((2 * tiles, 8, 256), F32),
            pltpu.VMEM((2 * tiles, 2 * cycles * channels, 128), F32),
            pltpu.VMEM((3, 256, orders), BF16),
            pltpu.VMEM((2, tiles, HALVES, cycles, 64, LANES), BF16),
            pltpu.VMEM((2, tiles, HALVES, cycles, 64, LANES), BF16),
            pltpu.VMEM((2, tiles, HALVES, cycles, 64, LANES), BF16),
            pltpu.VMEM((cycles * channels, orders), BF16),
            pltpu.VMEM((cycles * channels, orders), BF16),
            *steps((512, 256, 128, 64)),
            pltpu.VMEM((BLOCKS, 3, 16, LANES), BF16),
            pltpu.VMEM((BLOCKS, 3, 16, LANES), BF16),
            pltpu.VMEM((BLOCKS, 512, LANES), F32),
            pltpu.VMEM((ells // 128, devices * 128 // ells, 1, LANES), F32),
            pltpu.VMEM((devices + 1, 1, LANES), F32),
            pltpu.SemaphoreType.DMA((tiles,)),
            pltpu.SemaphoreType.DMA((6,)),
            pltpu.SemaphoreType.DMA,
            pltpu.SemaphoreType.DMA((2, tiles)),
            pltpu.SemaphoreType.DMA((2,)),
            pltpu.SemaphoreType.DMA((STEPS,)),
            pltpu.SemaphoreType.DMA((STEPS, BLOCKS)),
            pltpu.SemaphoreType.DMA((3,)),
            pltpu.SemaphoreType.DMA((BLOCKS,)),
            pltpu.SemaphoreType.DMA((2,)),
        ],
        compiler_params=pltpu.CompilerParams(
            collective_id=0, has_side_effects=True, vmem_limit_bytes=int(53.55 * MIB)
        ),
        cost_estimate=pl.CostEstimate(flops=10_000_000_000, bytes_accessed=16 * MIB, transcendentals=0),
    )(
        legendre,
        sky_maps,
        jnp.asarray(constants),
        owner_table.reshape(4, 128),
        owner_table,
    )


def per_device(sky_maps, legendre, owner_table):
    devices = lax.axis_size(AXES)
    harmonics, spectra = main_call(devices, sky_maps, legendre, owner_table)
    return (harmonics, spectra)


def solution(mesh):
    return jax.shard_map(
        per_device,
        mesh=mesh,
        in_specs=(P(None, AXES, None), P(AXES, None, None), P()),
        out_specs=(P(AXES, None, None, None), P(None, AXES)),
        check_vma=False,
    )
```

```python
import functools
import math

import jax
import jax.numpy as jnp
import numpy as np
from jax import lax
from jax.experimental import pallas as pl
from jax.experimental.pallas import tpu as pltpu
from jax.sharding import PartitionSpec as P

AXES = ("blk", "grp")
MESH = pl.DeviceIdType.MESH
MIB = 1024 * 1024
F32, BF16, I32 = jnp.float32, jnp.bfloat16, jnp.int32

WIDTHS = (128, 128, 256, 256, 256, 256, 256, 256, 128, 128)
TILES = tuple((sum(WIDTHS[:t]), width) for t, width in enumerate(WIDTHS))
HALVES = 2
BLOCKS = HALVES * len(TILES)
STEPS = 4
ORDERS = (
    (1, 2, 5, 3, 4, 0), (3, 5, 1, 0, 2, 4), (2, 1, 5, 3, 4, 0), (3, 5, 2, 4, 0, 1),
    (5, 4, 2, 1, 3, 0), (4, 3, 5, 2, 0, 1), (0, 3, 2, 1, 5, 4), (0, 2, 1, 4, 5, 3),
    (4, 1, 3, 5, 2, 0), (3, 5, 4, 0, 2, 1), (2, 1, 0, 5, 4, 3), (4, 3, 0, 5, 2, 1),
    (5, 1, 3, 2, 0, 4), (2, 3, 4, 0, 1, 5), (3, 2, 4, 0, 1, 5), (1, 0, 4, 3, 2, 5),
    (3, 2, 4, 5, 0, 1), (1, 5, 3, 2, 0, 4), (5, 1, 2, 0, 3, 4), (1, 3, 2, 4, 5, 0),
)

PROGRAM = (
    ("F", 0, 0), ("F", 1, 0), ("F", 2, 0), ("F", 3, 0), ("F", 4, 0), ("F", 5, 0), ("F", 6, 0), ("F", 7, 0),
    ("F", 8, 0), ("F", 9, 0), ("K", 0, 0), ("S", 0, 0), ("S", 1, 0), ("K", 1, 0), ("S", 2, 0), ("S", 3, 0),
    ("K", 2, 0), ("S", 4, 0), ("S", 5, 0), ("K", 3, 0), ("S", 6, 0), ("K", 4, 0), ("S", 8, 0), ("S", 9, 0),
    ("K", 5, 0), ("S", 10, 0), ("K", 6, 0), ("S", 7, 0), ("S", 12, 0), ("K", 7, 0), ("S", 11, 0), ("S", 14, 0),
    ("S", 15, 0), ("K", 8, 0), ("S", 13, 0), ("K", 9, 0), ("S", 16, 0), ("S", 17, 0), ("S", 18, 0), ("S", 1, 1),
    ("S", 4, 1), ("S", 0, 1), ("S", 5, 1), ("S", 3, 1), ("S", 19, 0), ("S", 2, 1), ("S", 8, 1), ("S", 6, 1),
    ("S", 7, 1), ("S", 15, 1), ("S", 9, 1), ("S", 10, 1), ("S", 11, 1), ("S", 17, 1), ("S", 12, 1), ("S", 0, 2),
    ("S", 14, 1), ("S", 13, 1), ("S", 18, 1), ("S", 19, 1), ("S", 5, 2), ("S", 16, 1), ("S", 1, 2), ("S", 15, 2),
    ("S", 2, 2), ("S", 8, 2), ("S", 4, 2), ("S", 10, 2), ("S", 3, 2), ("S", 17, 2), ("S", 7, 2), ("S", 9, 2),
    ("S", 6, 2), ("S", 14, 2), ("S", 11, 2), ("S", 18, 2), ("S", 12, 2), ("S", 19, 2), ("S", 0, 3), ("S", 13, 2),
    ("S", 1, 3), ("S", 5, 3), ("S", 16, 2), ("S", 15, 3), ("S", 2, 3), ("S", 8, 3), ("S", 4, 3), ("S", 3, 3),
    ("S", 10, 3), ("S", 17, 3), ("S", 7, 3), ("S", 9, 3), ("S", 6, 3), ("S", 14, 3), ("S", 18, 3), ("S", 11, 3),
    ("S", 19, 3), ("S", 12, 3), ("S", 13, 3), ("S", 16, 3), ("E", 0, 0), ("E", 2, 0), ("E", 1, 0), ("E", 4, 0),
    ("E", 3, 0), ("E", 7, 0), ("E", 9, 0), ("E", 5, 0), ("E", 6, 0), ("E", 8, 0),
)


def split_bf16(values):
    high = values.astype(BF16)
    low = (values - high.astype(F32)).astype(BF16)
    return high, low


def dot3(left, right_high, right_low):
    high, low = split_bf16(left)
    dot = functools.partial(jnp.dot, preferred_element_type=F32)
    return dot(high, right_high) + (dot(high, right_low) + dot(low, right_high))


def tables(pixels, order_count, width):
    coarse = pixels // width
    k1, m1 = np.meshgrid(np.arange(coarse), np.arange(coarse), indexing="ij")
    angle = 2.0 * math.pi * ((k1 * m1) % coarse) / coarse
    first = np.concatenate([np.cos(angle.T), -np.sin(angle.T)], axis=0)
    k2 = np.arange(width)[:, None]
    m = np.arange(order_count)[None, :]
    angle = 2.0 * math.pi * ((k2 * m) % pixels) / pixels
    cosine, sine = np.cos(angle) / math.sqrt(pixels), np.sin(angle) / math.sqrt(pixels)
    second = np.block([[cosine, -sine], [sine, cosine]])
    out = np.zeros((second.shape[0] + first.shape[0], second.shape[1]), np.float32)
    out[: second.shape[0]] = second
    out[second.shape[0] :, :coarse] = first
    flips = row_flips()
    for core in range(2):
        out[second.shape[0] : second.shape[0] + flips.shape[1], 256 * (core + 1) : 256 * (core + 2)] = flips[core]
    return out


def position():
    blk, grp = lax.axis_index("blk"), lax.axis_index("grp")
    x, y = blk // 16, (blk // 4) % 4
    z = grp * 2 + (blk // 2) % 2
    return x, y, z, blk % 2


def device_at(x, y, z, core):
    return ((x * 4 + y) * 2 + z % 2) * 2 + core, z // 2


def moved(chip, core, gen):
    axis, c = gen % 3, chip[gen % 3]
    other = jnp.where((gen // 3 + core) % 2 == 0, c + 1 - 2 * (c % 2), 3 - c)
    return chip[:axis] + (other,) + chip[axis + 1 :]


def row_flips():
    out = np.zeros((2, 2, len(TILES), HALVES, 2, 32, 2), np.int32)
    for core, half, t, h, part, low, j in np.ndindex(*out.shape):
        flips = [0, 0, 0]
        for k, gen in enumerate(ORDERS[HALVES * t + h]):
            if ((half * 32 + low) >> (5 - k)) & 1:
                flips[gen % 3] ^= 1 if (gen // 3 + core + part) % 2 == 0 else 3
        device = ((flips[0] * 4 + flips[1]) * 2 + flips[2] % 2) * 4 + part * 2 + flips[2] // 2
        out[core, half, t, h, part, low, j] = device * 4 + h * 2 + j
    return out.reshape(2, -1, 256)


def spectral_values(x_ref, first, second):
    maps, cycles, coarse, width = x_ref.shape
    rows = maps * cycles
    columns = second.shape[1]
    spread = jnp.concatenate([x_ref[i // cycles, i % cycles] for i in range(rows)], axis=1)
    stage = dot3(first[:, :coarse], *split_bf16(spread))
    stages = []
    for i in range(rows):
        piece = stage[:, i * width : (i + 1) * width]
        stages.append(jnp.concatenate([piece[:coarse], piece[coarse:]], axis=1))
    full = dot3(jnp.concatenate(stages, axis=0), *split_bf16(second))
    m1 = lax.broadcasted_iota(I32, (1, coarse, columns), 1)
    col = lax.broadcasted_iota(I32, (1, coarse, columns), 2)
    full = jnp.where((col % coarse) == m1, full.reshape(rows, coarse, columns), 0.0)
    return jnp.sum(full, axis=1).astype(BF16)


def main_body(
    maps,
    cycles,
    orders,
    legendre_ref,
    sky_ref,
    tables_ref,
    table_ref,
    owner_ref,
    harm_ref,
    spectra_ref,
    leg,
    sky,
    second_buf,
    first_buf,
    flips,
    table,
    owner,
    lines,
    coefs,
    hot,
    own,
    out_core,
    got,
    four,
    four_got,
    s1,
    r1,
    s2,
    r2,
    s3,
    r3,
    s4,
    r4,
    s5,
    r5,
    acc,
    power,
    power_got,
    leg_sem,
    in_sem,
    core_send,
    core_recv,
    four_sem,
    step_send,
    step_recv,
    last_send,
    last_recv,
    power_sem,
):
    x, y, z, core = position()
    chip = (x, y, z)
    place = x * 4 + y
    member = ((z % 2) * 2 + core) * 2 + z // 2
    members = power.shape[1]
    me = place * members + member
    channels = 2 * maps
    tiles = len(TILES)

    def leg_copy(t):
        lanes = pl.ds(*TILES[t])
        return pltpu.make_async_copy(legendre_ref.at[:, :, lanes], leg.at[:, :, lanes], leg_sem.at[t])

    coarse = sky.shape[2]
    depth = second_buf.shape[0]
    mine = pl.ds(pl.multiple_of(256 * (core + 1), 256), 256)
    small = [
        pltpu.make_async_copy(tables_ref.at[pl.ds(depth, flips.shape[0]), mine], flips, in_sem.at[1]),
        pltpu.make_async_copy(table_ref, table, in_sem.at[2]),
    ]
    loads = [
        pltpu.make_async_copy(tables_ref.at[pl.ds(0, depth)], second_buf, in_sem.at[3]),
        pltpu.make_async_copy(tables_ref.at[pl.ds(depth, first_buf.shape[0]), pl.ds(0, 128)], first_buf, in_sem.at[4]),
        pltpu.make_async_copy(owner_ref, owner, in_sem.at[5]),
    ]
    for load in small:
        load.start()
    leg_copy(0).start()

    def sky_copy(k, carry):
        lanes = pl.ds(pl.multiple_of(k * 128, 128), 128)
        pltpu.make_async_copy(sky_ref.at[:, :, lanes], sky.at[:, :, k, :], in_sem.at[0]).start()
        return carry

    lax.fori_loop(0, coarse, sky_copy, 0)
    for load in loads:
        load.start()
    loads.append(pltpu.make_async_copy(sky, sky, in_sem.at[0]))

    barrier = pltpu.get_barrier_semaphore()
    partner = device_at(x, y, z, 1 - core)
    across = [device_at(*moved(chip, core, g), core) for g in range(6)]
    near = [partner] + across
    for device in near:
        pl.semaphore_signal(barrier, inc=1, device_id=device, device_id_type=MESH)

    def remote(src, dst, send, recv, device):
        return pltpu.make_async_remote_copy(
            src_ref=src, dst_ref=dst, send_sem=send, recv_sem=recv, device_id=device, device_id_type=MESH
        )

    def core_copy(half, t):
        place_in = (half, slice(None), slice(None), slice(None), pl.ds(*TILES[t]))
        i = (1 - half) * tiles + t
        return remote(out_core.at[place_in], got.at[place_in], core_send, core_recv.at[i % 4], partner)

    def make_hot(i):
        column = jnp.transpose(lines[i])[:, 0:1].astype(I32)
        lane = lax.broadcasted_iota(I32, (256, orders), 1)
        hot[i % 3] = jnp.where(column == lane, 1.0, 0.0).astype(BF16)

    def permute(i):
        half, t = 1 - i // tiles, i % tiles
        if half:
            leg_copy(t).wait()
        one_hot = hot[i % 3]
        first, width = TILES[t]
        lanes = slice(first, first + width)
        group = 256 // width
        for r in range(0, cycles, group):
            rows = jnp.concatenate([leg[r + n, :, lanes] for n in range(group)], axis=1)
            picked = jnp.dot(one_hot, rows, preferred_element_type=F32).astype(BF16)
            for h in range(HALVES):
                for n in range(group):
                    part = picked[128 * h : 128 * (h + 1), width * n : width * (n + 1)]
                    own[half, h, r + n, :, lanes] = part[:64]
                    out_core[half, h, r + n, :, lanes] = part[64:]
        core_copy(half, t).start()

    base = ((place * 2 + z % 2) * 4 + core * 2 + z // 2) * 4
    for load in small:
        load.wait()
    digits = jnp.concatenate([table[...] >> 4, table[...] & 15], axis=0).astype(F32).astype(BF16)
    for i in range(2 * tiles):
        row = (1 - i // tiles) * tiles + i % tiles
        slot = flips[row : row + 1, :].astype(I32) ^ base
        spot = jnp.where(lax.broadcasted_iota(I32, (128, 256), 0) == (slot & 127), 1.0, 0.0).astype(BF16)
        found = jnp.dot(digits, spot, preferred_element_type=F32)
        found = found[0:4] * 16.0 + found[4:8]
        found = jnp.where(lax.broadcasted_iota(I32, (4, 256), 0) == (slot >> 7), found, 0.0)
        lines[i] = jnp.broadcast_to(jnp.sum(found, axis=0, keepdims=True), (8, 256))
    for i in range(2):
        make_hot(i)

    pl.semaphore_wait(barrier, len(near))
    permute(0)
    for load in loads:
        load.wait()
    for t in range(1, tiles):
        leg_copy(t).start()
    spectral = spectral_values(sky, first_buf[...], second_buf[...])
    rows = maps * cycles
    out_row = lax.broadcasted_iota(I32, (cycles * channels, rows), 0)
    in_row = lax.broadcasted_iota(I32, (cycles * channels, rows), 1)
    value = jnp.zeros((cycles * channels, orders), F32)
    for q in range(2):
        wanted = (in_row % cycles) * channels + 2 * (in_row // cycles) + q
        pick = jnp.where(out_row == wanted, 1.0, 0.0).astype(BF16)
        value = value + jnp.dot(pick, spectral[:, q * orders : (q + 1) * orders], preferred_element_type=F32)
    four[...] = value.astype(BF16)
    four_copy = remote(four, four_got, four_sem.at[0], four_sem.at[1], partner)
    four_copy.start()

    def coefficients(i):
        every = jnp.concatenate([four[...], four_got[...]], axis=0)
        mine = jnp.concatenate([hot[i % 3, 128 * h : 128 * h + 64, :] for h in range(HALVES)], axis=0)
        coefs[i] = lax.dot_general(every, mine, (((1,), (1,)), ((), ())), preferred_element_type=F32)

    def lanes_of(t):
        return slice(TILES[t][0], TILES[t][0] + TILES[t][1])

    def partial(i, g):
        lane = lax.broadcasted_iota(I32, (channels, 128), 1) // 32
        sides = []
        for side in range(2):
            total = jnp.zeros((channels, 128), F32)
            for q in range(4):
                r = side * 4 + q
                piece = coefs[i, r * channels : (r + 1) * channels, :]
                shift = (32 * (q - g)) % 128
                piece = pltpu.roll(piece, shift, 1) if shift else piece
                total = jnp.where(lane == q, piece, total)
            sides.append(total)
        line = jnp.concatenate(sides, axis=1)
        wide = jnp.broadcast_to(line[None], (32, channels, 256)).reshape(256, 256)
        row = lax.broadcasted_iota(I32, (256, 256), 0) // channels
        col = lax.broadcasted_iota(I32, (256, 256), 1) % 32
        left = jnp.where(row == col, wide, 0.0).astype(BF16)
        at = slice(32 * (g % 2), 32 * (g % 2) + 32)
        lanes = lanes_of(i % tiles)
        right = jnp.concatenate(
            [ref[1 - i // tiles, g // 2, r, at, lanes] for ref in (own, got) for r in range(cycles)], axis=0
        )
        return jnp.dot(left, right, preferred_element_type=F32)

    senders, receivers = (s1, s2, s3, s4), (r1, r2, r3, r4)

    def step_copy(k, b):
        device = across[ORDERS[b][k]]
        at = (b % HALVES, slice(None), pl.ds(*TILES[b // HALVES]))
        return remote(senders[k].at[at], receivers[k].at[at], step_send.at[k], step_recv.at[k, b], device)

    def sums(i):
        half, t = 1 - i // tiles, i % tiles
        if i + 1 < 2 * tiles:
            permute(i + 1)
        if i == 0:
            four_copy.wait_recv()
            coefficients(0)
        core_copy(half, t).wait_recv()
        for g in range(4):
            at = (g // 2, slice((g % 2) * 256, (g % 2 + 1) * 256), lanes_of(t))
            value = partial(i, g)
            if half:
                s1[at] = value.astype(BF16)
            else:
                acc[at] = value
        if i + 1 < 2 * tiles:
            coefficients(i + 1)
        if i + 2 < 2 * tiles:
            make_hot(i + 2)
        if half:
            for h in range(HALVES):
                step_copy(0, HALVES * t + h).start()

    def last_copies(b):
        low, high = ORDERS[b][5], ORDERS[b][4]
        both = device_at(*moved(moved(chip, core, low), core, high), core)
        at, rest = (b % HALVES,), (slice(None), pl.ds(*TILES[b // HALVES]))
        return [
            remote(s5.at[at + (i,) + rest], r5.at[at + (i,) + rest], last_send.at[i], last_recv.at[b], device)
            for i, device in enumerate([across[low], across[high], both])
        ]

    def reduce_step(k, b):
        step_copy(k, b).wait_recv()
        arrived = receivers[k]
        h, lanes = b % HALVES, lanes_of(b // HALVES)
        if k + 1 < STEPS:
            n = 256 >> k
            leaving = acc[h, n : 2 * n, lanes] + arrived[h, n : 2 * n, lanes].astype(F32)
            senders[k + 1][h, :, lanes] = leaving.astype(BF16)
            step_copy(k + 1, b).start()
        else:
            n = 16
            leaving = acc[h, n : 4 * n, lanes] + arrived[h, n : 4 * n, lanes].astype(F32)
            for i in range(3):
                s5[h, i, :, lanes] = leaving[n * i : n * (i + 1)].astype(BF16)
            for copy in last_copies(b):
                copy.start()
        acc[h, 0:n, lanes] = acc[h, 0:n, lanes] + arrived[h, 0:n, lanes].astype(F32)

    def power_copy(c, m):
        there = device_at(c // 4, c % 4, (m % 2) * 2 + m // 4, (m // 2) % 2)
        self = me == c * members + m
        device = tuple(jnp.where(self, other, value) for value, other in zip(there, partner))
        row = jnp.where(self, power_got.shape[0] - 1, me)
        return remote(power.at[c, m], power_got.at[row], power_sem.at[0], power_sem.at[1], device)

    share = spectra_ref.shape[1]

    def finish(t):
        first, width = TILES[t]
        lanes = slice(first, first + width)
        ell = first + lax.broadcasted_iota(I32, (2 * channels, width), 1)
        total = [None] * maps
        for h in range(HALVES):
            b = HALVES * t + h
            at = (h, slice(None), slice(None), pl.ds(first, width))
            remote(s5.at[at], r5.at[at], last_send.at[0], last_recv.at[b], partner).wait_recv()
            value = acc[h, 0:16, lanes]
            for i in range(3):
                value = value + r5[h, i, :, lanes].astype(F32)
            pair = [owner[base + 2 * h + s] for s in range(2)]
            order = jnp.where(lax.broadcasted_iota(I32, (2 * channels, 1), 0) < channels, pair[0], pair[1])
            value = jnp.where(ell >= order, value, 0.0)
            for s in range(2):
                for a in range(maps):
                    row = s * channels + 2 * a
                    harm_ref[2 * h + s, a, :, lanes] = value[row : row + 2]
            weighted = jnp.where(order == 0, value, 2.0 * value)
            for s in range(2):
                mode = value[s * channels : (s + 1) * channels]
                heavy = weighted[s * channels : (s + 1) * channels]
                for k in range(maps // 2 + 1):
                    turned = mode if k == 0 else jnp.concatenate([mode[2 * k :], mode[: 2 * k]], axis=0)
                    term = heavy * turned
                    total[k] = term if total[k] is None else total[k] + term
        rows = []
        for i in range(maps):
            for j in range(i, maps):
                k, a = (j - i, i) if j - i <= maps // 2 else (maps - (j - i), j)
                rows.append(total[k][2 * a : 2 * a + 1] + total[k][2 * a + 1 : 2 * a + 2])
        group = lax.broadcasted_iota(I32, (members, 128), 1) // share
        own_group = group == lax.broadcasted_iota(I32, (members, 128), 0)
        for half in range(width // 128):
            c = first // 128 + half
            sides = [None] * (power.shape[3] // 128)
            for p, row in enumerate(rows):
                piece = jnp.where(own_group, row[:, 128 * half : 128 * (half + 1)], 0.0)
                shift = (share * p) % 128
                piece = pltpu.roll(piece, shift, 1) if shift else piece
                side = share * p // 128
                sides[side] = piece if sides[side] is None else sides[side] + piece
            block = jnp.concatenate(sides, axis=1)
            for m in range(members):
                power[c, m] = block[m : m + 1]
            for m in range(members):
                power_copy(c, m).start()

    for kind, which, k in PROGRAM:
        if kind == "F":
            sums(which)
        elif kind == "K":
            sums(tiles + which)
        elif kind == "S":
            reduce_step(k, which)
        else:
            finish(which)

    others = power_got.shape[0] - 1
    whole = remote(power_got.at[0:others], power_got.at[0:others], power_sem.at[0], power_sem.at[1], partner)
    whole.wait_recv()
    power_got[me] = power[place, member]
    total = jnp.sum(power_got[0:others], axis=0)
    ell = share * me + lax.broadcasted_iota(I32, (1, 128), 1) % share
    for side in range(total.shape[1] // 128):
        line = total[:, 128 * side : 128 * (side + 1)] / (2 * ell + 1).astype(F32)
        line = pltpu.roll(line, (128 - share * member) % 128, 1)
        for p in range(128 // share * side, min(128 // share * (side + 1), spectra_ref.shape[0])):
            shift = (128 - share * p) % 128
            spectra_ref[p : p + 1, :] = (pltpu.roll(line, shift, 1) if shift else line)[:, :share]

    whole.wait_send()
    remote(out_core, got, core_send, core_recv.at[0], partner).wait_send()
    four_copy.wait_send()
    for k in range(STEPS):
        remote(senders[k], receivers[k], step_send.at[k], step_recv.at[k, 0], partner).wait_send()
    for i in range(3):
        remote(s5.at[:, i], r5.at[:, i], last_send.at[i], last_recv.at[0], partner).wait_send()


def main_call(devices, sky_maps, legendre, owner_table):
    maps, cycles, pixels = sky_maps.shape
    _, orders, ells = legendre.shape
    width = 128
    coarse = pixels // width
    channels = 2 * maps
    tiles = len(TILES)
    pairs = maps * (maps + 1) // 2
    constants = tables(pixels, orders, width)
    hbm = pl.BlockSpec(memory_space=pltpu.HBM)
    vmem = pl.BlockSpec(memory_space=pltpu.VMEM)

    def steps(rows_of):
        return [pltpu.VMEM((HALVES, n, ells), BF16) for n in rows_of for _ in range(2)]

    return pl.pallas_call(
        functools.partial(main_body, maps, cycles, orders),
        out_shape=[
            jax.ShapeDtypeStruct((4, maps, 2, ells), F32),
            jax.ShapeDtypeStruct((pairs, ells // devices), F32),
        ],
        in_specs=[hbm] * 5,
        out_specs=[vmem] * 2,
        scratch_shapes=[
            pltpu.VMEM((cycles, orders, ells), BF16),
            pltpu.VMEM((maps, cycles, coarse, width), F32),
            pltpu.VMEM((2 * width, 2 * orders), F32),
            pltpu.VMEM((2 * coarse, 128), F32),
            pltpu.VMEM((32, 256), F32),
            pltpu.VMEM((4, 128), I32),
            pltpu.SMEM((orders,), I32),
            pltpu.VMEM((2 * tiles, 8, 256), F32),
            pltpu.VMEM((2 * tiles, 2 * cycles * channels, 128), F32),
            pltpu.VMEM((3, 256, orders), BF16),
            pltpu.VMEM((2, HALVES, cycles, 64, ells), BF16),
            pltpu.VMEM((2, HALVES, cycles, 64, ells), BF16),
            pltpu.VMEM((2, HALVES, cycles, 64, ells), BF16),
            pltpu.VMEM((cycles * channels, orders), BF16),
            pltpu.VMEM((cycles * channels, orders), BF16),
            *steps((512, 256, 128, 64)),
            pltpu.VMEM((HALVES, 3, 16, ells), BF16),
            pltpu.VMEM((HALVES, 3, 16, ells), BF16),
            pltpu.VMEM((HALVES, 512, ells), F32),
            pltpu.VMEM((ells // 128, devices * 128 // ells, 1, 256), F32),
            pltpu.VMEM((devices + 1, 1, 256), F32),
            pltpu.SemaphoreType.DMA((tiles,)),
            pltpu.SemaphoreType.DMA((6,)),
            pltpu.SemaphoreType.DMA,
            pltpu.SemaphoreType.DMA((4,)),
            pltpu.SemaphoreType.DMA((2,)),
            pltpu.SemaphoreType.DMA((STEPS,)),
            pltpu.SemaphoreType.DMA((STEPS, BLOCKS)),
            pltpu.SemaphoreType.DMA((3,)),
            pltpu.SemaphoreType.DMA((BLOCKS,)),
            pltpu.SemaphoreType.DMA((2,)),
        ],
        compiler_params=pltpu.CompilerParams(
            collective_id=0, has_side_effects=True, vmem_limit_bytes=int(53.55 * MIB)
        ),
        cost_estimate=pl.CostEstimate(flops=10_000_000_000, bytes_accessed=16 * MIB, transcendentals=0),
    )(
        legendre,
        sky_maps,
        jnp.asarray(constants),
        owner_table.reshape(4, 128),
        owner_table,
    )


def per_device(sky_maps, legendre, owner_table):
    devices = lax.axis_size(AXES)
    harmonics, spectra = main_call(devices, sky_maps, legendre, owner_table)
    return (harmonics, spectra)


def solution(mesh):
    return jax.shard_map(
        per_device,
        mesh=mesh,
        in_specs=(P(None, AXES, None), P(AXES, None, None), P()),
        out_specs=(P(AXES, None, None, None), P(None, AXES)),
        check_vma=False,
    )
```

```python
import functools
import math

import jax
import jax.numpy as jnp
import numpy as np
from jax import lax
from jax.experimental import pallas as pl
from jax.experimental.pallas import tpu as pltpu
from jax.sharding import PartitionSpec as P

AXES = ("blk", "grp")
MESH = pl.DeviceIdType.MESH
MIB = 1024 * 1024
F32, BF16, I32 = jnp.float32, jnp.bfloat16, jnp.int32

WIDTHS = (128, 128, 256, 256, 256, 256, 256, 256, 128, 128)
TILES = tuple((sum(WIDTHS[:t]), width) for t, width in enumerate(WIDTHS))
HALVES = 2
BLOCKS = HALVES * len(TILES)
STEPS = 4
ORDERS = (
    (1, 2, 5, 3, 4, 0), (3, 5, 1, 0, 2, 4), (2, 1, 5, 3, 4, 0), (3, 5, 2, 4, 0, 1),
    (5, 4, 2, 1, 3, 0), (4, 3, 5, 2, 0, 1), (0, 3, 2, 1, 5, 4), (0, 2, 1, 4, 5, 3),
    (4, 1, 3, 5, 2, 0), (3, 5, 4, 0, 2, 1), (2, 1, 0, 5, 4, 3), (4, 3, 0, 5, 2, 1),
    (5, 1, 3, 2, 0, 4), (2, 3, 4, 0, 1, 5), (3, 2, 4, 0, 1, 5), (1, 0, 4, 3, 2, 5),
    (3, 2, 4, 5, 0, 1), (1, 5, 3, 2, 0, 4), (5, 1, 2, 0, 3, 4), (1, 3, 2, 4, 5, 0),
)

PROGRAM = (
    ("F", 0, 0), ("F", 1, 0), ("F", 2, 0), ("F", 3, 0), ("F", 4, 0), ("F", 5, 0), ("F", 6, 0), ("F", 7, 0),
    ("F", 8, 0), ("F", 9, 0), ("K", 0, 0), ("S", 0, 0), ("S", 1, 0), ("K", 1, 0), ("S", 2, 0), ("S", 3, 0),
    ("K", 2, 0), ("S", 4, 0), ("S", 5, 0), ("K", 3, 0), ("S", 6, 0), ("K", 4, 0), ("S", 8, 0), ("S", 9, 0),
    ("K", 5, 0), ("S", 10, 0), ("K", 6, 0), ("S", 7, 0), ("S", 12, 0), ("K", 7, 0), ("S", 11, 0), ("S", 14, 0),
    ("S", 15, 0), ("K", 8, 0), ("S", 13, 0), ("K", 9, 0), ("S", 16, 0), ("S", 17, 0), ("S", 18, 0), ("S", 1, 1),
    ("S", 4, 1), ("S", 0, 1), ("S", 5, 1), ("S", 3, 1), ("S", 19, 0), ("S", 2, 1), ("S", 8, 1), ("S", 6, 1),
    ("S", 7, 1), ("S", 15, 1), ("S", 9, 1), ("S", 10, 1), ("S", 11, 1), ("S", 17, 1), ("S", 12, 1), ("S", 0, 2),
    ("S", 14, 1), ("S", 13, 1), ("S", 18, 1), ("S", 19, 1), ("S", 5, 2), ("S", 16, 1), ("S", 1, 2), ("S", 15, 2),
    ("S", 2, 2), ("S", 8, 2), ("S", 4, 2), ("S", 10, 2), ("S", 3, 2), ("S", 17, 2), ("S", 7, 2), ("S", 9, 2),
    ("S", 6, 2), ("S", 14, 2), ("S", 11, 2), ("S", 18, 2), ("S", 12, 2), ("S", 19, 2), ("S", 0, 3), ("S", 13, 2),
    ("S", 1, 3), ("S", 5, 3), ("S", 16, 2), ("S", 15, 3), ("S", 2, 3), ("S", 8, 3), ("S", 4, 3), ("S", 3, 3),
    ("S", 10, 3), ("S", 17, 3), ("S", 7, 3), ("S", 9, 3), ("S", 6, 3), ("S", 14, 3), ("S", 18, 3), ("S", 11, 3),
    ("S", 19, 3), ("S", 12, 3), ("S", 13, 3), ("S", 16, 3), ("E", 0, 0), ("E", 2, 0), ("E", 1, 0), ("E", 4, 0),
    ("E", 3, 0), ("E", 7, 0), ("E", 9, 0), ("E", 5, 0), ("E", 6, 0), ("E", 8, 0),
)


def arrival_slots():
    sent, waited = {}, {}
    for at, (kind, which, k) in enumerate(PROGRAM):
        if kind == "F":
            sent.update({(0, HALVES * which + h): at for h in range(HALVES)})
        elif kind == "S":
            waited[k, which] = at
            if k + 1 < STEPS:
                sent[k + 1, which] = at
    gen = {(k, b): ORDERS[b][k] for k, b in sent}
    slots, last = {}, []
    for later in sorted(sent, key=lambda m: (sent[m], m)):
        for slot, earlier in enumerate(last):
            if any(
                gen[m] == gen[later] and sent[m] >= waited[earlier] and waited[m] <= sent[later] for m in sent
            ):
                break
        else:
            slot = len(last)
            last.append(None)
        slots[later], last[slot] = slot, later
    return slots, len(last)


def split_bf16(values):
    high = values.astype(BF16)
    low = (values - high.astype(F32)).astype(BF16)
    return high, low


def dot3(left, right_high, right_low):
    high, low = split_bf16(left)
    dot = functools.partial(jnp.dot, preferred_element_type=F32)
    return dot(high, right_high) + (dot(high, right_low) + dot(low, right_high))


def tables(pixels, order_count, width):
    coarse = pixels // width
    k1, m1 = np.meshgrid(np.arange(coarse), np.arange(coarse), indexing="ij")
    angle = 2.0 * math.pi * ((k1 * m1) % coarse) / coarse
    first = np.concatenate([np.cos(angle.T), -np.sin(angle.T)], axis=0)
    k2 = np.arange(width)[:, None]
    m = np.arange(order_count)[None, :]
    angle = 2.0 * math.pi * ((k2 * m) % pixels) / pixels
    cosine, sine = np.cos(angle) / math.sqrt(pixels), np.sin(angle) / math.sqrt(pixels)
    second = np.block([[cosine, -sine], [sine, cosine]])
    out = np.zeros((second.shape[0] + first.shape[0], second.shape[1]), np.float32)
    out[: second.shape[0]] = second
    out[second.shape[0] :, :coarse] = first
    flips = row_flips()
    for core in range(2):
        out[second.shape[0] : second.shape[0] + flips.shape[1], 256 * (core + 1) : 256 * (core + 2)] = flips[core]
    return out


def position():
    blk, grp = lax.axis_index("blk"), lax.axis_index("grp")
    x, y = blk // 16, (blk // 4) % 4
    z = grp * 2 + (blk // 2) % 2
    return x, y, z, blk % 2


def device_at(x, y, z, core):
    return ((x * 4 + y) * 2 + z % 2) * 2 + core, z // 2


def moved(chip, core, gen):
    axis, c = gen % 3, chip[gen % 3]
    other = jnp.where((gen // 3 + core) % 2 == 0, c + 1 - 2 * (c % 2), 3 - c)
    return chip[:axis] + (other,) + chip[axis + 1 :]


def row_flips():
    out = np.zeros((2, 2, len(TILES), HALVES, 2, 32, 2), np.int32)
    for core, half, t, h, part, low, j in np.ndindex(*out.shape):
        flips = [0, 0, 0]
        for k, gen in enumerate(ORDERS[HALVES * t + h]):
            if ((half * 32 + low) >> (5 - k)) & 1:
                flips[gen % 3] ^= 1 if (gen // 3 + core + part) % 2 == 0 else 3
        device = ((flips[0] * 4 + flips[1]) * 2 + flips[2] % 2) * 4 + part * 2 + flips[2] // 2
        out[core, half, t, h, part, low, j] = device * 4 + h * 2 + j
    return out.reshape(2, -1, 256)


def spectral_values(x_ref, first, second):
    maps, cycles, coarse, width = x_ref.shape
    rows = maps * cycles
    columns = second.shape[1]
    spread = jnp.concatenate([x_ref[i // cycles, i % cycles] for i in range(rows)], axis=1)
    stage = dot3(first[:, :coarse], *split_bf16(spread))
    stages = []
    for i in range(rows):
        piece = stage[:, i * width : (i + 1) * width]
        stages.append(jnp.concatenate([piece[:coarse], piece[coarse:]], axis=1))
    full = dot3(jnp.concatenate(stages, axis=0), *split_bf16(second))
    m1 = lax.broadcasted_iota(I32, (1, coarse, columns), 1)
    col = lax.broadcasted_iota(I32, (1, coarse, columns), 2)
    full = jnp.where((col % coarse) == m1, full.reshape(rows, coarse, columns), 0.0)
    return jnp.sum(full, axis=1).astype(BF16)


def main_body(
    maps,
    cycles,
    orders,
    legendre_ref,
    sky_ref,
    tables_ref,
    table_ref,
    owner_ref,
    harm_ref,
    spectra_ref,
    leg,
    sky,
    second_buf,
    first_buf,
    flips,
    table,
    owner,
    lines,
    coefs,
    hot,
    own,
    out_core,
    got,
    four,
    four_got,
    s1,
    r1,
    s2,
    r2,
    s3,
    r3,
    s4,
    r4,
    s5,
    r5,
    acc,
    power,
    power_got,
    leg_sem,
    in_sem,
    core_send,
    core_recv,
    four_sem,
    step_send,
    step_recv,
    last_send,
    last_recv,
    power_sem,
):
    x, y, z, core = position()
    chip = (x, y, z)
    place = x * 4 + y
    member = ((z % 2) * 2 + core) * 2 + z // 2
    members = power.shape[1]
    me = place * members + member
    channels = 2 * maps
    tiles = len(TILES)

    def leg_copy(t):
        lanes = pl.ds(*TILES[t])
        return pltpu.make_async_copy(legendre_ref.at[:, :, lanes], leg.at[:, :, lanes], leg_sem.at[t])

    coarse = sky.shape[2]
    depth = second_buf.shape[0]
    mine = pl.ds(pl.multiple_of(256 * (core + 1), 256), 256)
    small = [
        pltpu.make_async_copy(tables_ref.at[pl.ds(depth, flips.shape[0]), mine], flips, in_sem.at[1]),
        pltpu.make_async_copy(table_ref, table, in_sem.at[2]),
    ]
    loads = [
        pltpu.make_async_copy(tables_ref.at[pl.ds(0, depth)], second_buf, in_sem.at[3]),
        pltpu.make_async_copy(tables_ref.at[pl.ds(depth, first_buf.shape[0]), pl.ds(0, 128)], first_buf, in_sem.at[4]),
        pltpu.make_async_copy(owner_ref, owner, in_sem.at[5]),
    ]
    for load in small:
        load.start()
    leg_copy(0).start()

    def sky_copy(k, carry):
        lanes = pl.ds(pl.multiple_of(k * 128, 128), 128)
        pltpu.make_async_copy(sky_ref.at[:, :, lanes], sky.at[:, :, k, :], in_sem.at[0]).start()
        return carry

    lax.fori_loop(0, coarse, sky_copy, 0)
    for load in loads:
        load.start()
    loads.append(pltpu.make_async_copy(sky, sky, in_sem.at[0]))

    barrier = pltpu.get_barrier_semaphore()
    partner = device_at(x, y, z, 1 - core)
    across = [device_at(*moved(chip, core, g), core) for g in range(6)]
    near = [partner] + across
    for device in near:
        pl.semaphore_signal(barrier, inc=1, device_id=device, device_id_type=MESH)

    def remote(src, dst, send, recv, device):
        return pltpu.make_async_remote_copy(
            src_ref=src, dst_ref=dst, send_sem=send, recv_sem=recv, device_id=device, device_id_type=MESH
        )

    def core_copy(half, t):
        place_in = (half, slice(None), slice(None), slice(None), pl.ds(*TILES[t]))
        i = (1 - half) * tiles + t
        return remote(out_core.at[place_in], got.at[place_in], core_send, core_recv.at[i % 8], partner)

    def make_hot(i):
        column = jnp.transpose(lines[i])[:, 0:1].astype(I32)
        lane = lax.broadcasted_iota(I32, (256, orders), 1)
        hot[i % 3] = jnp.where(column == lane, 1.0, 0.0).astype(BF16)

    def permute(i):
        half, t = 1 - i // tiles, i % tiles
        if half:
            leg_copy(t).wait()
        one_hot = hot[i % 3]
        first, width = TILES[t]
        lanes = slice(first, first + width)
        group = 256 // width
        for r in range(0, cycles, group):
            rows = jnp.concatenate([leg[r + n, :, lanes] for n in range(group)], axis=1)
            picked = jnp.dot(one_hot, rows, preferred_element_type=F32).astype(BF16)
            for h in range(HALVES):
                for n in range(group):
                    part = picked[128 * h : 128 * (h + 1), width * n : width * (n + 1)]
                    own[half, h, r + n, :, lanes] = part[:64]
                    out_core[half, h, r + n, :, lanes] = part[64:]
        core_copy(half, t).start()

    base = ((place * 2 + z % 2) * 4 + core * 2 + z // 2) * 4
    for load in small:
        load.wait()
    digits = jnp.concatenate([table[...] >> 4, table[...] & 15], axis=0).astype(F32).astype(BF16)
    for i in range(2 * tiles):
        row = (1 - i // tiles) * tiles + i % tiles
        slot = flips[row : row + 1, :].astype(I32) ^ base
        spot = jnp.where(lax.broadcasted_iota(I32, (128, 256), 0) == (slot & 127), 1.0, 0.0).astype(BF16)
        found = jnp.dot(digits, spot, preferred_element_type=F32)
        found = found[0:4] * 16.0 + found[4:8]
        found = jnp.where(lax.broadcasted_iota(I32, (4, 256), 0) == (slot >> 7), found, 0.0)
        lines[i] = jnp.broadcast_to(jnp.sum(found, axis=0, keepdims=True), (8, 256))
    for i in range(3):
        make_hot(i)

    pl.semaphore_wait(barrier, len(near))
    permute(0)
    for load in loads:
        load.wait()
    for t in range(1, tiles):
        leg_copy(t).start()
    spectral = spectral_values(sky, first_buf[...], second_buf[...])
    rows = maps * cycles
    out_row = lax.broadcasted_iota(I32, (cycles * channels, rows), 0)
    in_row = lax.broadcasted_iota(I32, (cycles * channels, rows), 1)
    value = jnp.zeros((cycles * channels, orders), F32)
    for q in range(2):
        wanted = (in_row % cycles) * channels + 2 * (in_row // cycles) + q
        pick = jnp.where(out_row == wanted, 1.0, 0.0).astype(BF16)
        value = value + jnp.dot(pick, spectral[:, q * orders : (q + 1) * orders], preferred_element_type=F32)
    four[...] = value.astype(BF16)
    four_copy = remote(four, four_got, four_sem.at[0], four_sem.at[1], partner)
    four_copy.start()
    permute(1)

    def coefficients(i):
        every = jnp.concatenate([four[...], four_got[...]], axis=0)
        mine = jnp.concatenate([hot[i % 3, 128 * h : 128 * h + 64, :] for h in range(HALVES)], axis=0)
        coefs[i] = lax.dot_general(every, mine, (((1,), (1,)), ((), ())), preferred_element_type=F32)

    def lanes_of(t):
        return slice(TILES[t][0], TILES[t][0] + TILES[t][1])

    def partial(i, g):
        lane = lax.broadcasted_iota(I32, (channels, 128), 1) // 32
        sides = []
        for side in range(2):
            total = jnp.zeros((channels, 128), F32)
            for q in range(4):
                r = side * 4 + q
                piece = coefs[i, r * channels : (r + 1) * channels, :]
                shift = (32 * (q - g)) % 128
                piece = pltpu.roll(piece, shift, 1) if shift else piece
                total = jnp.where(lane == q, piece, total)
            sides.append(total)
        line = jnp.concatenate(sides, axis=1)
        wide = jnp.broadcast_to(line[None], (32, channels, 256)).reshape(256, 256)
        row = lax.broadcasted_iota(I32, (256, 256), 0) // channels
        col = lax.broadcasted_iota(I32, (256, 256), 1) % 32
        left = jnp.where(row == col, wide, 0.0).astype(BF16)
        at = slice(32 * (g % 2), 32 * (g % 2) + 32)
        lanes = lanes_of(i % tiles)
        right = jnp.concatenate(
            [ref[1 - i // tiles, g // 2, r, at, lanes] for ref in (own, got) for r in range(cycles)], axis=0
        )
        return jnp.dot(left, right, preferred_element_type=F32)

    senders, receivers = (s1, s2, s3, s4), (r1, r2, r3, r4)

    slots, _ = arrival_slots()

    def step_copy(k, b):
        device = across[ORDERS[b][k]]
        at = (b % HALVES, slice(None), pl.ds(*TILES[b // HALVES]))
        return remote(senders[k].at[at], receivers[k].at[at], step_send.at[k], step_recv.at[slots[k, b]], device)

    def sums(i):
        half, t = 1 - i // tiles, i % tiles
        if 0 < i < 2 * tiles - 2:
            permute(i + 2)
        if i == 0:
            four_copy.wait_recv()
            coefficients(0)
        core_copy(half, t).wait_recv()
        for g in range(4):
            at = (g // 2, slice((g % 2) * 256, (g % 2 + 1) * 256), lanes_of(t))
            value = partial(i, g)
            if half:
                s1[at] = value.astype(BF16)
            else:
                acc[at] = value
        if i + 1 < 2 * tiles:
            coefficients(i + 1)
        if i + 3 < 2 * tiles:
            make_hot(i + 3)
        if half:
            for h in range(HALVES):
                step_copy(0, HALVES * t + h).start()
        if i == 0:
            permute(2)

    def last_copies(b):
        low, high = ORDERS[b][5], ORDERS[b][4]
        both = device_at(*moved(moved(chip, core, low), core, high), core)
        at, rest = (b % HALVES,), (slice(None), pl.ds(*TILES[b // HALVES]))
        return [
            remote(s5.at[at + (i,) + rest], r5.at[at + (i,) + rest], last_send.at[i], last_recv.at[b], device)
            for i, device in enumerate([across[low], across[high], both])
        ]

    def reduce_step(k, b):
        step_copy(k, b).wait_recv()
        arrived = receivers[k]
        h, lanes = b % HALVES, lanes_of(b // HALVES)
        if k + 1 < STEPS:
            n = 256 >> k
            leaving = acc[h, n : 2 * n, lanes] + arrived[h, n : 2 * n, lanes].astype(F32)
            senders[k + 1][h, :, lanes] = leaving.astype(BF16)
            step_copy(k + 1, b).start()
        else:
            n = 16
            leaving = acc[h, n : 4 * n, lanes] + arrived[h, n : 4 * n, lanes].astype(F32)
            for i in range(3):
                s5[h, i, :, lanes] = leaving[n * i : n * (i + 1)].astype(BF16)
            for copy in last_copies(b):
                copy.start()
        acc[h, 0:n, lanes] = acc[h, 0:n, lanes] + arrived[h, 0:n, lanes].astype(F32)

    def power_copy(c, m):
        there = device_at(c // 4, c % 4, (m % 2) * 2 + m // 4, (m // 2) % 2)
        self = me == c * members + m
        device = tuple(jnp.where(self, other, value) for value, other in zip(there, partner))
        row = jnp.where(self, power_got.shape[0] - 1, me)
        return remote(power.at[c, m], power_got.at[row], power_sem.at[0], power_sem.at[1], device)

    share = spectra_ref.shape[1]

    def finish(t):
        first, width = TILES[t]
        lanes = slice(first, first + width)
        ell = first + lax.broadcasted_iota(I32, (2 * channels, width), 1)
        total = [None] * maps
        for h in range(HALVES):
            b = HALVES * t + h
            at = (h, slice(None), slice(None), pl.ds(first, width))
            remote(s5.at[at], r5.at[at], last_send.at[0], last_recv.at[b], partner).wait_recv()
            value = acc[h, 0:16, lanes]
            for i in range(3):
                value = value + r5[h, i, :, lanes].astype(F32)
            pair = [owner[base + 2 * h + s] for s in range(2)]
            order = jnp.where(lax.broadcasted_iota(I32, (2 * channels, 1), 0) < channels, pair[0], pair[1])
            value = jnp.where(ell >= order, value, 0.0)
            for s in range(2):
                for a in range(maps):
                    row = s * channels + 2 * a
                    harm_ref[2 * h + s, a, :, lanes] = value[row : row + 2]
            weighted = jnp.where(order == 0, value, 2.0 * value)
            for s in range(2):
                mode = value[s * channels : (s + 1) * channels]
                heavy = weighted[s * channels : (s + 1) * channels]
                for k in range(maps // 2 + 1):
                    turned = mode if k == 0 else jnp.concatenate([mode[2 * k :], mode[: 2 * k]], axis=0)
                    term = heavy * turned
                    total[k] = term if total[k] is None else total[k] + term
        rows = []
        for i in range(maps):
            for j in range(i, maps):
                k, a = (j - i, i) if j - i <= maps // 2 else (maps - (j - i), j)
                rows.append(total[k][2 * a : 2 * a + 1] + total[k][2 * a + 1 : 2 * a + 2])
        group = lax.broadcasted_iota(I32, (members, 128), 1) // share
        own_group = group == lax.broadcasted_iota(I32, (members, 128), 0)
        for half in range(width // 128):
            c = first // 128 + half
            sides = [None] * (power.shape[3] // 128)
            for p, row in enumerate(rows):
                piece = jnp.where(own_group, row[:, 128 * half : 128 * (half + 1)], 0.0)
                shift = (share * p) % 128
                piece = pltpu.roll(piece, shift, 1) if shift else piece
                side = share * p // 128
                sides[side] = piece if sides[side] is None else sides[side] + piece
            block = jnp.concatenate(sides, axis=1)
            for m in range(members):
                power[c, m] = block[m : m + 1]
            for m in range(members):
                power_copy(c, m).start()

    for kind, which, k in PROGRAM:
        if kind == "F":
            sums(which)
        elif kind == "K":
            sums(tiles + which)
        elif kind == "S":
            reduce_step(k, which)
        else:
            finish(which)

    others = power_got.shape[0] - 1
    whole = remote(power_got.at[0:others], power_got.at[0:others], power_sem.at[0], power_sem.at[1], partner)
    whole.wait_recv()
    power_got[me] = power[place, member]
    total = jnp.sum(power_got[0:others], axis=0)
    ell = share * me + lax.broadcasted_iota(I32, (1, 128), 1) % share
    for side in range(total.shape[1] // 128):
        line = total[:, 128 * side : 128 * (side + 1)] / (2 * ell + 1).astype(F32)
        line = pltpu.roll(line, (128 - share * member) % 128, 1)
        for p in range(128 // share * side, min(128 // share * (side + 1), spectra_ref.shape[0])):
            shift = (128 - share * p) % 128
            spectra_ref[p : p + 1, :] = (pltpu.roll(line, shift, 1) if shift else line)[:, :share]

    whole.wait_send()
    remote(out_core, got, core_send, core_recv.at[0], partner).wait_send()
    four_copy.wait_send()
    for k in range(STEPS):
        remote(senders[k], receivers[k], step_send.at[k], step_recv.at[0], partner).wait_send()
    for i in range(3):
        remote(s5.at[:, i], r5.at[:, i], last_send.at[i], last_recv.at[0], partner).wait_send()


def main_call(devices, sky_maps, legendre, owner_table):
    maps, cycles, pixels = sky_maps.shape
    _, orders, ells = legendre.shape
    width = 128
    coarse = pixels // width
    channels = 2 * maps
    tiles = len(TILES)
    pairs = maps * (maps + 1) // 2
    constants = tables(pixels, orders, width)
    hbm = pl.BlockSpec(memory_space=pltpu.HBM)
    vmem = pl.BlockSpec(memory_space=pltpu.VMEM)

    def steps(rows_of):
        return [pltpu.VMEM((HALVES, n, ells), BF16) for n in rows_of for _ in range(2)]

    return pl.pallas_call(
        functools.partial(main_body, maps, cycles, orders),
        out_shape=[
            jax.ShapeDtypeStruct((4, maps, 2, ells), F32),
            jax.ShapeDtypeStruct((pairs, ells // devices), F32),
        ],
        in_specs=[hbm] * 5,
        out_specs=[vmem] * 2,
        scratch_shapes=[
            pltpu.VMEM((cycles, orders, ells), BF16),
            pltpu.VMEM((maps, cycles, coarse, width), F32),
            pltpu.VMEM((2 * width, 2 * orders), F32),
            pltpu.VMEM((2 * coarse, 128), F32),
            pltpu.VMEM((32, 256), F32),
            pltpu.VMEM((4, 128), I32),
            pltpu.SMEM((orders,), I32),
            pltpu.VMEM((2 * tiles, 8, 256), F32),
            pltpu.VMEM((2 * tiles, 2 * cycles * channels, 128), F32),
            pltpu.VMEM((3, 256, orders), BF16),
            pltpu.VMEM((2, HALVES, cycles, 64, ells), BF16),
            pltpu.VMEM((2, HALVES, cycles, 64, ells), BF16),
            pltpu.VMEM((2, HALVES, cycles, 64, ells), BF16),
            pltpu.VMEM((cycles * channels, orders), BF16),
            pltpu.VMEM((cycles * channels, orders), BF16),
            *steps((512, 256, 128, 64)),
            pltpu.VMEM((HALVES, 3, 16, ells), BF16),
            pltpu.VMEM((HALVES, 3, 16, ells), BF16),
            pltpu.VMEM((HALVES, 512, ells), F32),
            pltpu.VMEM((ells // 128, devices * 128 // ells, 1, 256), F32),
            pltpu.VMEM((devices + 1, 1, 256), F32),
            pltpu.SemaphoreType.DMA((tiles,)),
            pltpu.SemaphoreType.DMA((6,)),
            pltpu.SemaphoreType.DMA,
            pltpu.SemaphoreType.DMA((8,)),
            pltpu.SemaphoreType.DMA((2,)),
            pltpu.SemaphoreType.DMA((STEPS,)),
            pltpu.SemaphoreType.DMA((arrival_slots()[1],)),
            pltpu.SemaphoreType.DMA((3,)),
            pltpu.SemaphoreType.DMA((BLOCKS,)),
            pltpu.SemaphoreType.DMA((2,)),
        ],
        compiler_params=pltpu.CompilerParams(
            collective_id=0, has_side_effects=True, vmem_limit_bytes=int(53.55 * MIB)
        ),
        cost_estimate=pl.CostEstimate(flops=10_000_000_000, bytes_accessed=16 * MIB, transcendentals=0),
    )(
        legendre,
        sky_maps,
        jnp.asarray(constants),
        owner_table.reshape(4, 128),
        owner_table,
    )


def per_device(sky_maps, legendre, owner_table):
    devices = lax.axis_size(AXES)
    harmonics, spectra = main_call(devices, sky_maps, legendre, owner_table)
    return (harmonics, spectra)


def solution(mesh):
    return jax.shard_map(
        per_device,
        mesh=mesh,
        in_specs=(P(None, AXES, None), P(AXES, None, None), P()),
        out_specs=(P(AXES, None, None, None), P(None, AXES)),
        check_vma=False,
    )
```

```python
import functools
import math

import jax
import jax.numpy as jnp
import numpy as np
from jax import lax
from jax.experimental import pallas as pl
from jax.experimental.pallas import tpu as pltpu
from jax.sharding import PartitionSpec as P

AXES = ("blk", "grp")
MESH = pl.DeviceIdType.MESH
MIB = 1024 * 1024
F32, BF16, I32 = jnp.float32, jnp.bfloat16, jnp.int32

WIDTHS = (128, 128, 256, 256, 256, 256, 256, 256, 128, 128)
TILES = tuple((sum(WIDTHS[:t]), width) for t, width in enumerate(WIDTHS))
HALVES = 2
BLOCKS = HALVES * len(TILES)
STEPS = 4
ORDERS = (
    (1, 2, 5, 3, 4, 0), (3, 5, 1, 0, 2, 4), (2, 1, 5, 3, 4, 0), (3, 5, 2, 4, 0, 1),
    (5, 4, 2, 1, 3, 0), (4, 3, 5, 2, 0, 1), (0, 3, 2, 1, 5, 4), (0, 2, 1, 4, 5, 3),
    (4, 1, 3, 5, 2, 0), (3, 5, 4, 0, 2, 1), (2, 1, 0, 5, 4, 3), (4, 3, 0, 5, 2, 1),
    (5, 1, 3, 2, 0, 4), (2, 3, 4, 0, 1, 5), (3, 2, 4, 0, 1, 5), (1, 0, 4, 3, 2, 5),
    (3, 2, 4, 5, 0, 1), (1, 5, 3, 2, 0, 4), (5, 1, 2, 0, 3, 4), (1, 3, 2, 4, 5, 0),
)

PROGRAM = (
    ("F", 0, 0), ("F", 1, 0), ("F", 2, 0), ("F", 3, 0), ("F", 4, 0), ("F", 5, 0), ("F", 6, 0), ("F", 7, 0),
    ("F", 8, 0), ("F", 9, 0), ("K", 0, 0), ("S", 0, 0), ("S", 1, 0), ("K", 1, 0), ("S", 2, 0), ("S", 3, 0),
    ("K", 2, 0), ("S", 4, 0), ("S", 5, 0), ("K", 3, 0), ("S", 6, 0), ("K", 4, 0), ("S", 8, 0), ("S", 9, 0),
    ("K", 5, 0), ("S", 10, 0), ("K", 6, 0), ("S", 7, 0), ("S", 12, 0), ("K", 7, 0), ("S", 11, 0), ("S", 14, 0),
    ("S", 15, 0), ("K", 8, 0), ("S", 13, 0), ("K", 9, 0), ("S", 16, 0), ("S", 17, 0), ("S", 18, 0), ("S", 1, 1),
    ("S", 4, 1), ("S", 0, 1), ("S", 5, 1), ("S", 3, 1), ("S", 19, 0), ("S", 2, 1), ("S", 8, 1), ("S", 6, 1),
    ("S", 7, 1), ("S", 15, 1), ("S", 9, 1), ("S", 10, 1), ("S", 11, 1), ("S", 17, 1), ("S", 12, 1), ("S", 0, 2),
    ("S", 14, 1), ("S", 13, 1), ("S", 18, 1), ("S", 19, 1), ("S", 5, 2), ("S", 16, 1), ("S", 1, 2), ("S", 15, 2),
    ("S", 2, 2), ("S", 8, 2), ("S", 4, 2), ("S", 10, 2), ("S", 3, 2), ("S", 17, 2), ("S", 7, 2), ("S", 9, 2),
    ("S", 6, 2), ("S", 14, 2), ("S", 11, 2), ("S", 18, 2), ("S", 12, 2), ("S", 19, 2), ("S", 0, 3), ("S", 13, 2),
    ("S", 1, 3), ("S", 5, 3), ("S", 16, 2), ("S", 15, 3), ("S", 2, 3), ("S", 8, 3), ("S", 4, 3), ("S", 3, 3),
    ("S", 10, 3), ("S", 17, 3), ("S", 7, 3), ("S", 9, 3), ("S", 6, 3), ("S", 14, 3), ("S", 18, 3), ("S", 11, 3),
    ("S", 19, 3), ("S", 12, 3), ("S", 13, 3), ("S", 16, 3), ("E", 0, 0), ("E", 2, 0), ("E", 1, 0), ("E", 4, 0),
    ("E", 3, 0), ("E", 7, 0), ("E", 9, 0), ("E", 5, 0), ("E", 6, 0), ("E", 8, 0),
)


def arrival_slots():
    sent, waited = {}, {}
    for at, (kind, which, k) in enumerate(PROGRAM):
        if kind == "F":
            sent.update({(0, HALVES * which + h): at for h in range(HALVES)})
        elif kind == "S":
            waited[k, which] = at
            if k + 1 < STEPS:
                sent[k + 1, which] = at
    gen = {(k, b): ORDERS[b][k] for k, b in sent}
    slots, last = {}, []
    for later in sorted(sent, key=lambda m: (sent[m], m)):
        for slot, earlier in enumerate(last):
            if any(
                gen[m] == gen[later] and sent[m] >= waited[earlier] and waited[m] <= sent[later] for m in sent
            ):
                break
        else:
            slot = len(last)
            last.append(None)
        slots[later], last[slot] = slot, later
    return slots, len(last)


def split_bf16(values):
    high = values.astype(BF16)
    low = (values - high.astype(F32)).astype(BF16)
    return high, low


def dot3(left, right_high, right_low):
    high, low = split_bf16(left)
    dot = functools.partial(jnp.dot, preferred_element_type=F32)
    return dot(high, right_high) + (dot(high, right_low) + dot(low, right_high))


def tables(pixels, order_count, width):
    coarse = pixels // width
    k1, m1 = np.meshgrid(np.arange(coarse), np.arange(coarse), indexing="ij")
    angle = 2.0 * math.pi * ((k1 * m1) % coarse) / coarse
    first = np.concatenate([np.cos(angle.T), -np.sin(angle.T)], axis=0)
    k2 = np.arange(width)[:, None]
    m = np.arange(order_count)[None, :]
    angle = 2.0 * math.pi * ((k2 * m) % pixels) / pixels
    cosine, sine = np.cos(angle) / math.sqrt(pixels), np.sin(angle) / math.sqrt(pixels)
    second = np.block([[cosine, -sine], [sine, cosine]])
    out = np.zeros((second.shape[0] + first.shape[0], second.shape[1]), np.float32)
    out[: second.shape[0]] = second
    out[second.shape[0] :, :coarse] = first
    flips = row_flips()
    for core in range(2):
        out[second.shape[0] : second.shape[0] + flips.shape[1], 256 * (core + 1) : 256 * (core + 2)] = flips[core]
    return out


def position():
    blk, grp = lax.axis_index("blk"), lax.axis_index("grp")
    x, y = blk // 16, (blk // 4) % 4
    z = grp * 2 + (blk // 2) % 2
    return x, y, z, blk % 2


def device_at(x, y, z, core):
    return ((x * 4 + y) * 2 + z % 2) * 2 + core, z // 2


def moved(chip, core, gen):
    axis, c = gen % 3, chip[gen % 3]
    other = jnp.where((gen // 3 + core) % 2 == 0, c + 1 - 2 * (c % 2), 3 - c)
    return chip[:axis] + (other,) + chip[axis + 1 :]


def row_flips():
    out = np.zeros((2, 2, len(TILES), HALVES, 2, 32, 2), np.int32)
    for core, half, t, h, part, low, j in np.ndindex(*out.shape):
        flips = [0, 0, 0]
        for k, gen in enumerate(ORDERS[HALVES * t + h]):
            if ((half * 32 + low) >> (5 - k)) & 1:
                flips[gen % 3] ^= 1 if (gen // 3 + core + part) % 2 == 0 else 3
        device = ((flips[0] * 4 + flips[1]) * 2 + flips[2] % 2) * 4 + part * 2 + flips[2] // 2
        out[core, half, t, h, part, low, j] = device * 4 + h * 2 + j
    return out.reshape(2, -1, 256)


def spectral_values(x_ref, first, second):
    maps, cycles, coarse, width = x_ref.shape
    rows = maps * cycles
    columns = second.shape[1]
    spread = jnp.concatenate([x_ref[i // cycles, i % cycles] for i in range(rows)], axis=1)
    stage = dot3(first[:, :coarse], *split_bf16(spread))
    stages = []
    for i in range(rows):
        piece = stage[:, i * width : (i + 1) * width]
        stages.append(jnp.concatenate([piece[:coarse], piece[coarse:]], axis=1))
    full = dot3(jnp.concatenate(stages, axis=0), *split_bf16(second))
    m1 = lax.broadcasted_iota(I32, (1, coarse, columns), 1)
    col = lax.broadcasted_iota(I32, (1, coarse, columns), 2)
    full = jnp.where((col % coarse) == m1, full.reshape(rows, coarse, columns), 0.0)
    return jnp.sum(full, axis=1).astype(BF16)


def main_body(
    maps,
    cycles,
    orders,
    legendre_ref,
    sky_ref,
    tables_ref,
    table_ref,
    owner_ref,
    harm_ref,
    spectra_ref,
    leg,
    sky,
    second_buf,
    first_buf,
    flips,
    table,
    owner,
    lines,
    coefs,
    hot,
    own,
    out_core,
    got,
    four,
    four_got,
    s1,
    r1,
    s2,
    r2,
    s3,
    r3,
    s4,
    r4,
    s5,
    r5,
    acc,
    power,
    power_got,
    leg_sem,
    in_sem,
    core_send,
    core_recv,
    four_sem,
    step_send,
    step_recv,
    last_send,
    last_recv,
    power_sem,
):
    x, y, z, core = position()
    chip = (x, y, z)
    place = x * 4 + y
    member = ((z % 2) * 2 + core) * 2 + z // 2
    members = power.shape[1]
    me = place * members + member
    channels = 2 * maps
    tiles = len(TILES)

    def leg_copy(t):
        lanes = pl.ds(*TILES[t])
        return pltpu.make_async_copy(legendre_ref.at[:, :, lanes], leg.at[:, :, lanes], leg_sem.at[t])

    coarse = sky.shape[2]
    depth = second_buf.shape[0]
    mine = pl.ds(pl.multiple_of(256 * (core + 1), 256), 256)
    small = [
        pltpu.make_async_copy(tables_ref.at[pl.ds(depth, flips.shape[0]), mine], flips, in_sem.at[1]),
        pltpu.make_async_copy(table_ref, table, in_sem.at[2]),
    ]
    loads = [
        pltpu.make_async_copy(tables_ref.at[pl.ds(0, depth)], second_buf, in_sem.at[3]),
        pltpu.make_async_copy(tables_ref.at[pl.ds(depth, first_buf.shape[0]), pl.ds(0, 128)], first_buf, in_sem.at[4]),
        pltpu.make_async_copy(owner_ref, owner, in_sem.at[5]),
    ]
    for load in small:
        load.start()
    leg_copy(0).start()

    def sky_copy(k, carry):
        lanes = pl.ds(pl.multiple_of(k * 128, 128), 128)
        pltpu.make_async_copy(sky_ref.at[:, :, lanes], sky.at[:, :, k, :], in_sem.at[0]).start()
        return carry

    lax.fori_loop(0, coarse, sky_copy, 0)
    for load in loads:
        load.start()
    loads.append(pltpu.make_async_copy(sky, sky, in_sem.at[0]))

    barrier = pltpu.get_barrier_semaphore()
    partner = device_at(x, y, z, 1 - core)
    across = [device_at(*moved(chip, core, g), core) for g in range(6)]
    near = [partner] + across
    for device in near:
        pl.semaphore_signal(barrier, inc=1, device_id=device, device_id_type=MESH)

    def remote(src, dst, send, recv, device):
        return pltpu.make_async_remote_copy(
            src_ref=src, dst_ref=dst, send_sem=send, recv_sem=recv, device_id=device, device_id_type=MESH
        )

    def core_copy(half, t):
        place_in = (half, slice(None), slice(None), slice(None), pl.ds(*TILES[t]))
        i = (1 - half) * tiles + t
        return remote(out_core.at[place_in], got.at[place_in], core_send, core_recv.at[i % 4], partner)

    def make_hot(i):
        column = jnp.transpose(lines[i])[:, 0:1].astype(I32)
        lane = lax.broadcasted_iota(I32, (256, orders), 1)
        hot[i % 3] = jnp.where(column == lane, 1.0, 0.0).astype(BF16)

    def permute(i):
        half, t = 1 - i // tiles, i % tiles
        if half:
            leg_copy(t).wait()
        one_hot = hot[i % 3]
        first, width = TILES[t]
        lanes = slice(first, first + width)
        group = 256 // width
        for r in range(0, cycles, group):
            rows = jnp.concatenate([leg[r + n, :, lanes] for n in range(group)], axis=1)
            picked = jnp.dot(one_hot, rows, preferred_element_type=F32).astype(BF16)
            for h in range(HALVES):
                for n in range(group):
                    part = picked[128 * h : 128 * (h + 1), width * n : width * (n + 1)]
                    own[half, h, r + n, :, lanes] = part[:64]
                    out_core[half, h, r + n, :, lanes] = part[64:]
        core_copy(half, t).start()

    base = ((place * 2 + z % 2) * 4 + core * 2 + z // 2) * 4
    for load in small:
        load.wait()
    digits = jnp.concatenate([table[...] >> 4, table[...] & 15], axis=0).astype(F32).astype(BF16)
    for i in range(2 * tiles):
        row = (1 - i // tiles) * tiles + i % tiles
        slot = flips[row : row + 1, :].astype(I32) ^ base
        spot = jnp.where(lax.broadcasted_iota(I32, (128, 256), 0) == (slot & 127), 1.0, 0.0).astype(BF16)
        found = jnp.dot(digits, spot, preferred_element_type=F32)
        found = found[0:4] * 16.0 + found[4:8]
        found = jnp.where(lax.broadcasted_iota(I32, (4, 256), 0) == (slot >> 7), found, 0.0)
        lines[i] = jnp.broadcast_to(jnp.sum(found, axis=0, keepdims=True), (8, 256))
    for i in range(2):
        make_hot(i)

    for load in loads:
        load.wait()
    for t in range(1, tiles):
        leg_copy(t).start()
    spectral = spectral_values(sky, first_buf[...], second_buf[...])
    rows = maps * cycles
    out_row = lax.broadcasted_iota(I32, (cycles * channels, rows), 0)
    in_row = lax.broadcasted_iota(I32, (cycles * channels, rows), 1)
    value = jnp.zeros((cycles * channels, orders), F32)
    for q in range(2):
        wanted = (in_row % cycles) * channels + 2 * (in_row // cycles) + q
        pick = jnp.where(out_row == wanted, 1.0, 0.0).astype(BF16)
        value = value + jnp.dot(pick, spectral[:, q * orders : (q + 1) * orders], preferred_element_type=F32)
    four[...] = value.astype(BF16)
    pl.semaphore_wait(barrier, len(near))
    four_copy = remote(four, four_got, four_sem.at[0], four_sem.at[1], partner)
    four_copy.start()
    permute(0)

    def coefficients(i):
        every = jnp.concatenate([four[...], four_got[...]], axis=0)
        mine = jnp.concatenate([hot[i % 3, 128 * h : 128 * h + 64, :] for h in range(HALVES)], axis=0)
        coefs[i] = lax.dot_general(every, mine, (((1,), (1,)), ((), ())), preferred_element_type=F32)

    def lanes_of(t):
        return slice(TILES[t][0], TILES[t][0] + TILES[t][1])

    def partial(i, g):
        lane = lax.broadcasted_iota(I32, (channels, 128), 1) // 32
        sides = []
        for side in range(2):
            total = jnp.zeros((channels, 128), F32)
            for q in range(4):
                r = side * 4 + q
                piece = coefs[i, r * channels : (r + 1) * channels, :]
                shift = (32 * (q - g)) % 128
                piece = pltpu.roll(piece, shift, 1) if shift else piece
                total = jnp.where(lane == q, piece, total)
            sides.append(total)
        line = jnp.concatenate(sides, axis=1)
        wide = jnp.broadcast_to(line[None], (32, channels, 256)).reshape(256, 256)
        row = lax.broadcasted_iota(I32, (256, 256), 0) // channels
        col = lax.broadcasted_iota(I32, (256, 256), 1) % 32
        left = jnp.where(row == col, wide, 0.0).astype(BF16)
        at = slice(32 * (g % 2), 32 * (g % 2) + 32)
        lanes = lanes_of(i % tiles)
        right = jnp.concatenate(
            [ref[1 - i // tiles, g // 2, r, at, lanes] for ref in (own, got) for r in range(cycles)], axis=0
        )
        return jnp.dot(left, right, preferred_element_type=F32)

    senders, receivers = (s1, s2, s3, s4), (r1, r2, r3, r4)

    slots, _ = arrival_slots()

    def step_copy(k, b):
        device = across[ORDERS[b][k]]
        at = (b % HALVES, slice(None), pl.ds(*TILES[b // HALVES]))
        return remote(senders[k].at[at], receivers[k].at[at], step_send.at[k], step_recv.at[slots[k, b]], device)

    def sums(i):
        half, t = 1 - i // tiles, i % tiles
        if i + 1 < 2 * tiles:
            permute(i + 1)
        if i == 0:
            four_copy.wait_recv()
            coefficients(0)
        core_copy(half, t).wait_recv()
        for g in range(4):
            at = (g // 2, slice((g % 2) * 256, (g % 2 + 1) * 256), lanes_of(t))
            value = partial(i, g)
            if half:
                s1[at] = value.astype(BF16)
            else:
                acc[at] = value
        if i + 1 < 2 * tiles:
            coefficients(i + 1)
        if i + 2 < 2 * tiles:
            make_hot(i + 2)
        if half:
            for h in range(HALVES):
                step_copy(0, HALVES * t + h).start()

    def last_copies(b):
        low, high = ORDERS[b][5], ORDERS[b][4]
        both = device_at(*moved(moved(chip, core, low), core, high), core)
        at, rest = (b % HALVES,), (slice(None), pl.ds(*TILES[b // HALVES]))
        return [
            remote(s5.at[at + (i,) + rest], r5.at[at + (i,) + rest], last_send.at[i], last_recv.at[b], device)
            for i, device in enumerate([across[low], across[high], both])
        ]

    def reduce_step(k, b):
        step_copy(k, b).wait_recv()
        arrived = receivers[k]
        h, lanes = b % HALVES, lanes_of(b // HALVES)
        if k + 1 < STEPS:
            n = 256 >> k
            leaving = acc[h, n : 2 * n, lanes] + arrived[h, n : 2 * n, lanes].astype(F32)
            senders[k + 1][h, :, lanes] = leaving.astype(BF16)
            step_copy(k + 1, b).start()
        else:
            n = 16
            leaving = acc[h, n : 4 * n, lanes] + arrived[h, n : 4 * n, lanes].astype(F32)
            for i in range(3):
                s5[h, i, :, lanes] = leaving[n * i : n * (i + 1)].astype(BF16)
            for copy in last_copies(b):
                copy.start()
        acc[h, 0:n, lanes] = acc[h, 0:n, lanes] + arrived[h, 0:n, lanes].astype(F32)

    def power_copy(c, m):
        there = device_at(c // 4, c % 4, (m % 2) * 2 + m // 4, (m // 2) % 2)
        self = me == c * members + m
        device = tuple(jnp.where(self, other, value) for value, other in zip(there, partner))
        row = jnp.where(self, power_got.shape[0] - 1, me)
        return remote(power.at[c, m], power_got.at[row], power_sem.at[0], power_sem.at[1], device)

    share = spectra_ref.shape[1]

    def finish(t):
        first, width = TILES[t]
        lanes = slice(first, first + width)
        ell = first + lax.broadcasted_iota(I32, (2 * channels, width), 1)
        total = [None] * maps
        for h in range(HALVES):
            b = HALVES * t + h
            at = (h, slice(None), slice(None), pl.ds(first, width))
            remote(s5.at[at], r5.at[at], last_send.at[0], last_recv.at[b], partner).wait_recv()
            value = acc[h, 0:16, lanes]
            for i in range(3):
                value = value + r5[h, i, :, lanes].astype(F32)
            pair = [owner[base + 2 * h + s] for s in range(2)]
            order = jnp.where(lax.broadcasted_iota(I32, (2 * channels, 1), 0) < channels, pair[0], pair[1])
            value = jnp.where(ell >= order, value, 0.0)
            for s in range(2):
                for a in range(maps):
                    row = s * channels + 2 * a
                    harm_ref[2 * h + s, a, :, lanes] = value[row : row + 2]
            weighted = jnp.where(order == 0, value, 2.0 * value)
            for s in range(2):
                mode = value[s * channels : (s + 1) * channels]
                heavy = weighted[s * channels : (s + 1) * channels]
                for k in range(maps // 2 + 1):
                    turned = mode if k == 0 else jnp.concatenate([mode[2 * k :], mode[: 2 * k]], axis=0)
                    term = heavy * turned
                    total[k] = term if total[k] is None else total[k] + term
        rows = []
        for i in range(maps):
            for j in range(i, maps):
                k, a = (j - i, i) if j - i <= maps // 2 else (maps - (j - i), j)
                rows.append(total[k][2 * a : 2 * a + 1] + total[k][2 * a + 1 : 2 * a + 2])
        group = lax.broadcasted_iota(I32, (members, 128), 1) // share
        own_group = group == lax.broadcasted_iota(I32, (members, 128), 0)
        for half in range(width // 128):
            c = first // 128 + half
            sides = [None] * (power.shape[3] // 128)
            for p, row in enumerate(rows):
                piece = jnp.where(own_group, row[:, 128 * half : 128 * (half + 1)], 0.0)
                shift = (share * p) % 128
                piece = pltpu.roll(piece, shift, 1) if shift else piece
                side = share * p // 128
                sides[side] = piece if sides[side] is None else sides[side] + piece
            block = jnp.concatenate(sides, axis=1)
            for m in range(members):
                power[c, m] = block[m : m + 1]
            for m in range(members):
                power_copy(c, m).start()

    for kind, which, k in PROGRAM:
        if kind == "F":
            sums(which)
        elif kind == "K":
            sums(tiles + which)
        elif kind == "S":
            reduce_step(k, which)
        else:
            finish(which)

    others = power_got.shape[0] - 1
    whole = remote(power_got.at[0:others], power_got.at[0:others], power_sem.at[0], power_sem.at[1], partner)
    whole.wait_recv()
    power_got[me] = power[place, member]
    total = jnp.sum(power_got[0:others], axis=0)
    ell = share * me + lax.broadcasted_iota(I32, (1, 128), 1) % share
    for side in range(total.shape[1] // 128):
        line = total[:, 128 * side : 128 * (side + 1)] / (2 * ell + 1).astype(F32)
        line = pltpu.roll(line, (128 - share * member) % 128, 1)
        for p in range(128 // share * side, min(128 // share * (side + 1), spectra_ref.shape[0])):
            shift = (128 - share * p) % 128
            spectra_ref[p : p + 1, :] = (pltpu.roll(line, shift, 1) if shift else line)[:, :share]

    whole.wait_send()
    remote(out_core, got, core_send, core_recv.at[0], partner).wait_send()
    four_copy.wait_send()
    for k in range(STEPS):
        remote(senders[k], receivers[k], step_send.at[k], step_recv.at[0], partner).wait_send()
    for i in range(3):
        remote(s5.at[:, i], r5.at[:, i], last_send.at[i], last_recv.at[0], partner).wait_send()


def main_call(devices, sky_maps, legendre, owner_table):
    maps, cycles, pixels = sky_maps.shape
    _, orders, ells = legendre.shape
    width = 128
    coarse = pixels // width
    channels = 2 * maps
    tiles = len(TILES)
    pairs = maps * (maps + 1) // 2
    constants = tables(pixels, orders, width)
    hbm = pl.BlockSpec(memory_space=pltpu.HBM)
    vmem = pl.BlockSpec(memory_space=pltpu.VMEM)

    def steps(rows_of):
        return [pltpu.VMEM((HALVES, n, ells), BF16) for n in rows_of for _ in range(2)]

    return pl.pallas_call(
        functools.partial(main_body, maps, cycles, orders),
        out_shape=[
            jax.ShapeDtypeStruct((4, maps, 2, ells), F32),
            jax.ShapeDtypeStruct((pairs, ells // devices), F32),
        ],
        in_specs=[hbm] * 5,
        out_specs=[vmem] * 2,
        scratch_shapes=[
            pltpu.VMEM((cycles, orders, ells), BF16),
            pltpu.VMEM((maps, cycles, coarse, width), F32),
            pltpu.VMEM((2 * width, 2 * orders), F32),
            pltpu.VMEM((2 * coarse, 128), F32),
            pltpu.VMEM((32, 256), F32),
            pltpu.VMEM((4, 128), I32),
            pltpu.SMEM((orders,), I32),
            pltpu.VMEM((2 * tiles, 8, 256), F32),
            pltpu.VMEM((2 * tiles, 2 * cycles * channels, 128), F32),
            pltpu.VMEM((3, 256, orders), BF16),
            pltpu.VMEM((2, HALVES, cycles, 64, ells), BF16),
            pltpu.VMEM((2, HALVES, cycles, 64, ells), BF16),
            pltpu.VMEM((2, HALVES, cycles, 64, ells), BF16),
            pltpu.VMEM((cycles * channels, orders), BF16),
            pltpu.VMEM((cycles * channels, orders), BF16),
            *steps((512, 256, 128, 64)),
            pltpu.VMEM((HALVES, 3, 16, ells), BF16),
            pltpu.VMEM((HALVES, 3, 16, ells), BF16),
            pltpu.VMEM((HALVES, 512, ells), F32),
            pltpu.VMEM((ells // 128, devices * 128 // ells, 1, 256), F32),
            pltpu.VMEM((devices + 1, 1, 256), F32),
            pltpu.SemaphoreType.DMA((tiles,)),
            pltpu.SemaphoreType.DMA((6,)),
            pltpu.SemaphoreType.DMA,
            pltpu.SemaphoreType.DMA((4,)),
            pltpu.SemaphoreType.DMA((2,)),
            pltpu.SemaphoreType.DMA((STEPS,)),
            pltpu.SemaphoreType.DMA((arrival_slots()[1],)),
            pltpu.SemaphoreType.DMA((3,)),
            pltpu.SemaphoreType.DMA((BLOCKS,)),
            pltpu.SemaphoreType.DMA((2,)),
        ],
        compiler_params=pltpu.CompilerParams(
            collective_id=0, has_side_effects=True, vmem_limit_bytes=int(53.55 * MIB)
        ),
        cost_estimate=pl.CostEstimate(flops=10_000_000_000, bytes_accessed=16 * MIB, transcendentals=0),
    )(
        legendre,
        sky_maps,
        jnp.asarray(constants),
        owner_table.reshape(4, 128),
        owner_table,
    )


def per_device(sky_maps, legendre, owner_table):
    devices = lax.axis_size(AXES)
    harmonics, spectra = main_call(devices, sky_maps, legendre, owner_table)
    return (harmonics, spectra)


def solution(mesh):
    return jax.shard_map(
        per_device,
        mesh=mesh,
        in_specs=(P(None, AXES, None), P(AXES, None, None), P()),
        out_specs=(P(AXES, None, None, None), P(None, AXES)),
        check_vma=False,
    )
```
